32 devices in a mesh: rep: 1 (over z), tp: 4 (over y), sp: 8 (over x, core).
Axes of the slice: x: 4, y: 4, z: 1, core: 2. Of those that a mesh axis runs over, the one named last changes fastest.
The devices are a block of a 4x4x8 slice.
Arguments:
- x_in: bfloat16 [4096, 5120], P(('rep', 'sp'))
- positions: int32 [4096], P(('rep', 'sp'))
- segments: int32 [4096], P(('rep', 'sp'))
- gain_attn: float32 [5120], replicated
- w_q: bfloat16 [5120, 4096], P(None, 'tp')
- w_k: bfloat16 [5120, 1024], P(None, 'tp')
- w_v: bfloat16 [5120, 1024], P(None, 'tp')
- w_o: bfloat16 [4096, 5120], P('tp')
- gain_mlp: float32 [5120], replicated
- w_gate: bfloat16 [5120, 32768], P(None, 'tp')
- w_up: bfloat16 [5120, 32768], P(None, 'tp')
- w_down: bfloat16 [32768, 5120], P('tp')
Outputs:
- output 1: bfloat16 [4096, 5120], P(('rep', 'sp'))
- output 2: bfloat16 [4096, 32, 128], P('rep', ('tp', 'sp'))
- output 3: bfloat16 [4096, 32, 128], P('rep', ('tp', 'sp'))
All inputs are finite; a program needn't handle non-finite values.
Results may differ from the reference program's by a relative error of at most 0.00708525.
Values are sent between devices in bfloat16 or wider.
A program may use at most 768 MiB of HBM per device.

```python
import jax
import jax.numpy as jnp
from jax import lax

TOKENS = 4096
MODEL_DIM = 5120
FF_DIM = 32768
Q_HEADS = 32
KV_HEADS = 8
HEAD_DIM = 128
NUM_REQS = 2
KV_SLOTS = 32
ROPE_BASE = 500000
NORM_EPS = 1e-5


def draw_layout(layout_key):
    cut_key, step_key, start_key = jax.random.split(layout_key, 3)
    cut_rows = jnp.sort(jax.random.choice(cut_key, TOKENS - 1, (NUM_REQS - 1,), replace=False) + 1).astype(jnp.int32)
    tok_index = jnp.arange(TOKENS, dtype=jnp.int32)
    segments = jnp.sum(tok_index[:, None] >= cut_rows[None, :], axis=1).astype(jnp.int32)
    step_sizes = jax.random.randint(step_key, (TOKENS,), 1, 4, dtype=jnp.int32)
    run_sum = jnp.cumsum(step_sizes)
    first_rows = jnp.concatenate([jnp.zeros((1,), jnp.int32), cut_rows])
    seg_base = run_sum[first_rows] - step_sizes[first_rows]
    start_pos = jax.random.randint(start_key, (NUM_REQS,), 0, 1024, dtype=jnp.int32)
    positions = (run_sum - seg_base[segments] + start_pos[segments]).astype(jnp.int32)
    return positions, segments


def setup_inputs(seed: int = 0, part: int = 0) -> dict:
    base_key = jax.random.key(seed)
    part_key = jax.random.fold_in(base_key, part)
    x_key, layout_key = jax.random.split(part_key, 2)
    w_keys = jax.random.split(base_key, 10)
    positions, segments = draw_layout(layout_key)
    d_scale = MODEL_DIM ** -0.5

    def normal_weight(key_w, shape, std_dev):
        return (jax.random.normal(key_w, shape, jnp.float32) * std_dev).astype(jnp.bfloat16)

    return {
        "x_in": jax.random.normal(x_key, (TOKENS, MODEL_DIM), jnp.float32).astype(jnp.bfloat16),
        "positions": positions,
        "segments": segments,
        "gain_attn": 1.0 + 0.25 * jax.random.normal(w_keys[0], (MODEL_DIM,), jnp.float32),
        "w_q": normal_weight(w_keys[1], (MODEL_DIM, Q_HEADS * HEAD_DIM), 1.6 * d_scale),
        "w_k": normal_weight(w_keys[2], (MODEL_DIM, KV_HEADS * HEAD_DIM), 1.6 * d_scale),
        "w_v": normal_weight(w_keys[3], (MODEL_DIM, KV_HEADS * HEAD_DIM), d_scale),
        "w_o": normal_weight(w_keys[4], (Q_HEADS * HEAD_DIM, MODEL_DIM), (Q_HEADS * HEAD_DIM) ** -0.5),
        "gain_mlp": 1.0 + 0.25 * jax.random.normal(w_keys[5], (MODEL_DIM,), jnp.float32),
        "w_gate": normal_weight(w_keys[6], (MODEL_DIM, FF_DIM), d_scale),
        "w_up": normal_weight(w_keys[7], (MODEL_DIM, FF_DIM), d_scale),
        "w_down": normal_weight(w_keys[8], (FF_DIM, MODEL_DIM), FF_DIM ** -0.5),
    }


def rms_norm(x_f32, gain_vec):
    mean_sq = jnp.mean(x_f32 * x_f32, axis=-1, keepdims=True)
    return (x_f32 * lax.rsqrt(mean_sq + NORM_EPS) * gain_vec).astype(jnp.bfloat16)


def rope_tables(positions):
    half_dim = HEAD_DIM // 2
    inv_freq = jnp.power(jnp.float32(ROPE_BASE), -jnp.arange(half_dim, dtype=jnp.float32) * (2.0 / HEAD_DIM))
    angles = positions.astype(jnp.float32)[:, None] * inv_freq[None, :]
    return jnp.cos(angles)[:, None, :], jnp.sin(angles)[:, None, :]


def rotate(t_f32, cos_t, sin_t):
    half_dim = HEAD_DIM // 2
    t_lo = t_f32[..., :half_dim]
    t_hi = t_f32[..., half_dim:]
    return jnp.concatenate([t_lo * cos_t - t_hi * sin_t, t_hi * cos_t + t_lo * sin_t], axis=-1)


def reference(x_in, positions, segments, gain_attn, w_q, w_k, w_v, w_o, gain_mlp, w_gate, w_up, w_down):
    x_f32 = x_in.astype(jnp.float32)
    u_norm = rms_norm(x_f32, gain_attn)
    cos_t, sin_t = rope_tables(positions)
    q_rot = rotate(jnp.dot(u_norm, w_q, preferred_element_type=jnp.float32).reshape(TOKENS, Q_HEADS, HEAD_DIM), cos_t, sin_t).astype(jnp.bfloat16)
    k_rot = rotate(jnp.dot(u_norm, w_k, preferred_element_type=jnp.float32).reshape(TOKENS, KV_HEADS, HEAD_DIM), cos_t, sin_t).astype(jnp.bfloat16)
    v_proj = jnp.dot(u_norm, w_v, preferred_element_type=jnp.float32).astype(jnp.bfloat16).reshape(TOKENS, KV_HEADS, HEAD_DIM)
    group_size = Q_HEADS // KV_HEADS
    tok_index = jnp.arange(TOKENS)
    allowed = (tok_index[:, None] >= tok_index[None, :]) & (segments[:, None] == segments[None, :])
    score_scale = HEAD_DIM ** -0.5

    def one_head(operands):
        q_one, k_one, v_one = operands
        scores = jnp.dot(q_one, k_one.T, preferred_element_type=jnp.float32) * score_scale
        scores = jnp.where(allowed, scores, -1e30)
        prob_bf16 = jax.nn.softmax(scores, axis=-1).astype(jnp.bfloat16)
        return jnp.dot(prob_bf16, v_one, preferred_element_type=jnp.float32).astype(jnp.bfloat16)

    q_heads = jnp.transpose(q_rot, (1, 0, 2))
    k_heads = jnp.repeat(jnp.transpose(k_rot, (1, 0, 2)), group_size, axis=0)
    v_heads = jnp.repeat(jnp.transpose(v_proj, (1, 0, 2)), group_size, axis=0)
    attn_out = jnp.transpose(lax.map(one_head, (q_heads, k_heads, v_heads)), (1, 0, 2)).reshape(TOKENS, Q_HEADS * HEAD_DIM)
    x_mid = x_f32 + jnp.dot(attn_out, w_o, preferred_element_type=jnp.float32)
    u_mlp = rms_norm(x_mid, gain_mlp)
    gate_act = jnp.dot(u_mlp, w_gate, preferred_element_type=jnp.float32)
    up_act = jnp.dot(u_mlp, w_up, preferred_element_type=jnp.float32)
    hidden = (jax.nn.silu(gate_act) * up_act).astype(jnp.bfloat16)
    y_out = (x_mid + jnp.dot(hidden, w_down, preferred_element_type=jnp.float32)).astype(jnp.bfloat16)
    slot_repeat = KV_SLOTS // KV_HEADS
    return y_out, jnp.repeat(k_rot, slot_repeat, axis=1), jnp.repeat(v_proj, slot_repeat, axis=1)
```

```python
import functools

import jax
import jax.numpy as jnp
from jax import lax
from jax.experimental import pallas as pl
from jax.experimental.pallas import tpu as pltpu
from jax.sharding import PartitionSpec as P

HEAD_DIM = 128
ROPE_BASE = 500000.0
NORM_EPS = 1e-5
QUERY_ROWS = 512


def rms_norm(x_f32, gain_vec):
    mean_sq = jnp.mean(x_f32 * x_f32, axis=-1, keepdims=True)
    return (x_f32 * lax.rsqrt(mean_sq + NORM_EPS) * gain_vec).astype(jnp.bfloat16)


def rope_tables(positions):
    half_dim = HEAD_DIM // 2
    inv_freq = jnp.power(jnp.float32(ROPE_BASE), -jnp.arange(half_dim, dtype=jnp.float32) * (2.0 / HEAD_DIM))
    angles = positions.astype(jnp.float32)[..., None] * inv_freq
    return jnp.cos(angles)[..., None, :], jnp.sin(angles)[..., None, :]


def rotate(t_f32, cos_t, sin_t):
    half_dim = HEAD_DIM // 2
    t_lo = t_f32[..., :half_dim]
    t_hi = t_f32[..., half_dim:]
    return jnp.concatenate([t_lo * cos_t - t_hi * sin_t, t_hi * cos_t + t_lo * sin_t], axis=-1)


def project_qkv(x_f32, positions, gain_attn, w_q, w_k, w_v):
    row_count = x_f32.shape[0]
    u_norm = rms_norm(x_f32, gain_attn)
    cos_t, sin_t = rope_tables(positions)
    q_rot = rotate(jnp.dot(u_norm, w_q, preferred_element_type=jnp.float32).reshape(row_count, -1, HEAD_DIM), cos_t, sin_t).astype(jnp.bfloat16)
    k_rot = rotate(jnp.dot(u_norm, w_k, preferred_element_type=jnp.float32).reshape(row_count, -1, HEAD_DIM), cos_t, sin_t).astype(jnp.bfloat16)
    v_proj = jnp.dot(u_norm, w_v, preferred_element_type=jnp.float32).astype(jnp.bfloat16).reshape(row_count, -1, HEAD_DIM)
    return q_rot, k_rot, v_proj


def masked_attention(q_blk, key_rows, val_rows, q_index, k_index, q_seg, k_seg):
    scores = jnp.einsum("qhgc,shc->hgqs", q_blk, key_rows, preferred_element_type=jnp.float32) * (HEAD_DIM ** -0.5)
    allowed = (q_index[:, None] >= k_index[None, :]) & (q_seg[:, None] == k_seg[None, :])
    scores = jnp.where(allowed, scores, -1e30)
    row_max = jnp.max(scores, axis=-1, keepdims=True)
    weights = jnp.exp(scores - row_max)
    prob_bf16 = (weights / jnp.sum(weights, axis=-1, keepdims=True)).astype(jnp.bfloat16)
    return jnp.einsum("hgqs,shc->qhgc", prob_bf16, val_rows, preferred_element_type=jnp.float32).astype(jnp.bfloat16)


MESH = pl.DeviceIdType.MESH
BF16, F32 = jnp.bfloat16, jnp.float32
VMEM_BYTES = 63 * 2 ** 20


def mlp_kernel(chunks, cb, attn, wo, x_hbm, gain, wg, wu, wd, y_hbm,
               wbuf, hbuf, xmid, srow, sin, p_own, p_out, d_in, f_in, e_in, ystage, *rest):
    n_ch = len(chunks)
    u2 = rest[:n_ch]
    (wsem, asem, xsem, s_s, s_r, u1s, u1r, u2s, u2r, ups, upr,
     d_s, d_r, f_s, f_r, e_s, e_r, a_l, a_s, a_r, h_s, h_r) = rest[n_ch:]
    rows, dim = x_hbm.shape
    depth = attn.shape[1]
    tp = lax.axis_size("tp")
    col = dim // tp
    nb = col // cb
    ff = wg.shape[1] // 2
    y = lax.axis_index("tp")
    s = lax.axis_index("sp")
    core = s % 2
    pair = s + 1 - 2 * core
    yp, ym, y2 = (y + 1) % tp, (y + tp - 1) % tp, (y + 2) % tp
    here = {"tp": y, "sp": s}
    to_pair, to_p, to_m, to_2 = ({"tp": y, "sp": pair}, {"tp": yp, "sp": s}, {"tp": ym, "sp": s}, {"tp": y2, "sp": s})
    starts = [sum(chunks[:i]) for i in range(n_ch)]
    n_g, n_d = ff // cb, tp * nb // 2

    def remote(src, dst, ssem, rsem, to):
        return pltpu.make_async_remote_copy(src, dst, ssem, rsem, device_id=to, device_id_type=MESH)

    def cols(block, width=None):
        return pl.ds(pl.multiple_of(block * (width or cb), 128), width or cb)

    def w_o_tile(t, slot):
        width = min(2 * cb, col - t * 2 * cb)
        return [pltpu.make_async_copy(wo.at[:, pl.ds(t * 2 * cb, width)],
                                      wbuf.at[slot, pl.ds(0, depth), pl.ds(0, width)], wsem.at[slot, 0])]

    def g_tile(n, slot):
        c = pl.ds(pl.multiple_of(core * ff + n * cb, 128), cb)
        return [pltpu.make_async_copy(wg.at[:, c], wbuf.at[slot, :, pl.ds(0, cb)], wsem.at[slot, 0]),
                pltpu.make_async_copy(wu.at[:, c], wbuf.at[slot, :, pl.ds(cb, cb)], wsem.at[slot, 1])]

    def d_cols(m):
        q = m // nb
        d = (2 + 3 * q + 3 * (q * (q - 1) // 2)) % 4
        return pl.ds(pl.multiple_of(((y + d) % tp) * col + (m % nb) * cb, 128), cb)

    def d_tile(p, slot):
        r = pl.ds(pl.multiple_of(core * ff, 128), ff)
        return [pltpu.make_async_copy(wd.at[r, d_cols(2 * p + i)], wbuf.at[slot, pl.ds(0, ff), pl.ds(i * cb, cb)],
                                      wsem.at[slot, i]) for i in range(2)]

    def start(copies):
        for c in copies:
            c.start()

    def wait(copies):
        for c in copies:
            c.wait()

    n_o = -(-col // (2 * cb))
    a_copy = pltpu.make_async_copy(attn, hbuf.at[pl.ds(0, rows), pl.ds(0, depth)], asem)
    a_copy.start()
    x_copies = [pltpu.make_async_copy(x_hbm.at[pl.ds(r0, r), cols(y, col)], u2[i].at[pl.ds(0, r), cols(y, col)], xsem.at[i])
                for i, (r0, r) in enumerate(zip(starts, chunks))]
    start(w_o_tile(0, 0))
    start(w_o_tile(1, 1))
    start(x_copies)

    barrier = pltpu.get_barrier_semaphore()
    for to in (to_pair, to_p, to_m, to_2):
        pl.semaphore_signal(barrier, inc=1, device_id=to, device_id_type=MESH)
    pl.semaphore_wait(barrier, 4)

    a_copy.wait()
    wait(x_copies)
    for t in range(n_o):
        if t + 2 < n_o:
            start(w_o_tile(t + 2, (t + 2) % 3))
        else:
            start(g_tile(t + 2 - n_o, (t + 2) % 3))
        wait(w_o_tile(t, t % 3))
        width = min(2 * cb, col - t * 2 * cb)
        xmid[:, pl.ds(t * 2 * cb, width)] = jnp.dot(hbuf[pl.ds(0, rows), pl.ds(0, depth)],
                                                    wbuf[t % 3, pl.ds(0, depth), pl.ds(0, width)],
                                                    preferred_element_type=F32)
    sq = jnp.zeros((rows, 128), F32)
    for i, (r0, r) in enumerate(zip(starts, chunks)):
        xmid[pl.ds(r0, r), :] += u2[i][pl.ds(0, r), cols(y, col)].astype(F32)
    for b in range(col // 128):
        v = xmid[:, pl.ds(b * 128, 128)]
        sq += v * v
    tot = jnp.broadcast_to(jnp.sum(sq, axis=1, keepdims=True), (rows, 128)).T
    srow[...] = tot[:8, :]
    stat = [remote(srow, sin.at[i], s_s.at[i], s_r.at[i], to) for i, to in enumerate((to_p, to_m, to_2))]
    start(stat)
    wait(stat)
    tot = srow[...] + sin[0] + sin[1] + sin[2]
    inv = lax.rsqrt(tot * (1.0 / dim) + NORM_EPS)
    inv_col = jnp.broadcast_to(inv[:1, :], (128, rows)).T

    def norm_chunk(i):
        r0, r = starts[i], chunks[i]
        for b in range(col // 128):
            c = pl.ds(pl.multiple_of(y * col + b * 128, 128), 128)
            u2[i][pl.ds(0, r), c] = (xmid[pl.ds(r0, r), pl.ds(b * 128, 128)] * inv_col[r0:r0 + r, :]
                                     * gain[:, c]).astype(BF16)

    def blk(i, row0, n_rows, rank):
        return u2[i].at[pl.ds(row0, n_rows), cols(rank, col)]

    def u_first(i):
        r = chunks[i]
        return [remote(blk(i, 0, r, y), blk(i, 0, r, y), u1s.at[i, 0], u1r.at[i, 1], to_p),
                remote(blk(i, 0, r, y), blk(i, 0, r, y), u1s.at[i, 1], u1r.at[i, 0], to_m)]

    def u_pair(i, j):
        r, rank = chunks[i], (y, yp, ym, y2)[j]
        return remote(blk(i, 0, r, rank), blk(i, r, r, rank), ups.at[i, j], upr.at[i, j], to_pair)

    def u_second(i):
        h = chunks[i] // 2
        return [remote(blk(i, h, h, yp), blk(i, h, h, yp), u2s.at[i, 0], u2r.at[i, 0], to_m),
                remote(blk(i, 0, h, ym), blk(i, 0, h, ym), u2s.at[i, 1], u2r.at[i, 1], to_p)]

    def u_start(i):
        start(u_first(i))
        u_pair(i, 0).start()

    def u_mid(i):
        first, second = u_first(i), u_second(i)
        first[1].wait_recv()
        second[0].start()
        u_pair(i, 1).start()
        first[0].wait_recv()
        second[1].start()
        u_pair(i, 2).start()

    def u_last(i):
        for c in u_second(i):
            c.wait_recv()
        u_pair(i, 3).start()

    def u_ready(i):
        for j in range(4):
            u_pair(i, j).wait_recv()

    def u_drain(i):
        for c in u_first(i) + u_second(i) + [u_pair(i, j) for j in range(4)]:
            c.wait_send()

    def bi(d, k):
        return {2: 0, 1: 1, 3: 2, 0: 3}[d] * nb + k

    def d_copy(i, m):
        r, par = chunks[i], i % 2
        return remote(p_out.at[m % 4, pl.ds(0, r)], d_in.at[par, m, pl.ds(0, r)], d_s.at[m % 4], d_r.at[par, m], to_pair)

    def t_add(i, m):
        r, par = chunks[i], i % 2
        d_copy(i, m).wait_recv()
        p_own[m, pl.ds(0, r)] += d_in[par, m, pl.ds(0, r)]

    def f_copies(i, k):
        h, par = chunks[i] // 2, i % 2
        return [remote(p_own.at[k, pl.ds(0, h)], f_in.at[par, 0, k, pl.ds(0, h)], f_s.at[0, k], f_r.at[par, 0, k], to_m),
                remote(p_own.at[k, pl.ds(h, h)], f_in.at[par, 1, k, pl.ds(0, h)], f_s.at[1, k], f_r.at[par, 1, k], to_p)]

    def e_copies(i, k):
        r, par = chunks[i], i % 2
        return [remote(p_own.at[2 * nb + k, pl.ds(0, r)], e_in.at[par, 0, k, pl.ds(0, r)], e_s.at[0, k], e_r.at[par, 0, k], to_m),
                remote(p_own.at[nb + k, pl.ds(0, r)], e_in.at[par, 1, k, pl.ds(0, r)], e_s.at[1, k], e_r.at[par, 1, k], to_p)]

    def t_e(i, k, side):
        h, par = chunks[i] // 2, i % 2
        f_copies(i, k)[side].wait_recv()
        m, r0 = (2 * nb + k, 0) if side == 0 else (nb + k, h)
        p_own[m, pl.ds(r0, h)] += f_in[par, side, k, pl.ds(0, h)]
        e_copies(i, k)[side].start()

    def y_at(i, row0, n_rows, rank, k):
        return y_hbm.at[pl.ds(starts[i] + row0, n_rows), pl.ds(pl.multiple_of(rank * col + k * cb, 128), cb)]

    def a_copies(i, k):
        r, par = chunks[i], i % 2
        src = ystage.at[par, k, pl.ds(0, r)]
        return [remote(src, y_at(i, 0, r, y, k), a_s.at[par, 0, k], a_r.at[par, 1, k], to_p),
                remote(src, y_at(i, 0, r, y, k), a_s.at[par, 1, k], a_r.at[par, 0, k], to_m)]

    def a_local(i, k):
        r, par = chunks[i], i % 2
        return pltpu.make_async_copy(ystage.at[par, k, pl.ds(0, r)], y_at(i, 0, r, y, k), a_l.at[par, k])

    def h_copies(i, k):
        h, par = chunks[i] // 2, i % 2
        return [remote(y_at(i, h, h, yp, k), y_at(i, h, h, yp, k), h_s.at[par, 0, k], h_r.at[par, 0, k], to_m),
                remote(y_at(i, 0, h, ym, k), y_at(i, 0, h, ym, k), h_s.at[par, 1, k], h_r.at[par, 1, k], to_p)]

    def t_final(i, k):
        r, par = chunks[i], i % 2
        for c in e_copies(i, k):
            c.wait_recv()
        v = (p_own[3 * nb + k, pl.ds(0, r)] + e_in[par, 0, k, pl.ds(0, r)] + e_in[par, 1, k, pl.ds(0, r)]
             + xmid[pl.ds(starts[i], r), cols(k)])
        ystage[par, k, pl.ds(0, r)] = v.astype(BF16)
        start(a_copies(i, k))
        a_local(i, k).start()

    def t_fwd(i, k):
        first, second = a_copies(i, k), h_copies(i, k)
        first[1].wait_recv()
        second[0].start()
        first[0].wait_recv()
        second[1].start()

    def t_halves(i, k):
        for c in h_copies(i, k):
            c.wait_recv()

    def t_drain(i, k):
        for c in f_copies(i, k) + e_copies(i, k) + a_copies(i, k) + h_copies(i, k):
            c.wait_send()
        a_local(i, k).wait()

    norm_chunk(0)
    u_start(0)
    for i in range(1, n_ch):
        norm_chunk(i)
    u_mid(0)
    if n_ch > 1:
        u_start(1)
    u_last(0)
    u_ready(0)

    base = n_o
    for i in range(n_ch):
        r = chunks[i]
        g_base, d_base = base % 3, (base + n_g) % 3
        base += n_g + n_d

        @pl.loop(0, n_g)
        def _(n, i=i, r=r, g_base=g_base):
            nxt = (g_base + n + 2) % 3

            @pl.when(n + 2 < n_g)
            def _():
                start(g_tile(n + 2, nxt))

            @pl.when(n + 2 >= n_g)
            def _():
                start(d_tile(n + 2 - n_g, nxt))

            slot = (g_base + n) % 3
            wait(g_tile(n, slot))
            g = jnp.dot(u2[i][...], wbuf[slot], preferred_element_type=F32)
            hbuf[pl.ds(0, 2 * r), cols(n)] = (jax.nn.silu(g[:, :cb]) * g[:, cb:]).astype(BF16)

            if i == 0:
                for j in range(1, n_ch):
                    t0 = G_U[0] + (j - 1) * G_U[2]

                    @pl.when(n == t0)
                    def _(j=j):
                        u_mid(j)
                        if j + 1 < n_ch:
                            u_start(j + 1)

                    @pl.when(n == t0 + G_U[1])
                    def _(j=j):
                        u_last(j)
            else:
                for k in range(nb):
                    @pl.when(n == G_E[0] + G_E[1] * k)
                    def _(k=k):
                        t_final(i - 1, k)

                    @pl.when(n == G_F[0] + G_F[1] * k)
                    def _(k=k):
                        t_fwd(i - 1, k)

                @pl.when(n == n_g - 1)
                def _():
                    for k in range(nb):
                        t_halves(i - 1, k)
                    for k in range(nb):
                        t_drain(i - 1, k)

        @pl.loop(0, n_d)
        def _(p, i=i, r=r, d_base=d_base):
            nxt = (d_base + p + 2) % 3

            @pl.when(p + 2 < n_d)
            def _():
                start(d_tile(p + 2, nxt))

            if i + 1 < n_ch:
                @pl.when(p + 2 >= n_d)
                def _():
                    start(g_tile(p + 2 - n_d, nxt))

            slot = (d_base + p) % 3
            wait(d_tile(p, slot))
            v = jnp.dot(hbuf[pl.ds(0, 2 * r), :], wbuf[slot, pl.ds(0, ff)], preferred_element_type=F32)
            for q in range(2):
                m = 2 * p + q
                p_own[m, pl.ds(0, r)] = v[:r, q * cb:(q + 1) * cb]

                @pl.when(p >= 2)
                def _(m=m):
                    d_copy(i, m).wait_send()

                p_out[m % 4, pl.ds(0, r)] = v[r:, q * cb:(q + 1) * cb]
                d_copy(i, m).start()

            @pl.when(p >= 1)
            def _():
                for q in range(2):
                    t_add(i, 2 * p - 2 + q)

            for k in range(nb):
                @pl.when(p == (k // 2) + 1)
                def _(k=k):
                    start(f_copies(i, k))
            for k in range(nb):
                for side, at in ((1, D_E1[k]), (0, D_E0[k])):
                    if at < n_d:
                        @pl.when(p == at)
                        def _(k=k, side=side):
                            t_e(i, k, side)

        for q in range(2):
            t_add(i, 2 * n_d - 2 + q)
        for k in range(nb):
            for side, at in ((1, D_E1[k]), (0, D_E0[k])):
                if at >= n_d:
                    t_e(i, k, side)
        for q in range(4):
            d_copy(i, 2 * n_d - 4 + q).wait_send()
        if i + 1 < n_ch:
            u_ready(i + 1)

    last = n_ch - 1
    for k in range(nb):
        t_final(last, k)
        if k >= 2:
            t_fwd(last, k - 2)
    for k in range(nb - 2, nb):
        t_fwd(last, k)
    for k in range(nb):
        t_halves(last, k)
    for k in range(nb):
        t_drain(last, k)
    for i in range(n_ch):
        u_drain(i)


CHUNKS = (256, 256)
G_U = (5, 4, 8)
G_E = (2, 2)
G_F = (6, 2)
D_E1 = (4, 5, 6, 7, 8)
D_E0 = (6, 7, 8, 9, 10)


def mlp_call(attn, wo, x_in, gain, wg, wu, wd):
    rows, dim = x_in.shape
    tp = lax.axis_size("tp")
    col, cb = dim // tp, 256
    nb = col // cb
    ff = wg.shape[1] // 2
    chunks = CHUNKS
    n_ch, rm = len(chunks), max(chunks)
    hb = tp * nb
    dma = pltpu.SemaphoreType.DMA
    anyspec = pl.BlockSpec(memory_space=pl.ANY)
    scratch = [
        pltpu.VMEM((3, dim, 2 * cb), BF16), pltpu.VMEM((max(rows, 2 * rm), max(ff, attn.shape[1])), BF16),
        pltpu.VMEM((rows, col), F32), pltpu.VMEM((8, rows), F32), pltpu.VMEM((tp - 1, 8, rows), F32),
        pltpu.VMEM((hb, rm, cb), F32), pltpu.VMEM((4, rm, cb), F32), pltpu.VMEM((2, hb, rm, cb), F32),
        pltpu.VMEM((2, 2, nb, rm // 2, cb), F32), pltpu.VMEM((2, 2, nb, rm, cb), F32), pltpu.VMEM((2, nb, rm, cb), BF16),
        *[pltpu.VMEM((2 * r, dim), BF16) for r in chunks],
        dma((3, 2)), dma(()), dma((n_ch,)), dma((3,)), dma((3,)),
        dma((n_ch, 2)), dma((n_ch, 2)), dma((n_ch, 2)), dma((n_ch, 2)), dma((n_ch, 4)), dma((n_ch, 4)),
        dma((4,)), dma((2, hb)), dma((2, nb)), dma((2, 2, nb)), dma((2, nb)), dma((2, 2, nb)),
        dma((2, nb)), dma((2, 2, nb)), dma((2, 2, nb)), dma((2, 2, nb)), dma((2, 2, nb)),
    ]
    return pl.pallas_call(
        functools.partial(mlp_kernel, chunks, cb), name="mlp",
        out_shape=jax.ShapeDtypeStruct((rows, dim), BF16),
        in_specs=[anyspec, anyspec, anyspec, pl.BlockSpec(memory_space=pltpu.VMEM), anyspec, anyspec, anyspec],
        out_specs=anyspec, scratch_shapes=scratch,
        compiler_params=pltpu.CompilerParams(collective_id=1, has_side_effects=True, vmem_limit_bytes=VMEM_BYTES),
    )(attn, wo, x_in, gain.reshape(1, dim), wg, wu, wd)


def solution(mesh):
    sp_size = mesh.shape["sp"]
    row_spec = P(("rep", "sp"), None)
    tok_spec = P(("rep", "sp"))
    full_spec = P(None)
    col_spec = P(None, "tp")
    wrow_spec = P("tp", None)
    cache_spec = P("rep", ("tp", "sp"), None)

    def local_layer(x_in, positions, segments, gain_attn, w_q, w_k, w_v, w_o, gain_mlp, w_gate, w_up, w_down):
        rows_local = x_in.shape[0]
        tokens = rows_local * sp_size
        heads_local = w_q.shape[1] // HEAD_DIM
        kv_local = w_k.shape[1] // HEAD_DIM
        kv_repeat = max(1, sp_size // kv_local)
        heads_dev = heads_local // sp_size
        slots_dev = kv_local * kv_repeat // sp_size
        group_size = heads_dev // slots_dev
        x_f32 = x_in.astype(jnp.float32)
        q_rot, k_rot, v_proj = project_qkv(x_f32, positions, gain_attn, w_q, w_k, w_v)
        k_send = jnp.repeat(k_rot, kv_repeat, axis=1).reshape(rows_local, sp_size, slots_dev, HEAD_DIM)
        v_send = jnp.repeat(v_proj, kv_repeat, axis=1).reshape(rows_local, sp_size, slots_dev, HEAD_DIM)
        send_buf = jnp.concatenate([q_rot.reshape(rows_local, sp_size, heads_dev, HEAD_DIM), k_send, v_send], axis=2)
        recv_buf = lax.all_to_all(send_buf, "sp", 1, 0, tiled=True).reshape(tokens, heads_dev + 2 * slots_dev, HEAD_DIM)
        seg_all = lax.all_gather(segments, "sp", tiled=True)
        q_all = recv_buf[:, :heads_dev].reshape(tokens, slots_dev, group_size, HEAD_DIM)
        k_all = recv_buf[:, heads_dev:heads_dev + slots_dev]
        v_all = recv_buf[:, heads_dev + slots_dev:]
        tok_index = jnp.arange(tokens)
        block_rows = min(tokens, QUERY_ROWS)
        pieces = []
        for block_idx in range(tokens // block_rows):
            row_start = block_idx * block_rows
            row_stop = row_start + block_rows
            pieces.append(masked_attention(q_all[row_start:row_stop], k_all[:row_stop], v_all[:row_stop],
                                           tok_index[row_start:row_stop], tok_index[:row_stop],
                                           seg_all[row_start:row_stop], seg_all[:row_stop]))
        attn_heads = jnp.concatenate(pieces, axis=0).reshape(sp_size, rows_local, heads_dev, HEAD_DIM)
        attn_local = lax.all_to_all(attn_heads, "sp", 0, 2, tiled=True).reshape(rows_local, heads_local * HEAD_DIM)
        attn_full = lax.all_gather(attn_local, "tp", axis=1, tiled=True)
        wo_cols = lax.all_to_all(w_o, "tp", 1, 0, tiled=True)
        y_out = mlp_call(attn_full, wo_cols, x_in, gain_mlp, w_gate, w_up, w_down)
        return y_out, k_all, v_all

    return jax.shard_map(local_layer, mesh=mesh,
                         in_specs=(row_spec, tok_spec, tok_spec, full_spec, col_spec, col_spec, col_spec, wrow_spec,
                                   full_spec, col_spec, col_spec, wrow_spec),
                         out_specs=(row_spec, cache_spec, cache_spec), check_vma=False)
```

```python
import functools

import jax
import jax.numpy as jnp
from jax import lax
from jax.experimental import pallas as pl
from jax.experimental.pallas import tpu as pltpu
from jax.sharding import PartitionSpec as P

HEAD_DIM = 128
ROPE_BASE = 500000.0
NORM_EPS = 1e-5
MESH = pl.DeviceIdType.MESH
BF16, F32 = jnp.bfloat16, jnp.float32
VMEM_BYTES = 63 * 2 ** 20
NIL, ONE, TWO, THREE, FOUR, EIGHT, SUB, LANES = 0, 1, 2, 3, 4, 8, 8, 128


def remote(src, dst, send_sem, recv_sem, to):
    return pltpu.make_async_remote_copy(src, dst, send_sem, recv_sem, device_id=to, device_id_type=MESH)


def start(copies):
    for c in copies:
        c.start()


def wait(copies):
    for c in copies:
        c.wait()


def top(n):
    return pl.ds(NIL, n)


def aligned(offset, n):
    return pl.ds(pl.multiple_of(offset, LANES), n)


def rope_tables(positions):
    half_dim = HEAD_DIM // 2
    inv_freq = jnp.power(jnp.float32(ROPE_BASE), -jnp.arange(half_dim, dtype=jnp.float32) * (2.0 / HEAD_DIM))
    angles = positions.astype(jnp.float32)[..., None] * inv_freq
    return jnp.cos(angles)[..., None, :], jnp.sin(angles)[..., None, :]


def front_kernel(heads, x_hbm, seg_row, rope_c, rope_s, gain, wq, wk, wv, wo,
                 kc, vc, attn, wo_g,
                 xu, wbuf, qb, kvb, sgb, fq, fk, m_b, l_b, acc, ao,
                 xsem, wsem, sg_s, sg_r, k1s, k1r, k2s, k2r, kps, kpr, w1s, w1r, w2s, w2r, w3s, w3r, wps, wpr,
                 a_l, a_s, a_r, h_s, h_r, csem):
    rows, dim = x_hbm.shape
    tp, sp = lax.axis_size("tp"), lax.axis_size("sp")
    hd = HEAD_DIM
    n_kv = wk.shape[ONE] // hd
    group = heads // n_kv
    wide = heads * hd
    col, wrow = dim // tp, wo.shape[NIL] // sp
    half = wrow // TWO
    y, s = lax.axis_index("tp"), lax.axis_index("sp")
    core, chip, n_chip = s % TWO, s // TWO, sp // TWO
    yp, ym = (y + ONE) % tp, (y + tp - ONE) % tp
    chip_at = lambda d: (chip + d) % n_chip * TWO
    up, dn, far = (chip_at(d) + core for d in (ONE, n_chip - ONE, TWO))
    pair = s + ONE - TWO * core
    to_pair, to_up, to_dn = ({"tp": y, "sp": d} for d in (pair, up, dn))
    to_p, to_m = ({"tp": d, "sp": s} for d in (yp, ym))
    scale2 = HEAD_DIM ** -0.5 * 1.4426950408889634

    kw = n_kv * hd
    n_x = xsem.shape[NIL]
    x_rows = rows // n_x
    x_copies = [pltpu.make_async_copy(x_hbm.at[pl.ds(i * x_rows, x_rows)], xu.at[pl.ds(i * x_rows, x_rows)], xsem.at[i])
                for i in range(n_x)]
    start(x_copies)
    kv_copies = [pltpu.make_async_copy(w, wbuf.at[NIL, :, pl.ds(i * kw, kw)], wsem.at[NIL, i]) for i, w in enumerate((wk, wv))]
    q_copies = [pltpu.make_async_copy(wq.at[:, pl.ds(t * TWO * kw, TWO * kw)], wbuf.at[ONE + t], wsem.at[ONE + t, NIL])
                for t in range(TWO)]

    barrier = pltpu.get_barrier_semaphore()
    for j in range(ONE, sp):
        pl.semaphore_signal(barrier, inc=ONE, device_id={"tp": y, "sp": (s + j) % sp}, device_id_type=MESH)
    for j in range(ONE, tp):
        pl.semaphore_signal(barrier, inc=ONE, device_id={"tp": (y + j) % tp, "sp": s}, device_id_type=MESH)

    def norm(i):
        x_copies[i].wait()
        step = x_rows // TWO

        @pl.loop(NIL, TWO)
        def _(j):
            rr = pl.ds(pl.multiple_of(i * x_rows + j * step, step), step)
            sq = jnp.zeros((step, LANES), F32)
            for b in range(dim // LANES):
                v = xu[rr, pl.ds(b * LANES, LANES)].astype(F32)
                sq += v * v
            inv = lax.rsqrt(jnp.sum(sq, axis=ONE, keepdims=True) * (1.0 / dim) + NORM_EPS)
            for b in range(dim // LANES):
                c = pl.ds(b * LANES, LANES)
                xu[rr, c] = (xu[rr, c].astype(F32) * inv * gain[:, c]).astype(BF16)

    norm(NIL)
    start(kv_copies)
    norm(ONE)
    pl.semaphore_wait(barrier, sp + tp - TWO)

    def w1(j):
        rank, mine = (y + j) % tp, aligned(s * wrow, wrow)
        return remote(wo.at[mine, aligned(rank * col, col)], wo_g.at[tp - ONE - j, mine],
                      w1s.at[j - ONE], w1r.at[tp - ONE - j], {"tp": rank, "sp": s})

    def sg(j):
        return remote(seg_row, sgb.at[s], sg_s.at[j], sg_r.at[j], {"tp": y, "sp": (s + j) % sp})

    for j in range(ONE, sp):
        sg(j).start()
    for j in range(ONE, tp):
        w1(j).start()

    def w_blk(dev, r0, n):
        return wo_g.at[:, pl.ds(pl.multiple_of(dev * wrow + r0, half), n)]

    def w2(side):
        b = w_blk(s, NIL, wrow)
        return remote(b, b, w2s.at[side], w2r.at[ONE - side], (to_up, to_dn)[side])

    def w3(side):
        b = w_blk((up, dn)[side], (half, NIL)[side], half)
        return remote(b, b, w3s.at[side], w3r.at[side], (to_dn, to_up)[side])

    def wp(j):
        b = w_blk((s, up, dn, far)[j], NIL, wrow)
        return remote(b, b, wps.at[j], wpr.at[j], to_pair)

    start(q_copies)
    for i in range(TWO, n_x):
        norm(i)

    def rope(t):
        return (t * rope_c[...] + pltpu.roll(t, hd // TWO, ONE) * rope_s[...]).astype(BF16)

    wait(kv_copies)
    r = jnp.dot(xu[...], wbuf[NIL], preferred_element_type=F32)
    for g in range(n_kv):
        kvb[s, TWO * g] = rope(r[:, g * hd:(g + ONE) * hd])
        kvb[s, TWO * g + ONE] = r[:, kw + g * hd:kw + (g + ONE) * hd].astype(BF16)

    def k_blk(dev, g, lo=NIL, n=TWO):
        return kvb.at[dev, pl.ds(TWO * g + lo, n)]

    def k1(g, side):
        b = k_blk(s, g)
        return remote(b, b, k1s.at[g, side], k1r.at[g, ONE - side], (to_up, to_dn)[side])

    def k2(g, side):
        b = k_blk((up, dn)[side], g, ONE - side, ONE)
        return remote(b, b, k2s.at[g, side], k2r.at[g, side], (to_dn, to_up)[side])

    def kp(g, j):
        b = k_blk((s, up, dn, far)[j], g)
        return remote(b, b, kps.at[g, j], kpr.at[g, j], to_pair)

    def k_start(g):
        k1(g, NIL).start()
        k1(g, ONE).start()
        kp(g, NIL).start()

    def k_mid(g):
        for side in range(TWO):
            k1(g, ONE - side).wait_recv()
            k2(g, side).start()
            kp(g, ONE + side).start()

    def k_last(g):
        k2(g, NIL).wait_recv()
        k2(g, ONE).wait_recv()
        kp(g, THREE).start()

    k_start(NIL)

    for t in range(TWO):
        q_copies[t].wait()
        r = jnp.dot(xu[...], wbuf[ONE + t], preferred_element_type=F32)
        for g in range(heads // TWO):
            qb[t * (heads // TWO) + g] = rope(r[:, g * hd:(g + ONE) * hd])

    for j in range(ONE, sp):
        sg(j).wait_recv()
    sgb[s] = seg_row[...]
    lane = lax.broadcasted_iota(jnp.int32, (rows, LANES), ONE).astype(F32)

    def seg_col(dev):
        return jnp.broadcast_to(sgb[dev, top(ONE), :], (LANES, rows)).T

    fq[...] = jnp.where(seg_col(s) == lane, 1.0, 0.0).astype(BF16)

    @pl.loop(NIL, sp)
    def _(b):
        fk[b] = jnp.where(seg_col(b) == lane, 0.0, -1e30).astype(BF16)

    def attend(h, g, b0, nb, own):
        nk = nb * rows
        q = jnp.concatenate([qb[h], fq[...]], axis=ONE)
        k = jnp.concatenate([kvb[pl.ds(b0, nb), TWO * g].reshape(nk, hd), fk[pl.ds(b0, nb)].reshape(nk, LANES)], axis=ONE)
        v = kvb[pl.ds(b0, nb), TWO * g + ONE].reshape(nk, hd)
        sc = lax.dot_general(q, k, (((ONE,), (ONE,)), ((), ())), preferred_element_type=F32)
        if own:
            lo = nk - rows
            i, j = (lax.broadcasted_iota(jnp.int32, (rows, rows), d) for d in range(TWO))
            tail = jnp.where(i >= j, sc[:, lo:], -1e30)
            sc = jnp.concatenate([sc[:, :lo], tail], axis=ONE) if lo else tail
        mx = jnp.max(sc, axis=ONE, keepdims=True)
        if own:
            mn = jnp.broadcast_to(mx, (rows, LANES))
        else:
            mn = jnp.maximum(m_b[h], mx)
            al = jnp.exp2((m_b[h] - mn) * scale2)
        ps = [jnp.exp2((sc[:, j * LANES:(j + ONE) * LANES] - mn) * scale2) for j in range(nk // LANES)]
        ls = functools.reduce(jnp.add, ps)
        o = jnp.dot(jnp.concatenate([p.astype(BF16) for p in ps], axis=ONE), v, preferred_element_type=F32)
        m_b[h] = mn
        if own:
            l_b[h], acc[h] = ls, o
        else:
            l_b[h] = l_b[h] * al + ls
            acc[h] = acc[h] * al + o

    def a_at(rank, h, r0, n):
        return attn.at[pl.ds(r0, n), aligned(rank * wide + h * hd, hd)]

    def a1(h, side):
        return remote(ao.at[h], a_at(y, h, NIL, rows), a_s.at[side, h], a_r.at[ONE - side, h], (to_p, to_m)[side])

    def a2(h, side):
        b = a_at((yp, ym)[side], h, (rows // TWO, NIL)[side], rows // TWO)
        return remote(b, b, h_s.at[side, h], h_r.at[side, h], (to_m, to_p)[side])

    def a_own(h):
        return pltpu.make_async_copy(ao.at[h], a_at(y, h, NIL, rows), a_l.at[h])

    def pass_on(h):
        for side in range(TWO):
            a1(h, ONE - side).wait_recv()
            a2(h, side).start()

    @pl.loop(NIL, n_kv)
    def _(g):
        @pl.when(g == NIL)
        def _():
            k_mid(NIL)
            k_start(ONE)

        kp(g, NIL).wait_recv()

        @pl.loop(NIL, group)
        def _(i):
            @pl.when(core == NIL)
            def _():
                attend(g * group + i, g, s, ONE, True)

            @pl.when(core == ONE)
            def _():
                attend(g * group + i, g, chip_at(NIL), TWO, True)

        k_last(g)
        for j in range(ONE, FOUR):
            kp(g, j).wait_recv()

        @pl.loop(NIL, group)
        def _(i):
            h = g * group + i

            @pl.when(chip >= ONE)
            def _():
                attend(h, g, chip_at(n_chip - ONE), TWO, False)

            @pl.when(chip == n_chip - ONE)
            def _():
                attend(h, g, chip_at(ONE), TWO, False)

            @pl.when(chip >= TWO)
            def _():
                attend(h, g, chip_at(TWO), TWO, False)

            ao[h] = (acc[h] / jnp.sum(l_b[h], axis=ONE, keepdims=True)).astype(BF16)
            a1(h, NIL).start()
            a1(h, ONE).start()
            a_own(h).start()

            @pl.when(h == ONE)
            def _():
                k_mid(ONE)
                for j in range(ONE, tp):
                    w1(j).wait_recv()
                w2(NIL).start()
                w2(ONE).start()
                wp(NIL).start()

            @pl.when(h >= TWO)
            def _():
                pass_on(h - TWO)

    mine_kv = s // (sp // n_kv)
    caches = [pltpu.make_async_copy(kvb.at[:, TWO * mine_kv + i], c, csem.at[i]) for i, c in enumerate((kc, vc))]
    start(caches)
    pass_on(heads - TWO)
    for side in range(TWO):
        w2(ONE - side).wait_recv()
        w3(side).start()
        wp(ONE + side).start()
    pass_on(heads - ONE)
    w3(NIL).wait_recv()
    w3(ONE).wait_recv()
    wp(THREE).start()

    @pl.loop(NIL, heads)
    def _(h):
        for side in range(TWO):
            a2(h, side).wait_recv()
            a1(h, side).wait_send()
            a2(h, side).wait_send()
        a_own(h).wait()

    for j in range(FOUR):
        wp(j).wait_recv()
        wp(j).wait_send()
        for g in range(n_kv):
            kp(g, j).wait_send()
    for side in range(TWO):
        w2(side).wait_send()
        w3(side).wait_send()
        for g in range(n_kv):
            k1(g, side).wait_send()
            k2(g, side).wait_send()
    for j in range(ONE, tp):
        w1(j).wait_send()
    for j in range(ONE, sp):
        sg(j).wait_send()
    wait(caches)


def front_call(x_in, positions, segments, gain, wq, wk, wv, wo):
    rows, dim = x_in.shape
    tp, sp = lax.axis_size("tp"), lax.axis_size("sp")
    heads, n_kv = wq.shape[ONE] // HEAD_DIM, wk.shape[ONE] // HEAD_DIM
    cos_t, sin_t = (t[:, NIL] for t in rope_tables(positions))
    rope_c = jnp.concatenate([cos_t, cos_t], axis=ONE)
    rope_s = jnp.concatenate([-sin_t, sin_t], axis=ONE)
    seg_row = jnp.broadcast_to(segments.astype(F32), (SUB, rows))
    dma = pltpu.SemaphoreType.DMA
    hbm, vmem = pl.BlockSpec(memory_space=pl.ANY), pl.BlockSpec(memory_space=pltpu.VMEM)
    kv_shape = jax.ShapeDtypeStruct((sp, rows, HEAD_DIM), BF16)
    per_head, stat = (heads, rows, HEAD_DIM), ((heads, rows, LANES), F32)
    bufs = [((rows, dim), BF16), ((THREE, dim, TWO * n_kv * HEAD_DIM), BF16), (per_head, BF16),
            ((sp, TWO * n_kv, rows, HEAD_DIM), BF16), ((sp, SUB, rows), F32), ((rows, LANES), BF16), ((sp, rows, LANES), BF16),
            stat, stat, stat, (per_head, BF16)]
    sems = [(FOUR,), (THREE, TWO), (sp,), (sp,)] + [(n_kv, TWO)] * FOUR + [(n_kv, FOUR)] * TWO + [(tp - ONE,)] * TWO
    sems += [(TWO,)] * FOUR + [(FOUR,)] * TWO + [(heads,)] + [(TWO, heads)] * FOUR + [(TWO,)]
    return pl.pallas_call(
        functools.partial(front_kernel, heads), name="front",
        out_shape=[kv_shape, kv_shape, jax.ShapeDtypeStruct((rows, tp * heads * HEAD_DIM), BF16),
                   jax.ShapeDtypeStruct((tp - ONE, wo.shape[NIL], dim // tp), BF16)],
        in_specs=[hbm] + [vmem] * FOUR + [hbm] * FOUR, out_specs=[hbm] * FOUR,
        scratch_shapes=[pltpu.VMEM(*b) for b in bufs] + [dma(q) for q in sems],
        compiler_params=pltpu.CompilerParams(collective_id=TWO, has_side_effects=True, vmem_limit_bytes=VMEM_BYTES),
    )(x_in, seg_row, rope_c, rope_s, gain.reshape(ONE, dim), wq, wk, wv, wo)


def mlp_kernel(chunks, cb, plan, attn, wo, wo_g, x_hbm, gain, wg, wu, wd, y_hbm,
               wbuf, hbuf, xmid, srow, sin, p_own, p_out, d_in, f_in, e_in, ystage, *rest):
    n_ch = len(chunks)
    u2 = rest[:n_ch]
    (wsem, asem, xsem, s_s, s_r, u1s, u1r, u2s, u2r, ups, upr,
     d_s, d_r, f_s, f_r, e_s, e_r, a_l, a_s, a_r, h_s, h_r) = rest[n_ch:]
    rows, dim = x_hbm.shape
    depth = attn.shape[ONE]
    tp = lax.axis_size("tp")
    col = dim // tp
    nb = col // cb
    wide = TWO * cb
    ff = wg.shape[ONE] // TWO
    slots = wbuf.shape[NIL]
    y, s = lax.axis_index("tp"), lax.axis_index("sp")
    core = s % TWO
    pair = s + ONE - TWO * core
    yp, ym, y2 = (y + ONE) % tp, (y + tp - ONE) % tp, (y + TWO) % tp
    to_pair, to_p, to_m, to_2 = ({"tp": y, "sp": pair}, {"tp": yp, "sp": s}, {"tp": ym, "sp": s}, {"tp": y2, "sp": s})
    starts = [sum(chunks[:i]) for i in range(n_ch)]
    n_g, n_d = ff // wide, nb * tp // FOUR

    def cols(block, width):
        return aligned(block * width, width)

    n_o = -(-col // wide)
    part = depth // tp

    def o_width(t):
        return min(wide, col - t * wide)

    def o_tile(t):
        w = o_width(t)
        srcs = [wo.at[:, aligned(y * col + t * wide, w)]] + [wo_g.at[j, :, pl.ds(t * wide, w)] for j in range(tp - ONE)]
        return [pltpu.make_async_copy(src, wbuf.at[t, aligned((y + j) % tp * part, part), top(w)], wsem.at[t, j])
                for j, src in enumerate(srcs)]

    def g_tile(n, slot):
        c = aligned(core * ff + n * cb, cb)
        return [pltpu.make_async_copy(w.at[:, c], wbuf.at[slot, :, pl.ds(i * cb, cb)], wsem.at[slot, i])
                for i, w in enumerate((wg, wu))]

    def d_cols(m):
        q = m // nb
        d = (TWO + THREE * q + THREE * (q * (q - ONE) // TWO)) % FOUR
        return aligned((y + d) % tp * col + m % nb * cb, cb)

    def d_tile(p, slot):
        return [pltpu.make_async_copy(wd.at[aligned(core * ff, ff), d_cols(TWO * p + i)],
                                      wbuf.at[slot, top(ff), pl.ds(i * cb, cb)], wsem.at[slot, i]) for i in range(TWO)]

    def two(tile, j, base):
        return [c for i in range(TWO) for c in tile(TWO * j + i, (base + TWO * j + i) % slots)]

    a_copy = pltpu.make_async_copy(attn, hbuf.at[top(rows), top(depth)], asem)
    x_copies = [pltpu.make_async_copy(x_hbm.at[pl.ds(r0, r), cols(y, col)], u2[i].at[top(r), cols(y, col)], xsem.at[i])
                for i, (r0, r) in enumerate(zip(starts, chunks))]
    a_copy.start()
    for t in range(n_o):
        start(o_tile(t))
        if not t:
            start(x_copies)
    base = n_o
    start(g_tile(NIL, base))

    barrier = pltpu.get_barrier_semaphore()
    for to in (to_pair, to_p, to_m, to_2):
        pl.semaphore_signal(barrier, inc=ONE, device_id=to, device_id_type=MESH)
    pl.semaphore_wait(barrier, FOUR)

    step = rows // TWO

    def stat(j, i):
        to = (to_p, to_m, to_2)[i]
        return remote(srow.at[j], sin.at[j, i], s_s.at[j, i], s_r.at[j, i], to)

    a_copy.wait()
    wait(x_copies)
    for j in range(TWO):
        for t in range(n_o):
            w = o_width(t)
            if not j:
                wait(o_tile(t))
            xmid[pl.ds(j * step, step), pl.ds(t * wide, w)] = jnp.dot(
                hbuf[pl.ds(j * step, step), top(depth)], wbuf[t, top(depth), top(w)], preferred_element_type=F32)
            if j and not t:
                start(g_tile(ONE, NIL))
        for i, (r0, r) in enumerate(zip(starts, chunks)):
            lo, hi = max(r0, j * step), min(r0 + r, j * step + step)
            if lo < hi:
                xmid[pl.ds(lo, hi - lo), :] += u2[i][pl.ds(lo - r0, hi - lo), cols(y, col)].astype(F32)
        sq = jnp.zeros((step, LANES), F32)
        for b in range(col // LANES):
            v = xmid[pl.ds(j * step, step), pl.ds(b * LANES, LANES)]
            sq += v * v
        srow[j] = jnp.broadcast_to(jnp.sum(sq, axis=ONE, keepdims=True), (step, LANES)).T[:SUB, :]
        for i in range(tp - ONE):
            stat(j, i).start()

    def inverse(j):
        for i in range(tp - ONE):
            stat(j, i).wait()
        tot = srow[j]
        for i in range(tp - ONE):
            tot += sin[j, i]
        inv = lax.rsqrt(tot * (1.0 / dim) + NORM_EPS)
        return jnp.broadcast_to(inv[:ONE, :], (LANES, step)).T

    def norm_rows(j, inv_col):
        for i, (r0, r) in enumerate(zip(starts, chunks)):
            lo, hi = max(r0, j * step), min(r0 + r, j * step + step)
            if lo < hi:
                for b in range(col // LANES):
                    c = aligned(y * col + b * LANES, LANES)
                    u2[i][pl.ds(lo - r0, hi - lo), c] = (xmid[pl.ds(lo, hi - lo), pl.ds(b * LANES, LANES)]
                                                         * inv_col[lo - j * step:hi - j * step, :] * gain[:, c]).astype(BF16)

    def u_blk(i, row0, n_rows, rank):
        return u2[i].at[pl.ds(row0, n_rows), cols(rank, col)]

    def u_first(i, side):
        b = u_blk(i, NIL, chunks[i], y)
        return remote(b, b, u1s.at[i, side], u1r.at[i, ONE - side], (to_p, to_m)[side])

    def u_second(i, side):
        h = chunks[i] // TWO
        b = u_blk(i, h, h, yp) if side == NIL else u_blk(i, NIL, h, ym)
        return remote(b, b, u2s.at[i, side], u2r.at[i, side], (to_m, to_p)[side])

    def u_pair(i, j):
        r, rank = chunks[i], (y, yp, ym, y2)[j]
        return remote(u_blk(i, NIL, r, rank), u_blk(i, r, r, rank), ups.at[i, j], upr.at[i, j], to_pair)

    def u_start(i):
        u_first(i, NIL).start()
        u_first(i, ONE).start()
        u_pair(i, NIL).start()

    def u_mid(i):
        for side in range(TWO):
            u_first(i, ONE - side).wait_recv()
            u_second(i, side).start()
            u_pair(i, ONE + side).start()

    def u_last(i):
        for side in range(TWO):
            u_second(i, side).wait_recv()
        u_pair(i, THREE).start()

    def u_ready(i):
        for j in range(FOUR):
            u_pair(i, j).wait_recv()

    def u_drain(i):
        for side in range(TWO):
            u_first(i, side).wait_send()
            u_second(i, side).wait_send()
        for j in range(FOUR):
            u_pair(i, j).wait_send()

    def d_copy(i, m, slot):
        r, par = chunks[i], i % TWO
        return remote(p_out.at[slot, top(r)], d_in.at[par, m, top(r)], d_s.at[slot], d_r.at[par, m], to_pair)

    def t_add(i, m):
        r, par = chunks[i], i % TWO
        d_copy(i, m, NIL).wait_recv()
        p_own[m, top(r)] += d_in[par, m, top(r)]

    def f_copy(i, k, side):
        h, par = chunks[i] // TWO, i % TWO
        return remote(p_own.at[k, pl.ds(side * h, h)], f_in.at[par, side, k, top(h)],
                      f_s.at[side, k], f_r.at[par, side, k], (to_m, to_p)[side])

    def t_f(i, k):
        f_copy(i, k, NIL).start()
        f_copy(i, k, ONE).start()

    def e_copy(i, k, side):
        r, par = chunks[i], i % TWO
        return remote(p_own.at[(TWO - side) * nb + k, top(r)], e_in.at[par, side, k, top(r)],
                      e_s.at[side, k], e_r.at[par, side, k], (to_m, to_p)[side])

    def t_e(i, k, side):
        h, par = chunks[i] // TWO, i % TWO
        f_copy(i, k, side).wait_recv()
        p_own[(TWO - side) * nb + k, pl.ds(side * h, h)] += f_in[par, side, k, top(h)]
        e_copy(i, k, side).start()

    def y_at(i, row0, n_rows, rank, k):
        return y_hbm.at[pl.ds(starts[i] + row0, n_rows), aligned(rank * col + k * cb, cb)]

    def a_copy_y(i, k, side):
        r, par = chunks[i], i % TWO
        return remote(ystage.at[par, k, top(r)], y_at(i, NIL, r, y, k), a_s.at[par, side, k], a_r.at[par, ONE - side, k],
                      (to_p, to_m)[side])

    def a_local(i, k):
        r, par = chunks[i], i % TWO
        return pltpu.make_async_copy(ystage.at[par, k, top(r)], y_at(i, NIL, r, y, k), a_l.at[par, k])

    def h_copy(i, k, side):
        h = chunks[i] // TWO
        b = y_at(i, h, h, yp, k) if side == NIL else y_at(i, NIL, h, ym, k)
        return remote(b, b, h_s.at[i, side, k], h_r.at[i, side, k], (to_m, to_p)[side])

    def t_final(i, k):
        r, par = chunks[i], i % TWO
        for side in range(TWO):
            e_copy(i, k, side).wait_recv()
        v = (p_own[THREE * nb + k, top(r)] + e_in[par, NIL, k, top(r)] + e_in[par, ONE, k, top(r)]
             + xmid[pl.ds(starts[i], r), pl.ds(k * cb, cb)])
        ystage[par, k, top(r)] = v.astype(BF16)
        for side in range(TWO):
            a_copy_y(i, k, side).start()
        a_local(i, k).start()

    def t_fwd(i, k):
        for side in range(TWO):
            a_copy_y(i, k, ONE - side).wait_recv()
            h_copy(i, k, side).start()

    def sums_sent(i):
        for k in range(nb):
            for side in range(TWO):
                f_copy(i, k, side).wait_send()
                e_copy(i, k, side).wait_send()

    def rows_done(i):
        for k in range(nb):
            for side in range(TWO):
                h_copy(i, k, side).wait_recv()
                h_copy(i, k, side).wait_send()
                a_copy_y(i, k, side).wait_send()
            a_local(i, k).wait()

    norm_rows(NIL, inverse(NIL))
    u_start(NIL)
    norm_rows(ONE, inverse(ONE))
    u_mid(NIL)
    u_start(ONE)
    u_last(NIL)
    u_ready(NIL)

    tasks = {"mid": u_mid, "last": u_last, "start": u_start, "e": t_e, "final": t_final, "fwd": t_fwd}

    def run(todo, at):
        for when, name, *args in todo:
            @pl.when(at == when)
            def _():
                tasks[name](*args)

    for i in range(n_ch):
        r = chunks[i]
        g_base, d_base = base % slots, (base + TWO * n_g) % slots
        base += TWO * (n_g + n_d)

        @pl.loop(NIL, n_g)
        def _(j):
            @pl.when(j + ONE < n_g)
            def _():
                start(two(g_tile, j + ONE, g_base))

            @pl.when(j + ONE >= n_g)
            def _():
                start(two(d_tile, NIL, d_base))

            wait(two(g_tile, j, g_base))
            for q in range(TWO):
                n = TWO * j + q
                g = jnp.dot(u2[i][...], wbuf[(g_base + n) % slots], preferred_element_type=F32)
                hbuf[top(TWO * r), aligned(n * cb, cb)] = (jax.nn.silu(g[:, :cb]) * g[:, cb:]).astype(BF16)
            run(plan[i][NIL], j)

        if i:
            sums_sent(i - ONE)

        @pl.loop(NIL, n_d)
        def _(p):
            @pl.when(p + ONE < n_d)
            def _():
                start(two(d_tile, p + ONE, d_base))

            if i + ONE < n_ch:
                @pl.when(p + ONE >= n_d)
                def _():
                    start(two(g_tile, NIL, base % slots))

            wait(two(d_tile, p, d_base))
            out = p % TWO * FOUR

            @pl.when(p >= TWO)
            def _():
                for q in range(FOUR):
                    d_copy(i, q, out + q).wait_send()

            for q in range(TWO):
                v = jnp.dot(hbuf[top(TWO * r), top(ff)], wbuf[(d_base + TWO * p + q) % slots, top(ff)],
                            preferred_element_type=F32)
                for e in range(TWO):
                    b = TWO * q + e
                    p_own[FOUR * p + b, top(r)] = v[:r, e * cb:(e + ONE) * cb]
                    p_out[out + b, top(r)] = v[r:, e * cb:(e + ONE) * cb]
            for q in range(FOUR):
                d_copy(i, FOUR * p + q, out + q).start()

            @pl.when(p >= ONE)
            def _():
                for q in range(FOUR):
                    t_add(i, FOUR * (p - ONE) + q)

            @pl.when(p == ONE)
            def _():
                for k in range(FOUR):
                    t_f(i, k)

            @pl.when(p == TWO)
            def _():
                for k in range(FOUR, nb):
                    t_f(i, k)
            run(plan[i][ONE], p)

        for q in range(FOUR):
            t_add(i, FOUR * (n_d - ONE) + q)
        for q in range(FOUR):
            for out in range(TWO):
                d_copy(i, q, FOUR * out + q).wait_send()
        for name, *args in plan[i][TWO]:
            tasks[name](*args)
        if i + ONE < n_ch:
            u_ready(i + ONE)

    last = n_ch - ONE
    if last >= TWO:
        rows_done(last - TWO)
    for k in range(nb):
        t_final(last, k)
        if k >= TWO:
            t_fwd(last, k - TWO)
    for k in range(nb - TWO, nb):
        t_fwd(last, k)
    for i in range(max(last - ONE, NIL), n_ch):
        rows_done(i)
    sums_sent(last)
    for i in range(n_ch):
        u_drain(i)


CHUNKS = (192, 192, 128)


def mlp_plan():
    early = lambda i: [(3, "e", i, 0, 1), (3, "e", i, 1, 1), (4, "e", i, 2, 1), (4, "e", i, 0, 0), (4, "e", i, 1, 0)]
    late = lambda i: [("e", i, 3, 1), ("e", i, 2, 0), ("e", i, 4, 1), ("e", i, 3, 0), ("e", i, 4, 0)]
    at_start = lambda i: [(0, *t) for t in late(i)]
    finals = lambda i, at: [(a, "final", i, k) for k, a in enumerate(at)]
    passed = lambda i, at: [(a, "fwd", i, k) for k, a in enumerate(at)]
    gather = [(1, "mid", 1), (1, "start", 2), (3, "last", 1), (4, "mid", 2), (6, "last", 2)]
    return ((gather, early(0), ()),
            (at_start(0) + finals(0, (1, 2, 3, 4, 5)) + passed(0, (5, 6, 6, 6, 7)), early(1), ()),
            (at_start(1) + finals(1, (2, 3, 4, 6, 7)), passed(1, (0, 1, 1, 2, 2)) + early(2), late(2)))


def mlp_call(attn, wo, wo_g, x_in, gain, wg, wu, wd):
    rows, dim = x_in.shape
    tp = lax.axis_size("tp")
    cb = TWO * LANES
    nb = dim // tp // cb
    col, ff = nb * cb, wg.shape[ONE] // TWO
    n_ch, rm = len(CHUNKS), max(CHUNKS)
    dma = pltpu.SemaphoreType.DMA
    two_two, par_two = [(n_ch, TWO)] * FOUR + [(n_ch, FOUR)] * TWO, (TWO, TWO, nb)
    sems = [(FOUR, tp), (), (n_ch,), (TWO, tp - ONE), (TWO, tp - ONE), *two_two, (EIGHT,), (TWO, tp * nb),
            (TWO, nb), par_two, (TWO, nb), par_two, (TWO, nb), par_two, par_two, (n_ch, TWO, nb), (n_ch, TWO, nb)]
    bufs = [((FOUR, dim, TWO * cb), BF16), ((max(rows, TWO * rm), max(ff, attn.shape[ONE])), BF16), ((rows, col), F32),
            ((TWO, SUB, rows // TWO), F32), ((TWO, tp - ONE, SUB, rows // TWO), F32), ((tp * nb, rm, cb), F32),
            ((EIGHT, rm, cb), F32), ((TWO, tp * nb, rm, cb), F32), ((TWO, TWO, nb, rm // TWO, cb), F32),
            ((TWO, TWO, nb, rm, cb), F32), ((TWO, nb, rm, cb), BF16), *[((TWO * r, dim), BF16) for r in CHUNKS]]
    hbm = pl.BlockSpec(memory_space=pl.ANY)
    return pl.pallas_call(
        functools.partial(mlp_kernel, CHUNKS, cb, mlp_plan()), name="mlp",
        out_shape=jax.ShapeDtypeStruct((rows, dim), BF16),
        in_specs=[hbm, hbm, hbm, hbm, pl.BlockSpec(memory_space=pltpu.VMEM), hbm, hbm, hbm], out_specs=hbm,
        scratch_shapes=[pltpu.VMEM(*b) for b in bufs] + [dma(q) for q in sems],
        compiler_params=pltpu.CompilerParams(collective_id=ONE, has_side_effects=True, vmem_limit_bytes=VMEM_BYTES),
    )(attn, wo, wo_g, x_in, gain.reshape(ONE, dim), wg, wu, wd)


def solution(mesh):
    row_spec = P(("rep", "sp"), None)
    tok_spec = P(("rep", "sp"))
    full_spec = P(None)
    col_spec = P(None, "tp")
    wrow_spec = P("tp", None)
    cache_spec = P("rep", ("tp", "sp"), None)

    def local_layer(x_in, positions, segments, gain_attn, w_q, w_k, w_v, w_o, gain_mlp, w_gate, w_up, w_down):
        kc, vc, attn, wo_g = front_call(x_in, positions, segments, gain_attn, w_q, w_k, w_v, w_o)
        y_out = mlp_call(attn, w_o, wo_g, x_in, gain_mlp, w_gate, w_up, w_down)
        return y_out, kc.reshape(-1, 1, HEAD_DIM), vc.reshape(-1, 1, HEAD_DIM)

    return jax.shard_map(local_layer, mesh=mesh,
                         in_specs=(row_spec, tok_spec, tok_spec, full_spec, col_spec, col_spec, col_spec, wrow_spec,
                                   full_spec, col_spec, col_spec, wrow_spec),
                         out_specs=(row_spec, cache_spec, cache_spec), check_vma=False)
```

```python
import functools

import jax
import jax.numpy as jnp
from jax import lax
from jax.experimental import pallas as pl
from jax.experimental.pallas import tpu as pltpu
from jax.sharding import PartitionSpec as P

HEAD_DIM = 128
ROPE_BASE = 500000.0
NORM_EPS = 1e-5
MESH = pl.DeviceIdType.MESH
BF16, F32 = jnp.bfloat16, jnp.float32
VMEM_BYTES = 67043328
NIL, ONE, TWO, THREE, FOUR, EIGHT, SUB, LANES = 0, 1, 2, 3, 4, 8, 8, 128


def remote(src, dst, send_sem, recv_sem, to):
    return pltpu.make_async_remote_copy(src, dst, send_sem, recv_sem, device_id=to, device_id_type=MESH)


def start(copies):
    for c in copies:
        c.start()


def wait(copies):
    for c in copies:
        c.wait()


def top(n):
    return pl.ds(NIL, n)


def aligned(offset, n):
    return pl.ds(pl.multiple_of(offset, LANES), n)


def rope_tables(positions):
    half_dim = HEAD_DIM // 2
    inv_freq = jnp.power(jnp.float32(ROPE_BASE), -(jnp.arange(HEAD_DIM) % half_dim).astype(jnp.float32) * (2.0 / HEAD_DIM))
    angles = positions.astype(jnp.float32)[:, None] * inv_freq
    return jnp.cos(angles), jnp.sin(angles) * jnp.where(jnp.arange(HEAD_DIM) < half_dim, -1.0, 1.0)


def layer_kernel(chunks, cb, plan, x_hbm, seg, rope_c, rope_s, gain_a, gain_m, wq, wk, wv, wo, wg, wu, wd,
                 kc, vc, attn, wo_g, y_hbm,
                 wbuf, u2, hbuf, qb, seg_row, sgb, fq, fk, xmid, srow, sin, p_own, p_out, d_in, f_in, e_in, ystage,
                 xsem, wsem, sg_s, sg_r, k1s, k1r, k2s, k2r, kps, kpr, w1s, w1r, w2s, w2r, w3s, w3r, wps, wpr,
                 t_s, t_r, v_s, v_r, csem, lsem, osem, xrsem,
                 s_s, s_r, u1s, u1r, u2s, u2r, ups, upr, d_s, d_r, f_s, f_r, e_s, e_r, a_l, a_s, a_r, h_s, h_r):
    rows, dim = x_hbm.shape
    tp, sp = lax.axis_size("tp"), lax.axis_size("sp")
    hd = HEAD_DIM
    heads = wq.shape[ONE] // hd
    n_kv = wk.shape[ONE] // hd
    group = heads // n_kv
    wide = heads * hd
    col, wrow = dim // tp, wo.shape[NIL] // sp
    half = wrow // TWO
    nb = col // cb
    pair_w = TWO * cb
    ff = wg.shape[ONE] // TWO
    slots = wbuf.shape[NIL]
    per_dev = TWO * n_kv
    y, s = lax.axis_index("tp"), lax.axis_index("sp")
    core, chip, n_chip = s % TWO, s // TWO, sp // TWO
    yp, ym, y2 = (y + ONE) % tp, (y + tp - ONE) % tp, (y + TWO) % tp
    chip_at = lambda d: (chip + d) % n_chip * TWO
    up, dn, far = (chip_at(d) + core for d in (ONE, n_chip - ONE, TWO))
    pair = s + ONE - TWO * core
    to_pair, to_up, to_dn = ({"tp": y, "sp": d} for d in (pair, up, dn))
    to_p, to_m, to_2 = ({"tp": d, "sp": s} for d in (yp, ym, y2))
    scale2 = HEAD_DIM ** -0.5 * 1.4426950408889634

    kw = n_kv * hd
    n_x = xsem.shape[NIL]
    x_rows = rows // n_x
    x_copies = [pltpu.make_async_copy(x_hbm.at[pl.ds(i * x_rows, x_rows)], u2.at[pl.ds(i * x_rows, x_rows)], xsem.at[i])
                for i in range(n_x)]
    start(x_copies)
    kv_copies = [pltpu.make_async_copy(w, wbuf.at[NIL, :, pl.ds(i * kw, kw)], wsem.at[NIL, i]) for i, w in enumerate((wk, wv))]
    q_copies = [pltpu.make_async_copy(wq.at[:, pl.ds(t * TWO * kw, TWO * kw)], wbuf.at[ONE + t], wsem.at[ONE + t, NIL])
                for t in range(TWO)]

    barrier = pltpu.get_barrier_semaphore()
    for j in range(ONE, sp):
        pl.semaphore_signal(barrier, inc=ONE, device_id={"tp": y, "sp": (s + j) % sp}, device_id_type=MESH)
    for j in range(ONE, tp):
        pl.semaphore_signal(barrier, inc=ONE, device_id={"tp": (y + j) % tp, "sp": s}, device_id_type=MESH)

    def norm(i):
        x_copies[i].wait()
        step = x_rows // TWO

        @pl.loop(NIL, TWO)
        def _(j):
            rr = pl.ds(pl.multiple_of(i * x_rows + j * step, step), step)
            sq = jnp.zeros((step, LANES), F32)
            for b in range(dim // LANES):
                v = u2[rr, pl.ds(b * LANES, LANES)].astype(F32)
                sq += v * v
            inv = lax.rsqrt(jnp.sum(sq, axis=ONE, keepdims=True) * (1.0 / dim) + NORM_EPS)
            for b in range(dim // LANES):
                c = pl.ds(b * LANES, LANES)
                u2[rr, c] = (u2[rr, c].astype(F32) * inv * gain_a[:, c]).astype(BF16)

    seg_row[...] = jnp.broadcast_to(seg[...].astype(F32), (SUB, rows))
    norm(NIL)
    start(kv_copies)
    norm(ONE)
    pl.semaphore_wait(barrier, sp + tp - TWO)

    def w1(j):
        rank, mine = (y + j) % tp, aligned(s * wrow, wrow)
        return remote(wo.at[mine, aligned(rank * col, col)], wo_g.at[tp - ONE - j, mine],
                      w1s.at[j - ONE], w1r.at[tp - ONE - j], {"tp": rank, "sp": s})

    def sg(j):
        return remote(seg_row, sgb.at[s], sg_s.at[j], sg_r.at[j], {"tp": y, "sp": (s + j) % sp})

    for j in range(ONE, sp):
        sg(j).start()
    for j in range(ONE, tp):
        w1(j).start()

    def w_blk(i, dev, r0, n):
        return wo_g.at[i, pl.ds(pl.multiple_of(dev * wrow + r0, half), n)]

    def w2(i, side):
        b = w_blk(i, s, NIL, wrow)
        return remote(b, b, w2s.at[i, side], w2r.at[i, ONE - side], (to_up, to_dn)[side])

    def w3(i, side):
        b = w_blk(i, (up, dn)[side], (half, NIL)[side], half)
        return remote(b, b, w3s.at[i, side], w3r.at[i, side], (to_dn, to_up)[side])

    def wp(i, j):
        b = w_blk(i, (s, up, dn, far)[j], NIL, wrow)
        return remote(b, b, wps.at[i, j], wpr.at[i, j], to_pair)

    def w_start(i):
        w1(tp - ONE - i).wait_recv()
        w2(i, NIL).start()
        w2(i, ONE).start()
        wp(i, NIL).start()

    def w_mid(i):
        for side in range(TWO):
            w2(i, ONE - side).wait_recv()
            w3(i, side).start()
            wp(i, ONE + side).start()

    def w_last(i):
        w3(i, NIL).wait_recv()
        w3(i, ONE).wait_recv()
        wp(i, THREE).start()

    start(q_copies)
    for i in range(TWO, n_x):
        norm(i)

    def rope(t):
        return (t * rope_c[...] + pltpu.roll(t, hd // TWO, ONE) * rope_s[...]).astype(BF16)

    wait(kv_copies)
    r = jnp.dot(u2[top(rows), :], wbuf[NIL], preferred_element_type=F32)
    for g in range(n_kv):
        hbuf[s * per_dev + TWO * g] = rope(r[:, g * hd:(g + ONE) * hd])
        hbuf[s * per_dev + TWO * g + ONE] = r[:, kw + g * hd:kw + (g + ONE) * hd].astype(BF16)

    def k_blk(dev, g, lo=NIL, n=TWO):
        return hbuf.at[pl.ds(dev * per_dev + TWO * g + lo, n)]

    def k1(g, side):
        b = k_blk(s, g)
        return remote(b, b, k1s.at[g, side], k1r.at[g, ONE - side], (to_up, to_dn)[side])

    def k2(g, side):
        b = k_blk((up, dn)[side], g, ONE - side, ONE)
        return remote(b, b, k2s.at[g, side], k2r.at[g, side], (to_dn, to_up)[side])

    def kp(g, j):
        b = k_blk((s, up, dn, far)[j], g)
        return remote(b, b, kps.at[g, j], kpr.at[g, j], to_pair)

    def k_start(g):
        k1(g, NIL).start()
        k1(g, ONE).start()
        kp(g, NIL).start()

    def k_mid(g):
        for side in range(TWO):
            k1(g, ONE - side).wait_recv()
            k2(g, side).start()
            kp(g, ONE + side).start()

    def k_last(g):
        k2(g, NIL).wait_recv()
        k2(g, ONE).wait_recv()
        kp(g, THREE).start()

    k_start(NIL)

    for t in range(TWO):
        q_copies[t].wait()
        r = jnp.dot(u2[top(rows), :], wbuf[ONE + t], preferred_element_type=F32)
        for g in range(heads // TWO):
            qb[t * (heads // TWO) + g] = rope(r[:, g * hd:(g + ONE) * hd])

    n_o = -(-col // pair_w)
    part = wide
    starts = [sum(chunks[:i]) for i in range(len(chunks))]
    n_ch = len(chunks)

    def cols(block, width):
        return aligned(block * width, width)

    def o_width(t):
        return min(pair_w, col - t * pair_w)

    def o_part(t, j):
        w = o_width(t)
        src = wo_g.at[j - ONE, :, pl.ds(t * pair_w, w)] if j else wo.at[:, aligned(y * col + t * pair_w, w)]
        return pltpu.make_async_copy(src, wbuf.at[t, aligned((y + j) % tp * part, part), top(w)], osem.at[t, j])

    def rows_of(i, row0, n):
        return pl.ds(TWO * starts[i] + row0, n)

    xr_copies = [pltpu.make_async_copy(x_hbm.at[pl.ds(r0, r), cols(y, col)], u2.at[rows_of(i, NIL, r), cols(y, col)], xrsem.at[i])
                 for i, (r0, r) in enumerate(zip(starts, chunks))]
    start(xr_copies)
    for t in range(n_o):
        o_part(t, NIL).start()

    for j in range(ONE, sp):
        sg(j).wait_recv()
    sgb[s] = seg_row[...]
    lane = lax.broadcasted_iota(jnp.int32, (rows, LANES), ONE).astype(F32)

    def seg_col(dev):
        return jnp.broadcast_to(sgb[dev, top(ONE), :], (LANES, rows)).T

    fq[...] = jnp.where(seg_col(s) == lane, 1.0, 0.0).astype(BF16)

    @pl.loop(NIL, sp)
    def _(b):
        fk[b] = jnp.where(seg_col(b) == lane, 0.0, -1e30).astype(BF16)

    def attend(h, i, g, b0, nb, own):
        nk = nb * rows
        both = lambda j: jnp.concatenate([hbuf[(b0 + d) * per_dev + TWO * g + j] for d in range(nb)], axis=NIL)
        q = jnp.concatenate([qb[h], fq[...]], axis=ONE)
        k = jnp.concatenate([both(NIL), fk[pl.ds(b0, nb)].reshape(nk, LANES)], axis=ONE)
        v = both(ONE)
        sc = lax.dot_general(q, k, (((ONE,), (ONE,)), ((), ())), preferred_element_type=F32)
        if own:
            lo = nk - rows
            a, b = (lax.broadcasted_iota(jnp.int32, (rows, rows), d) for d in range(TWO))
            tail = jnp.where(a >= b, sc[:, lo:], -1e30)
            sc = jnp.concatenate([sc[:, :lo], tail], axis=ONE) if lo else tail
        at = aligned(i * rows, rows)
        mx = jnp.max(sc, axis=ONE, keepdims=True)
        if own:
            mn = jnp.broadcast_to(mx, (rows, LANES))
        else:
            mn = jnp.maximum(xmid[group + i], mx)
            al = jnp.exp2((xmid[group + i] - mn) * scale2)
        ps = [jnp.exp2((sc[:, j * LANES:(j + ONE) * LANES] - mn) * scale2) for j in range(nk // LANES)]
        ls = functools.reduce(jnp.add, ps)
        o = jnp.dot(jnp.concatenate([p.astype(BF16) for p in ps], axis=ONE), v, preferred_element_type=F32)
        xmid[group + i] = mn
        if own:
            p_own[at, top(LANES)] = ls
            xmid[i] = o
        else:
            p_own[at, top(LANES)] = p_own[at, top(LANES)] * al + ls
            xmid[i] = xmid[i] * al + o

    def a_at(rank, h, r0, n):
        return attn.at[pl.ds(r0, n), aligned(rank * wide + h * hd, hd)]

    def a1(h, side):
        return remote(qb.at[h], a_at(y, h, NIL, rows), t_s.at[side, h], t_r.at[ONE - side, h], (to_p, to_m)[side])

    def a2(h, side):
        b = a_at((yp, ym)[side], h, (rows // TWO, NIL)[side], rows // TWO)
        return remote(b, b, v_s.at[side, h], v_r.at[side, h], (to_m, to_p)[side])

    def pass_on(h):
        for side in range(TWO):
            a1(h, ONE - side).wait_recv()
            a2(h, side).start()

    @pl.loop(NIL, n_kv)
    def _(g):
        @pl.when(g == NIL)
        def _():
            k_mid(NIL)
            k_start(ONE)

        kp(g, NIL).wait_recv()

        @pl.loop(NIL, group)
        def _(i):
            @pl.when(core == NIL)
            def _():
                attend(g * group + i, i, g, s, ONE, True)

            @pl.when(core == ONE)
            def _():
                attend(g * group + i, i, g, chip_at(NIL), TWO, True)

        k_last(g)
        for j in range(ONE, FOUR):
            kp(g, j).wait_recv()

        @pl.loop(NIL, group)
        def _(i):
            h = g * group + i

            @pl.when(chip >= ONE)
            def _():
                attend(h, i, g, chip_at(n_chip - ONE), TWO, False)

            @pl.when(chip == n_chip - ONE)
            def _():
                attend(h, i, g, chip_at(ONE), TWO, False)

            @pl.when(chip >= TWO)
            def _():
                attend(h, i, g, chip_at(TWO), TWO, False)

            total = jnp.sum(p_own[aligned(i * rows, rows), top(LANES)], axis=ONE, keepdims=True)
            qb[h] = (xmid[i] / total).astype(BF16)
            a1(h, NIL).start()
            a1(h, ONE).start()

            @pl.when(h == NIL)
            def _():
                k_mid(ONE)
                for b in range(tp - ONE):
                    w_start(b)

            for b in range(tp - TWO):
                @pl.when(h == heads - FOUR + b)
                def _():
                    w_mid(b)

            @pl.when(h >= TWO)
            def _():
                pass_on(h - TWO)

    mine_kv = s // (sp // n_kv)
    caches = [pltpu.make_async_copy(hbuf.at[d * per_dev + TWO * mine_kv + i], c.at[pl.ds(d * rows, rows)], csem.at[i, d])
              for i, c in enumerate((kc, vc)) for d in range(sp)]
    start(caches)
    pass_on(heads - TWO)
    w_mid(tp - TWO)
    pass_on(heads - ONE)

    def w_done(i):
        for j in range(FOUR):
            wp(i, j).wait_recv()
        for t in range(n_o):
            o_part(t, i + ONE).start()

    for g in range(n_kv):
        for j in range(FOUR):
            kp(g, j).wait_send()
        for side in range(TWO):
            k1(g, side).wait_send()
            k2(g, side).wait_send()
    wait(caches)

    def head_in(d, h):
        rank = (y + d) % tp
        return pltpu.make_async_copy(a_at(rank, h, NIL, rows), hbuf.at[rank * heads + h], lsem.at[d, h])

    for h in range(heads):
        hbuf[y * heads + h] = qb[h]
        head_in(ONE, h).start()
        head_in(THREE, h).start()

    for i in range(tp - ONE):
        w_last(i)
        if i:
            w_done(i - ONE)
    for h in range(heads):
        for side in range(TWO):
            a2(h, side).wait_recv()
        head_in(TWO, h).start()
    w_done(tp - TWO)
    for h in range(heads):
        for d in range(ONE, tp):
            head_in(d, h).wait()

    def wide_rows(r0, n):
        return jnp.concatenate([hbuf[b, pl.ds(r0, n)] for b in range(hbuf.shape[NIL])], axis=ONE)

    def front_sent():
        @pl.loop(NIL, heads)
        def _(h):
            for side in range(TWO):
                a1(h, side).wait_send()
                a2(h, side).wait_send()
        for i in range(tp - ONE):
            w1(i + ONE).wait_send()
            for j in range(FOUR):
                wp(i, j).wait_send()
            for side in range(TWO):
                w2(i, side).wait_send()
                w3(i, side).wait_send()
        for j in range(ONE, sp):
            sg(j).wait_send()

    n_g, n_d = ff // pair_w, nb * tp // FOUR

    def g_tile(n, slot, which):
        c = aligned(core * ff + n * pair_w, pair_w)
        return pltpu.make_async_copy((wg, wu)[which].at[:, c], wbuf.at[slot], wsem.at[slot, NIL])

    def g_pair(n, base):
        return [g_tile(n, (base + TWO * n + i) % slots, i) for i in range(TWO)]

    def d_cols(m):
        q = m // nb
        d = (TWO + THREE * q + THREE * (q * (q - ONE) // TWO)) % FOUR
        return aligned((y + d) % tp * col + m % nb * cb, cb)

    def d_tile(p, slot):
        return [pltpu.make_async_copy(wd.at[aligned(core * ff, ff), d_cols(TWO * p + i)],
                                      wbuf.at[slot, top(ff), pl.ds(i * cb, cb)], wsem.at[slot, i]) for i in range(TWO)]

    def d_pair(p, base):
        return [c for i in range(TWO) for c in d_tile(TWO * p + i, (base + TWO * p + i) % slots)]

    base = n_o

    lanes = srow.shape[-ONE]

    def stat(i, j):
        return remote(srow.at[i], sin.at[i, j], s_s.at[i, j], s_r.at[i, j], (to_p, to_m, to_2)[j])

    def x1_rows(i):
        r0, r = starts[i], chunks[i]
        for t in range(n_o):
            w = o_width(t)
            if not i:
                wait([o_part(t, j) for j in range(tp)])
            v = jnp.dot(wide_rows(r0, r), wbuf[t, top(tp * part), top(w)], preferred_element_type=F32)
            for q in range(w // LANES):
                xmid[t * FOUR + q, pl.ds(r0, r)] = v[:, q * LANES:(q + ONE) * LANES]
        sq = jnp.zeros((r, LANES), F32)
        for b in range(col // LANES):
            v = xmid[b, pl.ds(r0, r)] + u2[rows_of(i, NIL, r), aligned(y * col + b * LANES, LANES)].astype(F32)
            xmid[b, pl.ds(r0, r)] = v
            sq += v * v
        tot = jnp.broadcast_to(jnp.sum(sq, axis=ONE, keepdims=True), (r, LANES))
        if r < lanes:
            tot = jnp.concatenate([tot, jnp.zeros((lanes - r, LANES), F32)], axis=NIL)
        srow[i] = tot.T[:SUB, :]
        for j in range(tp - ONE):
            stat(i, j).start()

    def norm_rows(i):
        r0, r = starts[i], chunks[i]
        for j in range(tp - ONE):
            stat(i, j).wait()
        tot = srow[i]
        for j in range(tp - ONE):
            tot += sin[i, j]
        inv = lax.rsqrt(tot * (1.0 / dim) + NORM_EPS)
        inv = jnp.broadcast_to(inv[:ONE, :], (LANES, lanes)).T[:r, :]
        for b in range(col // LANES):
            c = aligned(y * col + b * LANES, LANES)
            u2[rows_of(i, NIL, r), c] = (xmid[b, pl.ds(r0, r)] * inv * gain_m[:, c]).astype(BF16)

    def u_blk(i, row0, n_rows, rank):
        return u2.at[rows_of(i, row0, n_rows), cols(rank, col)]

    def u_first(i, side, turn):
        h = chunks[i] // TWO
        b = u_blk(i, h * (side + turn - TWO * side * turn), h, y)
        return remote(b, b, u1s.at[i, side, turn], u1r.at[i, ONE - side, turn], (to_p, to_m)[side])

    def u_second(i, side):
        h = chunks[i] // TWO
        b = u_blk(i, h, h, yp) if side == NIL else u_blk(i, NIL, h, ym)
        return remote(b, b, u2s.at[i, side], u2r.at[i, side], (to_m, to_p)[side])

    def u_pair(i, j):
        r, rank = chunks[i], (y, yp, ym, y2)[j]
        return remote(u_blk(i, NIL, r, rank), u_blk(i, r, r, rank), ups.at[i, j], upr.at[i, j], to_pair)

    def u_start(i):
        for turn in range(TWO):
            u_first(i, NIL, turn).start()
            u_first(i, ONE, turn).start()
        u_pair(i, NIL).start()

    def u_mid(i):
        for side in range(TWO):
            u_first(i, ONE - side, NIL).wait_recv()
            u_second(i, side).start()

    def u_last(i):
        for side in range(TWO):
            u_first(i, ONE - side, ONE).wait_recv()
            u_pair(i, ONE + side).start()
        for side in range(TWO):
            u_second(i, side).wait_recv()
        u_pair(i, THREE).start()

    def u_ready(i):
        for j in range(FOUR):
            u_pair(i, j).wait_recv()

    def u_drain(i):
        for side in range(TWO):
            for turn in range(TWO):
                u_first(i, side, turn).wait_send()
            u_second(i, side).wait_send()
        for j in range(FOUR):
            u_pair(i, j).wait_send()

    def blk_rows(m, row0, n):
        return pl.ds(pl.multiple_of(m * max(chunks) + row0, EIGHT), n)

    def d_copy(i, m, slot):
        r, par = chunks[i], i % TWO
        return remote(p_out.at[slot, top(r)], d_in.at[par, m, top(r)], d_s.at[slot], d_r.at[par, m], to_pair)

    def t_add(i, m):
        r, par = chunks[i], i % TWO
        d_copy(i, m, NIL).wait_recv()
        p_own[blk_rows(m, NIL, r), :] += d_in[par, m, top(r)]

    def f_copy(i, k, side):
        h, par = chunks[i] // TWO, i % TWO
        return remote(p_own.at[blk_rows(k, side * h, h)], f_in.at[par, side, k, top(h)],
                      f_s.at[side, k], f_r.at[par, side, k], (to_m, to_p)[side])

    def t_f(i, k):
        f_copy(i, k, NIL).start()
        f_copy(i, k, ONE).start()

    def e_copy(i, k, side):
        r, par = chunks[i], i % TWO
        return remote(p_own.at[blk_rows((TWO - side) * nb + k, NIL, r)], e_in.at[par, side, k, top(r)],
                      e_s.at[side, k], e_r.at[par, side, k], (to_m, to_p)[side])

    def t_e(i, k, side):
        h, par = chunks[i] // TWO, i % TWO
        f_copy(i, k, side).wait_recv()
        p_own[blk_rows((TWO - side) * nb + k, side * h, h), :] += f_in[par, side, k, top(h)]
        e_copy(i, k, side).start()

    def y_at(i, row0, n_rows, rank, k):
        return y_hbm.at[pl.ds(starts[i] + row0, n_rows), aligned(rank * col + k * cb, cb)]

    def a_copy_y(i, k, side):
        r, par = chunks[i], i % TWO
        return remote(ystage.at[par, k, top(r)], y_at(i, NIL, r, y, k), a_s.at[par, side, k], a_r.at[par, ONE - side, k],
                      (to_p, to_m)[side])

    def a_local(i, k):
        r, par = chunks[i], i % TWO
        return pltpu.make_async_copy(ystage.at[par, k, top(r)], y_at(i, NIL, r, y, k), a_l.at[par, k])

    def h_copy(i, k, side):
        h = chunks[i] // TWO
        b = y_at(i, h, h, yp, k) if side == NIL else y_at(i, NIL, h, ym, k)
        return remote(b, b, h_s.at[i, side, k], h_r.at[i, side, k], (to_m, to_p)[side])

    def t_final(i, k):
        r, par = chunks[i], i % TWO
        for side in range(TWO):
            e_copy(i, k, side).wait_recv()
        v = (p_own[blk_rows(THREE * nb + k, NIL, r), :] + e_in[par, NIL, k, top(r)] + e_in[par, ONE, k, top(r)]
             + jnp.concatenate([xmid[TWO * k + q, pl.ds(starts[i], r)] for q in range(TWO)], axis=ONE))
        ystage[par, k, top(r)] = v.astype(BF16)
        for side in range(TWO):
            a_copy_y(i, k, side).start()
        a_local(i, k).start()

    def t_fwd(i, k):
        for side in range(TWO):
            a_copy_y(i, k, ONE - side).wait_recv()
            h_copy(i, k, side).start()

    def sums_sent(i):
        for k in range(nb):
            for side in range(TWO):
                f_copy(i, k, side).wait_send()
                e_copy(i, k, side).wait_send()

    def rows_done(i):
        for k in range(nb):
            for side in range(TWO):
                h_copy(i, k, side).wait_recv()
                h_copy(i, k, side).wait_send()
                a_copy_y(i, k, side).wait_send()
            a_local(i, k).wait()

    g_tile(NIL, base, NIL).start()
    wait(xr_copies)
    for i in range(n_ch):
        x1_rows(i)
        if i == ONE:
            norm_rows(NIL)
            u_start(NIL)
    g_tile(NIL, NIL, ONE).start()
    norm_rows(ONE)
    u_mid(NIL)
    u_start(ONE)
    front_sent()
    for i in range(TWO, n_ch):
        norm_rows(i)
    u_last(NIL)
    u_ready(NIL)

    tasks = {"mid": u_mid, "last": u_last, "start": u_start, "e": t_e, "final": t_final, "fwd": t_fwd}

    def run(todo, at):
        for when, name, *args in todo:
            @pl.when(at == when)
            def _():
                tasks[name](*args)

    for i in range(n_ch):
        r = chunks[i]
        g_base, d_base = base % slots, (base + TWO * n_g) % slots
        base += TWO * (n_g + n_d)

        @pl.loop(NIL, n_g)
        def _(j):
            @pl.when(j + ONE < n_g)
            def _():
                start(g_pair(j + ONE, g_base))

            @pl.when(j + ONE >= n_g)
            def _():
                start(d_pair(NIL, d_base))

            wait(g_pair(j, g_base))
            g, u = (jnp.dot(u2[rows_of(i, NIL, TWO * r), :], wbuf[(g_base + TWO * j + q) % slots], preferred_element_type=F32)
                    for q in range(TWO))
            g = (jax.nn.silu(g) * u).astype(BF16)
            for q in range(FOUR):
                hbuf[FOUR * j + q, top(TWO * r)] = g[:, q * LANES:(q + ONE) * LANES]
            run(plan[i][NIL], j)

        if i:
            sums_sent(i - ONE)

        @pl.loop(NIL, n_d)
        def _(p):
            @pl.when(p + ONE < n_d)
            def _():
                start(d_pair(p + ONE, d_base))

            if i + ONE < n_ch:
                @pl.when(p + ONE >= n_d)
                def _():
                    start(g_pair(NIL, base % slots))

            wait(d_pair(p, d_base))
            out = p % TWO * FOUR

            @pl.when(p >= TWO)
            def _():
                for q in range(FOUR):
                    d_copy(i, q, out + q).wait_send()

            for q in range(TWO):
                v = jnp.dot(wide_rows(NIL, TWO * r), wbuf[(d_base + TWO * p + q) % slots, top(ff)],
                            preferred_element_type=F32)
                for e in range(TWO):
                    b = TWO * q + e
                    p_own[blk_rows(FOUR * p + b, NIL, r), :] = v[:r, e * cb:(e + ONE) * cb]
                    p_out[out + b, top(r)] = v[r:, e * cb:(e + ONE) * cb]
            for q in range(FOUR):
                d_copy(i, FOUR * p + q, out + q).start()

            @pl.when(p >= ONE)
            def _():
                for q in range(FOUR):
                    t_add(i, FOUR * (p - ONE) + q)

            @pl.when(p == ONE)
            def _():
                for k in range(FOUR):
                    t_f(i, k)

            @pl.when(p == TWO)
            def _():
                for k in range(FOUR, nb):
                    t_f(i, k)
            run(plan[i][ONE], p)

        for q in range(FOUR):
            t_add(i, FOUR * (n_d - ONE) + q)
        for q in range(FOUR):
            for out in range(TWO):
                d_copy(i, q, FOUR * out + q).wait_send()
        for name, *args in plan[i][TWO]:
            tasks[name](*args)
        if i + ONE < n_ch:
            u_ready(i + ONE)

    last = n_ch - ONE
    if last >= TWO:
        rows_done(last - TWO)
    for k in range(nb):
        t_final(last, k)
        if k >= TWO:
            t_fwd(last, k - TWO)
    for k in range(nb - TWO, nb):
        t_fwd(last, k)
    for i in range(max(last - ONE, NIL), n_ch):
        rows_done(i)
    sums_sent(last)
    for i in range(n_ch):
        u_drain(i)


CHUNKS = (192, 192, 128)


def mlp_plan():
    early = lambda i: [(3, "e", i, 0, 1), (3, "e", i, 1, 1), (4, "e", i, 2, 1), (4, "e", i, 0, 0), (4, "e", i, 1, 0)]
    late = lambda i: [("e", i, 3, 1), ("e", i, 2, 0), ("e", i, 4, 1), ("e", i, 3, 0), ("e", i, 4, 0)]
    at_start = lambda i: [(0, *t) for t in late(i)]
    finals = lambda i, at: [(a, "final", i, k) for k, a in enumerate(at)]
    passed = lambda i, at: [(a, "fwd", i, k) for k, a in enumerate(at)]
    gather = [(1, "mid", 1), (1, "start", 2), (3, "last", 1), (4, "mid", 2), (6, "last", 2)]
    return ((gather, early(0), ()),
            (at_start(0) + finals(0, (1, 2, 3, 4, 5)) + passed(0, (5, 6, 6, 6, 7)), early(1), ()),
            (at_start(1) + finals(1, (2, 3, 4, 6, 7)), passed(1, (0, 1, 1, 2, 2)) + early(2), late(2)))


def layer_call(x_in, positions, segments, gain_a, gain_m, wq, wk, wv, wo, wg, wu, wd):
    rows, dim = x_in.shape
    tp, sp = lax.axis_size("tp"), lax.axis_size("sp")
    heads, n_kv = wq.shape[ONE] // HEAD_DIM, wk.shape[ONE] // HEAD_DIM
    cb = TWO * LANES
    col, ff = dim // tp, wg.shape[ONE] // TWO
    nb = col // cb
    n_ch, rm = len(CHUNKS), max(CHUNKS)
    lanes = -(-rm // LANES) * LANES
    rope_c, rope_s = rope_tables(positions)
    dma = pltpu.SemaphoreType.DMA
    hbm, vmem = pl.BlockSpec(memory_space=pl.ANY), pl.BlockSpec(memory_space=pltpu.VMEM)
    bufs = [((FOUR, dim, TWO * cb), BF16), ((TWO * rows, dim), BF16), ((ff // LANES, rows, LANES), BF16),
            ((heads, rows, HEAD_DIM), BF16), ((SUB, rows), F32), ((sp, SUB, rows), F32), ((rows, LANES), BF16),
            ((sp, rows, LANES), BF16), ((col // LANES, rows, LANES), F32), ((n_ch, SUB, lanes), F32), ((n_ch, tp - ONE, SUB, lanes), F32),
            ((tp * nb * rm, cb), F32), ((EIGHT, rm, cb), F32), ((TWO, tp * nb, rm, cb), F32),
            ((TWO, TWO, nb, rm // TWO, cb), F32), ((TWO, TWO, nb, rm, cb), F32), ((TWO, nb, rm, cb), BF16)]
    sems = [(FOUR,), (FOUR, TWO), (sp,), (sp,)] + [(n_kv, TWO)] * FOUR + [(n_kv, FOUR)] * TWO + [(tp - ONE,)] * TWO
    sems += [(tp - ONE, TWO)] * FOUR + [(tp - ONE, FOUR)] * TWO + [(TWO, heads)] * FOUR + [(TWO, sp), (tp, heads), (THREE, tp), (n_ch,)]
    sems += [(n_ch, tp - ONE)] * TWO + [(n_ch, TWO, TWO)] * TWO + [(n_ch, TWO)] * TWO + [(n_ch, FOUR)] * TWO
    sems += [(EIGHT,), (TWO, tp * nb)] + [(TWO, nb), (TWO, TWO, nb)] * TWO + [(TWO, nb)] + [(TWO, TWO, nb)] * TWO
    sems += [(n_ch, TWO, nb)] * TWO
    cache = jax.ShapeDtypeStruct((sp * rows, HEAD_DIM), BF16)
    kc, vc, _, _, y_out = pl.pallas_call(
        functools.partial(layer_kernel, CHUNKS, cb, mlp_plan()), name="layer",
        out_shape=[cache, cache, jax.ShapeDtypeStruct((rows, tp * heads * HEAD_DIM), BF16), jax.ShapeDtypeStruct((tp - ONE, wo.shape[NIL], col), BF16),
                   jax.ShapeDtypeStruct((rows, dim), BF16)],
        in_specs=[hbm] + [vmem] * (FOUR + ONE) + [hbm] * (FOUR + THREE), out_specs=[hbm] * (FOUR + ONE),
        scratch_shapes=[pltpu.VMEM(*b) for b in bufs] + [dma(q) for q in sems],
        compiler_params=pltpu.CompilerParams(collective_id=ONE, has_side_effects=True, vmem_limit_bytes=VMEM_BYTES),
    )(x_in, segments.reshape(ONE, rows), rope_c, rope_s, gain_a.reshape(ONE, dim), gain_m.reshape(ONE, dim),
      wq, wk, wv, wo, wg, wu, wd)
    return y_out, kc, vc


def solution(mesh):
    row_spec = P(("rep", "sp"), None)
    tok_spec = P(("rep", "sp"))
    full_spec = P(None)
    col_spec = P(None, "tp")
    wrow_spec = P("tp", None)
    cache_spec = P("rep", ("tp", "sp"), None)

    def local_layer(x_in, positions, segments, gain_attn, w_q, w_k, w_v, w_o, gain_mlp, w_gate, w_up, w_down):
        y_out, kc, vc = layer_call(x_in, positions, segments, gain_attn, gain_mlp, w_q, w_k, w_v, w_o, w_gate, w_up, w_down)
        return y_out, kc.reshape(-1, 1, HEAD_DIM), vc.reshape(-1, 1, HEAD_DIM)

    return jax.shard_map(local_layer, mesh=mesh,
                         in_specs=(row_spec, tok_spec, tok_spec, full_spec, col_spec, col_spec, col_spec, wrow_spec,
                                   full_spec, col_spec, col_spec, wrow_spec),
                         out_specs=(row_spec, cache_spec, cache_spec), check_vma=False)
```

```python
import functools

import jax
import jax.numpy as jnp
import numpy as np
from jax import lax
from jax.experimental import pallas as pl
from jax.experimental.pallas import tpu as pltpu
from jax.sharding import PartitionSpec as P

HEAD_DIM = 128
ROPE_BASE = 500000.0
NORM_EPS = 1e-5
MESH = pl.DeviceIdType.MESH
BF16, F32 = jnp.bfloat16, jnp.float32
VMEM_BYTES = 67043328
NIL, ONE, TWO, THREE, FOUR, EIGHT, SUB, LANES = 0, 1, 2, 3, 4, 8, 8, 128


def remote(src, dst, send_sem, recv_sem, to):
    return pltpu.make_async_remote_copy(src, dst, send_sem, recv_sem, device_id=to, device_id_type=MESH)


def start(copies):
    for c in copies:
        c.start()


def wait(copies):
    for c in copies:
        c.wait()


def top(n):
    return pl.ds(NIL, n)


def aligned(offset, n):
    return pl.ds(pl.multiple_of(offset, LANES), n)


def layer_kernel(chunks, cb, plan, x_hbm, seg, pos, freq, gain_a, gain_m, wq, wk, wv, wo, wg, wu, wd,
                 kc, vc, attn, wo_g, y_hbm,
                 wbuf, u2, hbuf, qb, rope_c, rope_s, seg_row, sgb, fq, xmid, srow, sin, p_own, p_out, d_in, f_in, e_in, ystage,
                 xsem, wsem, sg_s, sg_r, k1s, k1r, k2s, k2r, kps, kpr, w1s, w1r, w2s, w2r, w3s, w3r, wps, wpr,
                 t_s, t_r, v_s, v_r, csem, lsem, osem, xrsem,
                 s_s, s_r, u1s, u1r, u2s, u2r, ups, upr, d_s, d_r, f_s, f_r, e_s, e_r, a_l, a_s, a_r, h_s, h_r):
    rows, dim = x_hbm.shape
    tp, sp = lax.axis_size("tp"), lax.axis_size("sp")
    hd = HEAD_DIM
    heads = wq.shape[ONE] // hd
    n_kv = wk.shape[ONE] // hd
    group = heads // n_kv
    wide = heads * hd
    col, wrow = dim // tp, wo.shape[NIL] // sp
    half = wrow // TWO
    nb = col // cb
    pair_w = TWO * cb
    ff = wg.shape[ONE] // TWO
    slots = wbuf.shape[NIL]
    per_dev = TWO * n_kv
    y, s = lax.axis_index("tp"), lax.axis_index("sp")
    core, chip, n_chip = s % TWO, s // TWO, sp // TWO
    yp, ym, y2 = (y + ONE) % tp, (y + tp - ONE) % tp, (y + TWO) % tp
    chip_at = lambda d: (chip + d) % n_chip * TWO
    up, dn, far = (chip_at(d) + core for d in (ONE, n_chip - ONE, TWO))
    pair = s + ONE - TWO * core
    to_pair, to_up, to_dn = ({"tp": y, "sp": d} for d in (pair, up, dn))
    to_p, to_m, to_2 = ({"tp": d, "sp": s} for d in (yp, ym, y2))
    scale2 = HEAD_DIM ** -0.5 * 1.4426950408889634

    kw = n_kv * hd
    n_x = xsem.shape[NIL]
    x_rows = rows // n_x
    x_copies = [pltpu.make_async_copy(x_hbm.at[pl.ds(i * x_rows, x_rows)], u2.at[pl.ds(i * x_rows, x_rows)], xsem.at[i])
                for i in range(n_x)]
    start(x_copies)
    kv_copies = [pltpu.make_async_copy(w, wbuf.at[NIL, :, pl.ds(i * kw, kw)], wsem.at[NIL, i]) for i, w in enumerate((wk, wv))]

    def q_copy(t):
        return pltpu.make_async_copy(wq.at[:, aligned(t * TWO * kw, TWO * kw)], wbuf.at[ONE + t], wsem.at[ONE + t, NIL])

    barrier = pltpu.get_barrier_semaphore()
    for j in range(ONE, sp):
        pl.semaphore_signal(barrier, inc=ONE, device_id={"tp": y, "sp": (s + j) % sp}, device_id_type=MESH)
    for j in range(ONE, tp):
        pl.semaphore_signal(barrier, inc=ONE, device_id={"tp": (y + j) % tp, "sp": s}, device_id_type=MESH)

    def norm(i):
        x_copies[i].wait()
        step = x_rows // TWO

        @pl.loop(NIL, TWO)
        def _(j):
            rr = pl.ds(pl.multiple_of(i * x_rows + j * step, step), step)
            sq = jnp.zeros((step, LANES), F32)
            for b in range(dim // LANES):
                v = u2[rr, pl.ds(b * LANES, LANES)].astype(F32)
                sq += v * v
            inv = lax.rsqrt(jnp.sum(sq, axis=ONE, keepdims=True) * (1.0 / dim) + NORM_EPS)
            for b in range(dim // LANES):
                c = pl.ds(b * LANES, LANES)
                u2[rr, c] = (u2[rr, c].astype(F32) * inv * gain_a[:, c]).astype(BF16)

    seg_row[...] = jnp.broadcast_to(seg[...].astype(F32), (SUB, rows))
    norm(NIL)
    start(kv_copies)
    norm(ONE)
    pl.semaphore_wait(barrier, sp + tp - TWO)

    def w1(j):
        rank, mine = (y + j) % tp, aligned(s * wrow, wrow)
        return remote(wo.at[mine, aligned(rank * col, col)], wo_g.at[tp - ONE - j, mine],
                      w1s.at[j - ONE], w1r.at[tp - ONE - j], {"tp": rank, "sp": s})

    def sg(j):
        return remote(seg_row, sgb.at[s], sg_s.at[j], sg_r.at[j], {"tp": y, "sp": (s + j) % sp})

    for j in range(ONE, sp):
        sg(j).start()
    for j in range(ONE, tp):
        w1(j).start()

    def w_blk(i, dev, r0, n):
        return wo_g.at[i, pl.ds(pl.multiple_of(dev * wrow + r0, half), n)]

    def w2(i, side):
        b = w_blk(i, s, NIL, wrow)
        return remote(b, b, w2s.at[i, side], w2r.at[i, ONE - side], (to_up, to_dn)[side])

    def w3(i, side):
        b = w_blk(i, (up, dn)[side], (half, NIL)[side], half)
        return remote(b, b, w3s.at[i, side], w3r.at[i, side], (to_dn, to_up)[side])

    def wp(i, j):
        b = w_blk(i, (s, up, dn, far)[j], NIL, wrow)
        return remote(b, b, wps.at[i, j], wpr.at[i, j], to_pair)

    def w_start(i):
        w1(tp - ONE - i).wait_recv()
        w2(i, NIL).start()
        w2(i, ONE).start()
        wp(i, NIL).start()

    def w_mid(i):
        for side in range(TWO):
            w2(i, ONE - side).wait_recv()
            w3(i, side).start()
            wp(i, ONE + side).start()

    def w_last(i):
        w3(i, NIL).wait_recv()
        w3(i, ONE).wait_recv()
        wp(i, THREE).start()

    q_copy(NIL).start()
    q_copy(ONE).start()
    for i in range(TWO, n_x):
        norm(i)

    def rope(t):
        return (t * rope_c[...] + pltpu.roll(t, hd // TWO, ONE) * rope_s[...]).astype(BF16)

    wait(kv_copies)
    angles = jnp.broadcast_to(pos[...].astype(F32), (LANES, rows)).T * freq[...]
    sign = jnp.where(lax.broadcasted_iota(jnp.int32, (rows, hd), ONE) < hd // TWO, -1.0, 1.0)
    rope_c[...] = jnp.cos(angles)
    rope_s[...] = jnp.sin(angles) * sign
    r = jnp.dot(u2[top(rows), :], wbuf[NIL], preferred_element_type=F32)
    for g in range(n_kv):
        hbuf[s * per_dev + TWO * g] = rope(r[:, g * hd:(g + ONE) * hd])
        hbuf[s * per_dev + TWO * g + ONE] = r[:, kw + g * hd:kw + (g + ONE) * hd].astype(BF16)

    def k_blk(dev, g, lo=NIL, n=TWO):
        return hbuf.at[pl.ds(dev * per_dev + TWO * g + lo, n)]

    def k1(g, side):
        b = k_blk(s, g)
        return remote(b, b, k1s.at[g, side], k1r.at[g, ONE - side], (to_up, to_dn)[side])

    def k2(g, side):
        b = k_blk((up, dn)[side], g, ONE - side, ONE)
        return remote(b, b, k2s.at[g, side], k2r.at[g, side], (to_dn, to_up)[side])

    def kp(g, j):
        b = k_blk((s, up, dn, far)[j], g)
        return remote(b, b, kps.at[g, j], kpr.at[g, j], to_pair)

    def k_start(g):
        k1(g, NIL).start()
        k1(g, ONE).start()
        kp(g, NIL).start()

    def k_mid(g):
        for side in range(TWO):
            k1(g, ONE - side).wait_recv()
            k2(g, side).start()
            kp(g, ONE + side).start()

    def k_last(g):
        k2(g, NIL).wait_recv()
        k2(g, ONE).wait_recv()
        kp(g, THREE).start()

    k_start(NIL)

    @pl.loop(NIL, TWO)
    def _(t):
        q_copy(t).wait()
        r = jnp.dot(u2[top(rows), :], wbuf[ONE + t], preferred_element_type=F32)
        for g in range(heads // TWO):
            qb[t * (heads // TWO) + g] = rope(r[:, g * hd:(g + ONE) * hd])

    n_o = -(-col // pair_w)
    part = wide
    starts = [sum(chunks[:i]) for i in range(len(chunks))]
    n_ch = len(chunks)

    def cols(block, width):
        return aligned(block * width, width)

    def o_width(t):
        return min(pair_w, col - t * pair_w)

    def o_part(t, j):
        w = o_width(t)
        src = wo_g.at[j - ONE, :, pl.ds(t * pair_w, w)] if j else wo.at[:, aligned(y * col + t * pair_w, w)]
        return pltpu.make_async_copy(src, wbuf.at[t, aligned((y + j) % tp * part, part), top(w)], osem.at[t, j])

    def rows_of(i, row0, n):
        return pl.ds(TWO * starts[i] + row0, n)

    xr_copies = [pltpu.make_async_copy(x_hbm.at[pl.ds(r0, r), cols(y, col)], u2.at[rows_of(i, NIL, r), cols(y, col)], xrsem.at[i])
                 for i, (r0, r) in enumerate(zip(starts, chunks))]
    start(xr_copies)
    for t in range(n_o):
        o_part(t, NIL).start()

    for j in range(ONE, sp):
        sg(j).wait_recv()
    sgb[s] = seg_row[...]
    lane = lax.broadcasted_iota(jnp.int32, (rows, LANES), ONE).astype(F32)

    def seg_col(dev):
        return jnp.broadcast_to(sgb[dev, top(ONE), :], (LANES, rows)).T

    def key_cols(b):
        return aligned(yp * col + b * LANES, LANES)

    fq[...] = jnp.where(seg_col(s) == lane, 1.0, 0.0).astype(BF16)

    @pl.loop(NIL, sp)
    def _(b):
        u2[pl.ds(rows, rows), key_cols(b)] = jnp.where(seg_col(b) == lane, 0.0, -1e30).astype(BF16)

    def attend(h, i, g, b0, nb, own):
        nk = nb * rows
        both = lambda j: jnp.concatenate([hbuf[(b0 + d) * per_dev + TWO * g + j] for d in range(nb)], axis=NIL)
        q = jnp.concatenate([qb[h], fq[...]], axis=ONE)
        feat = jnp.concatenate([u2[pl.ds(rows, rows), key_cols(b0 + d)] for d in range(nb)], axis=NIL)
        k = jnp.concatenate([both(NIL), feat], axis=ONE)
        v = both(ONE)
        sc = lax.dot_general(q, k, (((ONE,), (ONE,)), ((), ())), preferred_element_type=F32)
        if own:
            lo = nk - rows
            a, b = (lax.broadcasted_iota(jnp.int32, (rows, rows), d) for d in range(TWO))
            tail = jnp.where(a >= b, sc[:, lo:], -1e30)
            sc = jnp.concatenate([sc[:, :lo], tail], axis=ONE) if lo else tail
        at = aligned(i * rows, rows)
        mx = jnp.max(sc, axis=ONE, keepdims=True)
        if own:
            mn = jnp.broadcast_to(mx, (rows, LANES))
        else:
            mn = jnp.maximum(xmid[group + i], mx)
            al = jnp.exp2((xmid[group + i] - mn) * scale2)
        ps = [jnp.exp2((sc[:, j * LANES:(j + ONE) * LANES] - mn) * scale2) for j in range(nk // LANES)]
        ls = functools.reduce(jnp.add, ps)
        o = jnp.dot(jnp.concatenate([p.astype(BF16) for p in ps], axis=ONE), v, preferred_element_type=F32)
        xmid[group + i] = mn
        if own:
            p_own[at, top(LANES)] = ls
            xmid[i] = o
        else:
            p_own[at, top(LANES)] = p_own[at, top(LANES)] * al + ls
            xmid[i] = xmid[i] * al + o

    def a_at(rank, h, r0, n):
        return attn.at[pl.ds(r0, n), aligned(rank * wide + h * hd, hd)]

    def a1(h, side):
        return remote(qb.at[h], a_at(y, h, NIL, rows), t_s.at[side, h], t_r.at[ONE - side, h], (to_p, to_m)[side])

    def a2(h, side):
        b = a_at((yp, ym)[side], h, (rows // TWO, NIL)[side], rows // TWO)
        return remote(b, b, v_s.at[side, h], v_r.at[side, h], (to_m, to_p)[side])

    def pass_on(h):
        for side in range(TWO):
            a1(h, ONE - side).wait_recv()
            a2(h, side).start()

    @pl.loop(NIL, n_kv)
    def _(g):
        @pl.when(g == NIL)
        def _():
            k_mid(NIL)
            k_start(ONE)

        kp(g, NIL).wait_recv()

        @pl.loop(NIL, group)
        def _(i):
            @pl.when(core == NIL)
            def _():
                attend(g * group + i, i, g, s, ONE, True)

            @pl.when(core == ONE)
            def _():
                attend(g * group + i, i, g, chip_at(NIL), TWO, True)

        k_last(g)
        for j in range(ONE, FOUR):
            kp(g, j).wait_recv()

        @pl.loop(NIL, group)
        def _(i):
            h = g * group + i

            @pl.loop(ONE, n_chip)
            def _(e):
                @pl.when(chip >= e)
                def _():
                    attend(h, i, g, chip_at(n_chip - e), TWO, False)

            total = jnp.sum(p_own[aligned(i * rows, rows), top(LANES)], axis=ONE, keepdims=True)
            qb[h] = (xmid[i] / total).astype(BF16)
            a1(h, NIL).start()
            a1(h, ONE).start()

            @pl.when(h == NIL)
            def _():
                k_mid(ONE)
                for b in range(tp - ONE):
                    w_start(b)

            for b in range(tp - TWO):
                @pl.when(h == heads - FOUR + b)
                def _():
                    w_mid(b)

            @pl.when(h >= TWO)
            def _():
                pass_on(h - TWO)

    mine_kv = s // (sp // n_kv)
    caches = [pltpu.make_async_copy(hbuf.at[d * per_dev + TWO * mine_kv + i], c.at[pl.ds(d * rows, rows)], csem.at[i, d])
              for i, c in enumerate((kc, vc)) for d in range(sp)]
    start(caches)
    pass_on(heads - TWO)
    w_mid(tp - TWO)
    pass_on(heads - ONE)

    def w_done(i):
        for j in range(FOUR):
            wp(i, j).wait_recv()
        for t in range(n_o):
            o_part(t, i + ONE).start()

    for g in range(n_kv):
        for j in range(FOUR):
            kp(g, j).wait_send()
        for side in range(TWO):
            k1(g, side).wait_send()
            k2(g, side).wait_send()
    wait(caches)

    def head_in(d, h):
        rank = (y + d) % tp
        return pltpu.make_async_copy(a_at(rank, h, NIL, rows), hbuf.at[rank * heads + h], lsem.at[d, h])

    for h in range(heads):
        hbuf[y * heads + h] = qb[h]
        head_in(ONE, h).start()
        head_in(THREE, h).start()

    for i in range(tp - ONE):
        w_last(i)
        if i:
            w_done(i - ONE)
    for h in range(heads):
        for side in range(TWO):
            a2(h, side).wait_recv()
        head_in(TWO, h).start()
    w_done(tp - TWO)
    for h in range(heads):
        for d in range(ONE, tp):
            head_in(d, h).wait()

    def wide_rows(r0, n):
        return jnp.concatenate([hbuf[b, pl.ds(r0, n)] for b in range(hbuf.shape[NIL])], axis=ONE)

    def front_sent():
        @pl.loop(NIL, heads)
        def _(h):
            for side in range(TWO):
                a1(h, side).wait_send()
                a2(h, side).wait_send()
        for i in range(tp - ONE):
            w1(i + ONE).wait_send()
            for j in range(FOUR):
                wp(i, j).wait_send()
            for side in range(TWO):
                w2(i, side).wait_send()
                w3(i, side).wait_send()
        for j in range(ONE, sp):
            sg(j).wait_send()

    n_g, n_d = ff // pair_w, nb * tp // FOUR

    def g_tile(n, slot, which):
        c = aligned(core * ff + n * pair_w, pair_w)
        return pltpu.make_async_copy((wg, wu)[which].at[:, c], wbuf.at[slot], wsem.at[slot, NIL])

    def g_pair(n, base):
        return [g_tile(n, (base + TWO * n + i) % slots, i) for i in range(TWO)]

    def d_cols(m):
        q = m // nb
        d = (TWO + THREE * q + THREE * (q * (q - ONE) // TWO)) % FOUR
        return aligned((y + d) % tp * col + m % nb * cb, cb)

    def d_tile(p, slot):
        return [pltpu.make_async_copy(wd.at[aligned(core * ff, ff), d_cols(TWO * p + i)],
                                      wbuf.at[slot, top(ff), pl.ds(i * cb, cb)], wsem.at[slot, i]) for i in range(TWO)]

    def d_pair(p, base):
        return [c for i in range(TWO) for c in d_tile(TWO * p + i, (base + TWO * p + i) % slots)]

    base = n_o

    lanes = srow.shape[-ONE]

    def stat(i, j):
        return remote(srow.at[i], sin.at[i, j], s_s.at[i, j], s_r.at[i, j], (to_p, to_m, to_2)[j])

    def x1_rows(i):
        r0, r = starts[i], chunks[i]
        def tile(t, w):
            v = jnp.dot(wide_rows(r0, r), wbuf[t, top(tp * part), top(w)], preferred_element_type=F32)
            for q in range(w // LANES):
                xmid[t * FOUR + q, pl.ds(r0, r)] = v[:, q * LANES:(q + ONE) * LANES]

        if not i:
            for t in range(n_o):
                wait([o_part(t, j) for j in range(tp)])

        @pl.loop(NIL, col // pair_w)
        def _(t):
            tile(t, pair_w)

        if col % pair_w:
            tile(n_o - ONE, col % pair_w)
        sq = jnp.zeros((r, LANES), F32)
        for b in range(col // LANES):
            v = xmid[b, pl.ds(r0, r)] + u2[rows_of(i, NIL, r), aligned(y * col + b * LANES, LANES)].astype(F32)
            xmid[b, pl.ds(r0, r)] = v
            sq += v * v
        tot = jnp.broadcast_to(jnp.sum(sq, axis=ONE, keepdims=True), (r, LANES))
        if r < lanes:
            tot = jnp.concatenate([tot, jnp.zeros((lanes - r, LANES), F32)], axis=NIL)
        srow[i] = tot.T[:SUB, :]
        for j in range(tp - ONE):
            stat(i, j).start()

    def norm_rows(i):
        r0, r = starts[i], chunks[i]
        for j in range(tp - ONE):
            stat(i, j).wait()
        tot = srow[i]
        for j in range(tp - ONE):
            tot += sin[i, j]
        inv = lax.rsqrt(tot * (1.0 / dim) + NORM_EPS)
        inv = jnp.broadcast_to(inv[:ONE, :], (LANES, lanes)).T[:r, :]
        for b in range(col // LANES):
            c = aligned(y * col + b * LANES, LANES)
            u2[rows_of(i, NIL, r), c] = (xmid[b, pl.ds(r0, r)] * inv * gain_m[:, c]).astype(BF16)

    def u_blk(i, row0, n_rows, rank):
        return u2.at[rows_of(i, row0, n_rows), cols(rank, col)]

    def u_first(i, side, turn):
        h = chunks[i] // TWO
        b = u_blk(i, h * (side + turn - TWO * side * turn), h, y)
        return remote(b, b, u1s.at[i, side, turn], u1r.at[i, ONE - side, turn], (to_p, to_m)[side])

    def u_second(i, side):
        h = chunks[i] // TWO
        b = u_blk(i, h, h, yp) if side == NIL else u_blk(i, NIL, h, ym)
        return remote(b, b, u2s.at[i, side], u2r.at[i, side], (to_m, to_p)[side])

    def u_pair(i, j):
        r, rank = chunks[i], (y, yp, ym, y2)[j]
        return remote(u_blk(i, NIL, r, rank), u_blk(i, r, r, rank), ups.at[i, j], upr.at[i, j], to_pair)

    def u_start(i):
        for turn in range(TWO):
            u_first(i, NIL, turn).start()
            u_first(i, ONE, turn).start()
        u_pair(i, NIL).start()

    def u_mid(i):
        for side in range(TWO):
            u_first(i, ONE - side, NIL).wait_recv()
            u_second(i, side).start()

    def u_near(i):
        for side in range(TWO):
            u_first(i, ONE - side, ONE).wait_recv()
            u_pair(i, ONE + side).start()

    def u_far(i):
        for side in range(TWO):
            u_second(i, side).wait_recv()
        u_pair(i, THREE).start()

    def u_last(i):
        u_near(i)
        u_far(i)

    def u_ready(i):
        for j in range(FOUR):
            u_pair(i, j).wait_recv()

    def u_drain(i):
        for side in range(TWO):
            for turn in range(TWO):
                u_first(i, side, turn).wait_send()
            u_second(i, side).wait_send()
        for j in range(FOUR):
            u_pair(i, j).wait_send()

    def blk_rows(m, row0, n):
        return pl.ds(pl.multiple_of(m * max(chunks) + row0, EIGHT), n)

    def d_copy(i, m, slot):
        r, par = chunks[i], i % TWO
        return remote(p_out.at[slot, top(r)], d_in.at[par, m, top(r)], d_s.at[slot], d_r.at[par, m], to_pair)

    def t_add(i, m):
        r, par = chunks[i], i % TWO
        d_copy(i, m, NIL).wait_recv()
        p_own[blk_rows(m, NIL, r), :] += d_in[par, m, top(r)]

    def f_copy(i, k, side):
        h, par = chunks[i] // TWO, i % TWO
        return remote(p_own.at[blk_rows(k, side * h, h)], f_in.at[par, side, k, top(h)],
                      f_s.at[side, k], f_r.at[par, side, k], (to_m, to_p)[side])

    def t_f(i, k):
        f_copy(i, k, NIL).start()
        f_copy(i, k, ONE).start()

    def e_copy(i, k, side):
        r, par = chunks[i], i % TWO
        return remote(p_own.at[blk_rows((TWO - side) * nb + k, NIL, r)], e_in.at[par, side, k, top(r)],
                      e_s.at[side, k], e_r.at[par, side, k], (to_m, to_p)[side])

    def t_e(i, k, side):
        h, par = chunks[i] // TWO, i % TWO
        f_copy(i, k, side).wait_recv()
        p_own[blk_rows((TWO - side) * nb + k, side * h, h), :] += f_in[par, side, k, top(h)]
        e_copy(i, k, side).start()

    def y_at(i, row0, n_rows, rank, k):
        return y_hbm.at[pl.ds(starts[i] + row0, n_rows), aligned(rank * col + k * cb, cb)]

    def a_copy_y(i, k, side):
        r, par = chunks[i], i % TWO
        return remote(ystage.at[par, k, top(r)], y_at(i, NIL, r, y, k), a_s.at[par, side, k], a_r.at[par, ONE - side, k],
                      (to_p, to_m)[side])

    def a_local(i, k):
        r, par = chunks[i], i % TWO
        return pltpu.make_async_copy(ystage.at[par, k, top(r)], y_at(i, NIL, r, y, k), a_l.at[par, k])

    def h_copy(i, k, side):
        h = chunks[i] // TWO
        b = y_at(i, h, h, yp, k) if side == NIL else y_at(i, NIL, h, ym, k)
        return remote(b, b, h_s.at[i, side, k], h_r.at[i, side, k], (to_m, to_p)[side])

    def t_final(i, k):
        r, par = chunks[i], i % TWO
        for side in range(TWO):
            e_copy(i, k, side).wait_recv()
        v = (p_own[blk_rows(THREE * nb + k, NIL, r), :] + e_in[par, NIL, k, top(r)] + e_in[par, ONE, k, top(r)]
             + jnp.concatenate([xmid[TWO * k + q, pl.ds(starts[i], r)] for q in range(TWO)], axis=ONE))
        ystage[par, k, top(r)] = v.astype(BF16)
        for side in range(TWO):
            a_copy_y(i, k, side).start()
        a_local(i, k).start()

    def t_fwd(i, k):
        for side in range(TWO):
            a_copy_y(i, k, ONE - side).wait_recv()
            h_copy(i, k, side).start()

    def sums_sent(i):
        for k in range(nb):
            for side in range(TWO):
                f_copy(i, k, side).wait_send()
                e_copy(i, k, side).wait_send()

    def rows_done(i):
        for k in range(nb):
            for side in range(TWO):
                h_copy(i, k, side).wait_recv()
                h_copy(i, k, side).wait_send()
                a_copy_y(i, k, side).wait_send()
            a_local(i, k).wait()

    g_tile(NIL, base, NIL).start()
    wait(xr_copies)
    x1_rows(NIL)
    x1_rows(n_ch - ONE)
    norm_rows(NIL)
    u_start(NIL)
    for i in range(ONE, n_ch - ONE):
        x1_rows(i)
    g_tile(NIL, NIL, ONE).start()
    start(g_pair(ONE, base))
    norm_rows(n_ch - ONE)
    u_mid(NIL)
    front_sent()
    u_near(NIL)
    for i in range(ONE, n_ch - ONE):
        norm_rows(i)
    u_start(ONE)
    for j in range(THREE):
        u_pair(NIL, j).wait_recv()

    def gate_up(q, ranks):
        return functools.reduce(jnp.add, [
            jnp.dot(u2[rows_of(NIL, NIL, TWO * chunks[NIL]), cols(rank, col)], wbuf[(base + q) % slots, cols(rank, col)],
                    preferred_element_type=F32) for rank in ranks])

    def put_hidden(i, j, g, u):
        g = (jax.nn.silu(g) * u).astype(BF16)
        for q in range(FOUR):
            hbuf[FOUR * j + q, top(TWO * chunks[i])] = g[:, q * LANES:(q + ONE) * LANES]

    wait(g_pair(NIL, base))
    r = chunks[NIL]

    @pl.loop(NIL, TWO)
    def _(q):
        v = gate_up(q, (y, yp, ym))
        for a in range(TWO):
            for b in range(TWO):
                d_in[ONE, FOUR * q + TWO * a + b, top(r)] = v[a * r:(a + ONE) * r, b * cb:(b + ONE) * cb]

    u_far(NIL)
    u_pair(NIL, THREE).wait_recv()
    part_sums = [jnp.concatenate([jnp.concatenate([d_in[ONE, FOUR * q + TWO * a + b, top(r)] for b in range(TWO)], axis=ONE)
                                  for a in range(TWO)], axis=NIL) for q in range(TWO)]
    put_hidden(NIL, NIL, *[part_sums[q] + gate_up(q, (y2,)) for q in range(TWO)])

    def t_own(i):
        for q in range(FOUR):
            t_add(i, FOUR * (n_d - ONE) + q)

    tasks = {"own": t_own, "mid": u_mid, "last": u_last, "start": u_start, "e": t_e, "final": t_final, "fwd": t_fwd}

    def run(todo, at):
        for when, name, *args in todo:
            @pl.when(at == when)
            def _():
                tasks[name](*args)

    for i in range(n_ch):
        r = chunks[i]
        g_base, d_base = base % slots, (base + TWO * n_g) % slots
        base += TWO * (n_g + n_d)

        @pl.loop(NIL if i else ONE, n_g)
        def _(j):
            @pl.when(j + ONE < n_g)
            def _():
                start(g_pair(j + ONE, g_base))

            @pl.when(j + ONE >= n_g)
            def _():
                start(d_pair(NIL, d_base))

            wait(g_pair(j, g_base))
            put_hidden(i, j, *[jnp.dot(u2[rows_of(i, NIL, TWO * r), :], wbuf[(g_base + TWO * j + q) % slots],
                                       preferred_element_type=F32) for q in range(TWO)])
            run(plan[i][NIL], j)

        if i:
            sums_sent(i - ONE)

        @pl.loop(NIL, n_d)
        def _(p):
            @pl.when(p + ONE < n_d)
            def _():
                start(d_pair(p + ONE, d_base))

            if i + ONE < n_ch:
                @pl.when(p + ONE >= n_d)
                def _():
                    start(g_pair(NIL, base % slots))

            wait(d_pair(p, d_base))
            out = p % TWO * FOUR

            @pl.when(p >= TWO)
            def _():
                for q in range(FOUR):
                    d_copy(i, q, out + q).wait_send()

            if i:
                @pl.when(p < TWO)
                def _():
                    for q in range(FOUR):
                        d_copy(i - ONE, q, out + q).wait_send()

            for q in range(TWO):
                v = jnp.dot(wide_rows(NIL, TWO * r), wbuf[(d_base + TWO * p + q) % slots, top(ff)],
                            preferred_element_type=F32)
                for e in range(TWO):
                    b = TWO * q + e
                    p_own[blk_rows(FOUR * p + b, NIL, r), :] = v[:r, e * cb:(e + ONE) * cb]
                    p_out[out + b, top(r)] = v[r:, e * cb:(e + ONE) * cb]
            for q in range(FOUR):
                d_copy(i, FOUR * p + q, out + q).start()

            @pl.when(p >= ONE)
            def _():
                for q in range(FOUR):
                    t_add(i, FOUR * (p - ONE) + q)

            @pl.when(p == ONE)
            def _():
                for k in range(FOUR):
                    t_f(i, k)

            @pl.when(p == TWO)
            def _():
                for k in range(FOUR, nb):
                    t_f(i, k)
            run(plan[i][ONE], p)

        if i + ONE == n_ch:
            for q in range(FOUR):
                t_add(i, FOUR * (n_d - ONE) + q)
            for q in range(EIGHT):
                d_copy(i, q, q).wait_send()
        for name, *args in plan[i][TWO]:
            tasks[name](*args)
        if i + ONE < n_ch:
            u_ready(i + ONE)

    last = n_ch - ONE
    if last >= TWO:
        rows_done(last - TWO)
    for k in range(nb):
        t_final(last, k)
        if k >= TWO:
            t_fwd(last, k - TWO)
    for k in range(nb - TWO, nb):
        t_fwd(last, k)
    for i in range(max(last - ONE, NIL), n_ch):
        rows_done(i)
    sums_sent(last)
    for i in range(n_ch):
        u_drain(i)


CHUNKS = (192, 192, 128)


def mlp_plan():
    early = lambda i: [(3, "e", i, 0, 1), (3, "e", i, 1, 1), (4, "e", i, 2, 1), (4, "e", i, 0, 0), (4, "e", i, 1, 0)]
    late = lambda i: [("e", i, 3, 1), ("e", i, 2, 0), ("e", i, 4, 1), ("e", i, 3, 0), ("e", i, 4, 0)]
    at_start = lambda i: [(0, *t) for t in late(i)] + [(0, "own", i)]
    finals = lambda i, at: [(a, "final", i, k) for k, a in enumerate(at)]
    passed = lambda i, at: [(a, "fwd", i, k) for k, a in enumerate(at)]
    gather = [(1, "mid", 1), (1, "start", 2), (3, "last", 1), (4, "mid", 2), (6, "last", 2)]
    return ((gather, early(0), ()),
            (at_start(0) + finals(0, (1, 2, 3, 4, 5)) + passed(0, (5, 6, 6, 6, 7)), early(1), ()),
            (at_start(1) + finals(1, (2, 3, 4, 6, 7)), passed(1, (0, 1, 1, 2, 2)) + early(2), late(2)))


def layer_call(x_in, positions, segments, gain_a, gain_m, wq, wk, wv, wo, wg, wu, wd):
    rows, dim = x_in.shape
    tp, sp = lax.axis_size("tp"), lax.axis_size("sp")
    heads, n_kv = wq.shape[ONE] // HEAD_DIM, wk.shape[ONE] // HEAD_DIM
    cb = TWO * LANES
    col, ff = dim // tp, wg.shape[ONE] // TWO
    nb = col // cb
    n_ch, rm = len(CHUNKS), max(CHUNKS)
    lanes = -(-rm // LANES) * LANES
    half_dim = np.arange(HEAD_DIM) % (HEAD_DIM // TWO)
    freq = jnp.asarray((ROPE_BASE ** (-half_dim * (2.0 / HEAD_DIM))).astype(np.float32)[None])
    dma = pltpu.SemaphoreType.DMA
    hbm, vmem = pl.BlockSpec(memory_space=pl.ANY), pl.BlockSpec(memory_space=pltpu.VMEM)
    bufs = [((FOUR, dim, TWO * cb), BF16), ((TWO * rows, dim), BF16), ((ff // LANES, rows, LANES), BF16),
            ((heads, rows, HEAD_DIM), BF16), ((rows, HEAD_DIM), F32), ((rows, HEAD_DIM), F32), ((SUB, rows), F32), ((sp, SUB, rows), F32), ((rows, LANES), BF16),
            ((col // LANES, rows, LANES), F32), ((n_ch, SUB, lanes), F32), ((n_ch, tp - ONE, SUB, lanes), F32),
            ((tp * nb * rm, cb), F32), ((EIGHT, rm, cb), F32), ((TWO, tp * nb, rm, cb), F32),
            ((TWO, TWO, nb, rm // TWO, cb), F32), ((TWO, TWO, nb, rm, cb), F32), ((TWO, nb, rm, cb), BF16)]
    sems = [(FOUR,), (FOUR, TWO), (sp,), (sp,)] + [(n_kv, TWO)] * FOUR + [(n_kv, FOUR)] * TWO + [(tp - ONE,)] * TWO
    sems += [(tp - ONE, TWO)] * FOUR + [(tp - ONE, FOUR)] * TWO + [(TWO, heads)] * FOUR + [(TWO, sp), (tp, heads), (THREE, tp), (n_ch,)]
    sems += [(n_ch, tp - ONE)] * TWO + [(n_ch, TWO, TWO)] * TWO + [(n_ch, TWO)] * TWO + [(n_ch, FOUR)] * TWO
    sems += [(EIGHT,), (TWO, tp * nb)] + [(TWO, nb), (TWO, TWO, nb)] * TWO + [(TWO, nb)] + [(TWO, TWO, nb)] * TWO
    sems += [(n_ch, TWO, nb)] * TWO
    cache = jax.ShapeDtypeStruct((sp * rows, HEAD_DIM), BF16)
    kc, vc, _, _, y_out = pl.pallas_call(
        functools.partial(layer_kernel, CHUNKS, cb, mlp_plan()), name="layer",
        out_shape=[cache, cache, jax.ShapeDtypeStruct((rows, tp * heads * HEAD_DIM), BF16), jax.ShapeDtypeStruct((tp - ONE, wo.shape[NIL], col), BF16),
                   jax.ShapeDtypeStruct((rows, dim), BF16)],
        in_specs=[hbm] + [vmem] * (FOUR + ONE) + [hbm] * (FOUR + THREE), out_specs=[hbm] * (FOUR + ONE),
        scratch_shapes=[pltpu.VMEM(*b) for b in bufs] + [dma(q) for q in sems],
        compiler_params=pltpu.CompilerParams(collective_id=ONE, has_side_effects=True, vmem_limit_bytes=VMEM_BYTES),
    )(x_in, segments.reshape(ONE, rows), positions.reshape(ONE, rows), freq, gain_a.reshape(ONE, dim), gain_m.reshape(ONE, dim),
      wq, wk, wv, wo, wg, wu, wd)
    return copy_out(y_out, kc, vc)


def copy_kernel(*refs):
    n = len(refs) // FOUR
    ins, outs, bufs, sems = (refs[i * n:(i + ONE) * n] for i in range(FOUR))

    def parts(src, dst, sem):
        step = src.shape[NIL] // sem.shape[ONE]
        return [(src.at[pl.ds(k * step, step)], dst.at[pl.ds(k * step, step)], k) for k in range(sem.shape[ONE])]

    for a, b, sem in zip(ins, bufs, sems):
        start([pltpu.make_async_copy(x, v, sem.at[NIL, k]) for x, v, k in parts(a, b, sem)])
    for a, b, o, sem in zip(ins, bufs, outs, sems):
        for (x, v, k), (_, d, _) in zip(parts(a, b, sem), parts(b, o, sem)):
            pltpu.make_async_copy(x, v, sem.at[NIL, k]).wait()
            pltpu.make_async_copy(v, d, sem.at[ONE, k]).start()
    for b, o, sem in zip(bufs, outs, sems):
        wait([pltpu.make_async_copy(v, d, sem.at[ONE, k]) for v, d, k in parts(b, o, sem)])


def copy_out(*arrays):
    hbm = pl.BlockSpec(memory_space=pl.ANY)
    return pl.pallas_call(
        copy_kernel, name="copy_out", out_shape=[jax.ShapeDtypeStruct(a.shape, a.dtype) for a in arrays],
        in_specs=[hbm] * len(arrays), out_specs=[hbm] * len(arrays),
        scratch_shapes=[pltpu.VMEM(a.shape, a.dtype) for a in arrays] + [pltpu.SemaphoreType.DMA((TWO, FOUR)) for _ in arrays],
        compiler_params=pltpu.CompilerParams(vmem_limit_bytes=VMEM_BYTES),
    )(*arrays)


def solution(mesh):
    row_spec = P(("rep", "sp"), None)
    tok_spec = P(("rep", "sp"))
    full_spec = P(None)
    col_spec = P(None, "tp")
    wrow_spec = P("tp", None)
    cache_spec = P("rep", ("tp", "sp"), None)

    def local_layer(x_in, positions, segments, gain_attn, w_q, w_k, w_v, w_o, gain_mlp, w_gate, w_up, w_down):
        y_out, kc, vc = layer_call(x_in, positions, segments, gain_attn, gain_mlp, w_q, w_k, w_v, w_o, w_gate, w_up, w_down)
        return y_out, kc.reshape(-1, 1, HEAD_DIM), vc.reshape(-1, 1, HEAD_DIM)

    return jax.shard_map(local_layer, mesh=mesh,
                         in_specs=(row_spec, tok_spec, tok_spec, full_spec, col_spec, col_spec, col_spec, wrow_spec,
                                   full_spec, col_spec, col_spec, wrow_spec),
                         out_specs=(row_spec, cache_spec, cache_spec), check_vma=False)
```

```python
import functools

import jax
import jax.numpy as jnp
from jax import lax
from jax.experimental import pallas as pl
from jax.experimental.pallas import tpu as pltpu
from jax.sharding import PartitionSpec as P

HEAD_DIM = 128
ROPE_BASE = 500000.0
NORM_EPS = 1e-5
MESH = pl.DeviceIdType.MESH
BF16, F32 = jnp.bfloat16, jnp.float32
VMEM_BYTES = 67043328
NIL, ONE, TWO, THREE, FOUR, EIGHT, SUB, LANES = 0, 1, 2, 3, 4, 8, 8, 128


def remote(src, dst, send_sem, recv_sem, to):
    return pltpu.make_async_remote_copy(src, dst, send_sem, recv_sem, device_id=to, device_id_type=MESH)


def start(copies):
    for c in copies:
        c.start()


def wait(copies):
    for c in copies:
        c.wait()


def top(n):
    return pl.ds(NIL, n)


def aligned(offset, n):
    return pl.ds(pl.multiple_of(offset, LANES), n)


def layer_kernel(chunks, cb, plan, x_hbm, seg, pos, freq, gain_a, gain_m, wq, wk, wv, wo, wg, wu, wd,
                 kc, vc, wo_g, y_hbm,
                 wbuf, u2, hbuf, qb, rope_c, rope_s, seg_row, sgb, fq, xmid, srow, sin, p_own, p_out, d_in, f_in, e_in, ystage,
                 xsem, wsem, sg_s, sg_r, k1s, k1r, k2s, k2r, kps, kpr, w1s, w1r, w2s, w2r, w3s, w3r, wps, wpr,
                 t_s, t_r, v_s, v_r, csem, osem, xrsem,
                 s_s, s_r, u1s, u1r, u2s, u2r, ups, upr, d_s, d_r, f_s, f_r, e_s, e_r, a_l, a_s, a_r, h_s, h_r):
    rows, dim = x_hbm.shape
    tp, sp = lax.axis_size("tp"), lax.axis_size("sp")
    hd = HEAD_DIM
    heads = wq.shape[ONE] // hd
    n_kv = wk.shape[ONE] // hd
    group = heads // n_kv
    wide = heads * hd
    col, wrow = dim // tp, wo.shape[NIL] // sp
    half = wrow // TWO
    nb = col // cb
    pair_w = TWO * cb
    ff = wg.shape[ONE] // TWO
    slots = wbuf.shape[NIL]
    per_dev = TWO * n_kv
    y, s = lax.axis_index("tp"), lax.axis_index("sp")
    core, chip, n_chip = s % TWO, s // TWO, sp // TWO
    yp, ym, y2 = (y + ONE) % tp, (y + tp - ONE) % tp, (y + TWO) % tp
    chip_at = lambda d: (chip + d) % n_chip * TWO
    up, dn, far = (chip_at(d) + core for d in (ONE, n_chip - ONE, TWO))
    pair = s + ONE - TWO * core
    to_pair, to_up, to_dn = ({"tp": y, "sp": d} for d in (pair, up, dn))
    to_p, to_m, to_2 = ({"tp": d, "sp": s} for d in (yp, ym, y2))
    scale2 = HEAD_DIM ** -0.5 * 1.4426950408889634

    kw = n_kv * hd
    n_x = xsem.shape[NIL]
    x_rows = rows // n_x
    x_copies = [pltpu.make_async_copy(x_hbm.at[pl.ds(i * x_rows, x_rows)], u2.at[pl.ds(i * x_rows, x_rows)], xsem.at[i])
                for i in range(n_x)]
    start(x_copies)
    kv_copies = [pltpu.make_async_copy(w, wbuf.at[NIL, :, pl.ds(i * kw, kw)], wsem.at[NIL, i]) for i, w in enumerate((wk, wv))]

    def q_copy(t):
        return pltpu.make_async_copy(wq.at[:, aligned(t * TWO * kw, TWO * kw)], wbuf.at[ONE + t], wsem.at[ONE + t, NIL])

    barrier = pltpu.get_barrier_semaphore()
    for j in range(ONE, sp):
        pl.semaphore_signal(barrier, inc=ONE, device_id={"tp": y, "sp": (s + j) % sp}, device_id_type=MESH)
    for j in range(ONE, tp):
        pl.semaphore_signal(barrier, inc=ONE, device_id={"tp": (y + j) % tp, "sp": s}, device_id_type=MESH)

    def norm(i):
        x_copies[i].wait()
        step = x_rows // TWO

        @pl.loop(NIL, TWO)
        def _(j):
            rr = pl.ds(pl.multiple_of(i * x_rows + j * step, step), step)
            sq = jnp.zeros((step, LANES), F32)
            for b in range(dim // LANES):
                v = u2[rr, pl.ds(b * LANES, LANES)].astype(F32)
                sq += v * v
            inv = lax.rsqrt(jnp.sum(sq, axis=ONE, keepdims=True) * (1.0 / dim) + NORM_EPS)
            for b in range(dim // LANES):
                c = pl.ds(b * LANES, LANES)
                u2[rr, c] = (u2[rr, c].astype(F32) * inv * gain_a[:, c]).astype(BF16)

    seg_row[...] = jnp.broadcast_to(seg[...].astype(F32), (SUB, rows))
    norm(NIL)
    start(kv_copies)
    norm(ONE)
    pl.semaphore_wait(barrier, sp + tp - TWO)

    def w1(j):
        rank, mine = (y + j) % tp, aligned(s * wrow, wrow)
        return remote(wo.at[mine, aligned(rank * col, col)], wo_g.at[tp - ONE - j, mine],
                      w1s.at[j - ONE], w1r.at[tp - ONE - j], {"tp": rank, "sp": s})

    def sg(j):
        return remote(seg_row, sgb.at[s], sg_s.at[j], sg_r.at[j], {"tp": y, "sp": (s + j) % sp})

    for j in range(ONE, sp):
        sg(j).start()
    for j in range(ONE, tp):
        w1(j).start()

    def w_blk(i, dev, r0, n):
        return wo_g.at[i, pl.ds(pl.multiple_of(dev * wrow + r0, half), n)]

    def w2(i, side):
        b = w_blk(i, s, NIL, wrow)
        return remote(b, b, w2s.at[side], w2r.at[i, ONE - side], (to_up, to_dn)[side])

    def w3(i, side):
        b = w_blk(i, (up, dn)[side], (half, NIL)[side], half)
        return remote(b, b, w3s.at[side], w3r.at[i, side], (to_dn, to_up)[side])

    def wp(i, j):
        b = w_blk(i, (s, up, dn, far)[j], NIL, wrow)
        return remote(b, b, wps.at[j], wpr.at[i, j], to_pair)

    def w_start(i):
        w1(tp - ONE - i).wait_recv()
        w2(i, NIL).start()
        w2(i, ONE).start()
        wp(i, NIL).start()

    def w_mid(i):
        for side in range(TWO):
            w2(i, ONE - side).wait_recv()
            w3(i, side).start()
            wp(i, ONE + side).start()

    def w_last(i):
        w3(i, NIL).wait_recv()
        w3(i, ONE).wait_recv()
        wp(i, THREE).start()

    q_copy(NIL).start()
    q_copy(ONE).start()
    for i in range(TWO, n_x):
        norm(i)

    def rope(t):
        return (t * rope_c[...] + pltpu.roll(t, hd // TWO, ONE) * rope_s[...]).astype(BF16)

    wait(kv_copies)
    angles = jnp.broadcast_to(pos[...].astype(F32), (LANES, rows)).T * freq[...]
    sign = jnp.where(lax.broadcasted_iota(jnp.int32, (rows, hd), ONE) < hd // TWO, -1.0, 1.0)
    rope_c[...] = jnp.cos(angles)
    rope_s[...] = jnp.sin(angles) * sign
    r = jnp.dot(u2[top(rows), :], wbuf[NIL], preferred_element_type=F32)
    for g in range(n_kv):
        hbuf[s * per_dev + TWO * g] = rope(r[:, g * hd:(g + ONE) * hd])
        hbuf[s * per_dev + TWO * g + ONE] = r[:, kw + g * hd:kw + (g + ONE) * hd].astype(BF16)

    def k_blk(dev, g, lo=NIL, n=TWO):
        return hbuf.at[pl.ds(dev * per_dev + TWO * g + lo, n)]

    def k1(g, side):
        b = k_blk(s, g)
        return remote(b, b, k1s.at[g, side], k1r.at[g, ONE - side], (to_up, to_dn)[side])

    def k2(g, side):
        b = k_blk((up, dn)[side], g, ONE - side, ONE)
        return remote(b, b, k2s.at[g, side], k2r.at[g, side], (to_dn, to_up)[side])

    def kp(g, j):
        b = k_blk((s, up, dn, far)[j], g)
        return remote(b, b, kps.at[g, j], kpr.at[g, j], to_pair)

    def k_start(g):
        k1(g, NIL).start()
        k1(g, ONE).start()
        kp(g, NIL).start()

    def k_mid(g):
        for side in range(TWO):
            k1(g, ONE - side).wait_recv()
            k2(g, side).start()
            kp(g, ONE + side).start()

    def k_last(g):
        k2(g, NIL).wait_recv()
        k2(g, ONE).wait_recv()
        kp(g, THREE).start()

    k_start(NIL)

    @pl.loop(NIL, TWO)
    def _(t):
        q_copy(t).wait()
        r = jnp.dot(u2[top(rows), :], wbuf[ONE + t], preferred_element_type=F32)
        for g in range(heads // TWO):
            qb[t * (heads // TWO) + g] = rope(r[:, g * hd:(g + ONE) * hd])

    n_o = -(-col // pair_w)
    part = wide
    starts = [sum(chunks[:i]) for i in range(len(chunks))]
    n_ch = len(chunks)

    def cols(block, width):
        return aligned(block * width, width)

    def o_width(t):
        return min(pair_w, col - t * pair_w)

    def o_part(t, j):
        w = o_width(t)
        src = wo_g.at[j - ONE, :, pl.ds(t * pair_w, w)] if j else wo.at[:, aligned(y * col + t * pair_w, w)]
        return pltpu.make_async_copy(src, wbuf.at[t, aligned((y + j) % tp * part, part), top(w)], osem.at[t, j])

    def rows_of(i, row0, n):
        return pl.ds(TWO * starts[i] + row0, n)

    xr_copies = [pltpu.make_async_copy(x_hbm.at[pl.ds(r0, r), cols(y, col)], u2.at[rows_of(i, NIL, r), cols(y, col)], xrsem.at[i])
                 for i, (r0, r) in enumerate(zip(starts, chunks))]
    start(xr_copies)
    for t in range(n_o):
        o_part(t, NIL).start()

    for j in range(ONE, sp):
        sg(j).wait_recv()
    sgb[s] = seg_row[...]
    lane = lax.broadcasted_iota(jnp.int32, (rows, LANES), ONE).astype(F32)

    def seg_col(dev):
        return jnp.broadcast_to(sgb[dev, top(ONE), :], (LANES, rows)).T

    def key_cols(b):
        return aligned(yp * col + b * LANES, LANES)

    fq[...] = jnp.where(seg_col(s) == lane, 1.0, 0.0).astype(BF16)

    @pl.loop(NIL, sp)
    def _(b):
        u2[pl.ds(rows, rows), key_cols(b)] = jnp.where(seg_col(b) == lane, 0.0, -1e30).astype(BF16)

    def attend(h, i, g, b0, nb, own):
        nk = nb * rows
        both = lambda j: jnp.concatenate([hbuf[(b0 + d) * per_dev + TWO * g + j] for d in range(nb)], axis=NIL)
        q = jnp.concatenate([qb[h], fq[...]], axis=ONE)
        feat = jnp.concatenate([u2[pl.ds(rows, rows), key_cols(b0 + d)] for d in range(nb)], axis=NIL)
        k = jnp.concatenate([both(NIL), feat], axis=ONE)
        v = both(ONE)
        sc = lax.dot_general(q, k, (((ONE,), (ONE,)), ((), ())), preferred_element_type=F32)
        if own:
            lo = nk - rows
            a, b = (lax.broadcasted_iota(jnp.int32, (rows, rows), d) for d in range(TWO))
            tail = jnp.where(a >= b, sc[:, lo:], -1e30)
            sc = jnp.concatenate([sc[:, :lo], tail], axis=ONE) if lo else tail
        at = aligned(i * rows, rows)
        mx = jnp.max(sc, axis=ONE, keepdims=True)
        if own:
            mn = jnp.broadcast_to(mx, (rows, LANES))
        else:
            mn = jnp.maximum(xmid[group + i], mx)
            al = jnp.exp2((xmid[group + i] - mn) * scale2)
        ps = [jnp.exp2((sc[:, j * LANES:(j + ONE) * LANES] - mn) * scale2) for j in range(nk // LANES)]
        ls = functools.reduce(jnp.add, ps)
        o = jnp.dot(jnp.concatenate([p.astype(BF16) for p in ps], axis=ONE), v, preferred_element_type=F32)
        xmid[group + i] = mn
        if own:
            p_own[at, top(LANES)] = ls
            xmid[i] = o
        else:
            p_own[at, top(LANES)] = p_own[at, top(LANES)] * al + ls
            xmid[i] = xmid[i] * al + o

    def a_at(rank, h, r0, n):
        b = rank * heads + h
        return wbuf.at[slots - ONE, pl.ds(pl.multiple_of(b // FOUR * rows + r0, LANES), n), aligned(b % FOUR * hd, hd)]

    def a1(h, side):
        return remote(qb.at[h], a_at(y, h, NIL, rows), t_s.at[side], t_r.at[ONE - side, h], (to_p, to_m)[side])

    def a2(h, side):
        b = a_at((yp, ym)[side], h, (rows // TWO, NIL)[side], rows // TWO)
        return remote(b, b, v_s.at[side], v_r.at[side], (to_m, to_p)[side])

    def pass_on(h):
        for side in range(TWO):
            a1(h, ONE - side).wait_recv()
            a2(h, side).start()

    @pl.loop(NIL, n_kv)
    def _(g):
        @pl.when(g == NIL)
        def _():
            k_mid(NIL)
            k_start(ONE)

        kp(g, NIL).wait_recv()

        def own_keys(i):
            @pl.when(core == NIL)
            def _():
                attend(g * group + i, i, g, s, ONE, True)

            @pl.when(core == ONE)
            def _():
                attend(g * group + i, i, g, chip_at(NIL), TWO, True)

        @pl.when(g == NIL)
        def _():
            pl.loop(NIL, group)(own_keys)
            w_start(NIL)

        k_last(g)
        for j in range(ONE, FOUR):
            kp(g, j).wait_recv()

        @pl.loop(NIL, group)
        def _(i):
            h = g * group + i

            @pl.when(g > NIL)
            def _():
                own_keys(i)

            @pl.loop(ONE, n_chip)
            def _(e):
                @pl.when(chip >= e)
                def _():
                    attend(h, i, g, chip_at(n_chip - e), TWO, False)

            total = jnp.sum(p_own[aligned(i * rows, rows), top(LANES)], axis=ONE, keepdims=True)
            qb[h] = (xmid[i] / total).astype(BF16)
            a1(h, NIL).start()
            a1(h, ONE).start()

            @pl.when(h == NIL)
            def _():
                k_mid(ONE)
                for b in range(ONE, tp - ONE):
                    w_start(b)

            for b in range(tp - TWO):
                @pl.when(h == heads - FOUR + b)
                def _():
                    w_mid(b)

            @pl.when(h >= TWO)
            def _():
                pass_on(h - TWO)

    mine_kv = s // (sp // n_kv)
    caches = [pltpu.make_async_copy(hbuf.at[d * per_dev + TWO * mine_kv + i], c.at[pl.ds(d * rows, rows)], csem.at[i, d])
              for i, c in enumerate((kc, vc)) for d in range(sp)]
    start(caches)
    w_mid(tp - TWO)
    pass_on(heads - TWO)

    def w_done(i):
        for j in range(FOUR):
            wp(i, j).wait_recv()
        for t in range(n_o):
            o_part(t, i + ONE).start()

    for i in range(tp - ONE):
        if i == tp - TWO:
            pass_on(heads - ONE)
        w_last(i)
    for i in range(tp - TWO):
        w_done(i)
    for h in range(heads):
        b = y * heads + h
        wbuf[slots - ONE, aligned(b // FOUR * rows, rows), aligned(b % FOUR * hd, hd)] = qb[h]

    def all_heads(side, n, send, recv):
        b = qb.at[:, top(n)]
        return remote(b, b, send.at[side], recv.at[side], to_p)

    for side in range(TWO):
        all_heads(side, rows // TWO, v_s, v_r).wait_recv()
        all_heads(side, rows // TWO, v_s, v_r).wait_send()
    w_done(tp - TWO)

    def attn_rows(r0, n):
        return jnp.concatenate([wbuf[slots - ONE, pl.ds(b * rows + r0, n), :] for b in range(tp * heads // FOUR)], axis=ONE)

    def wide_rows(n):
        return jnp.concatenate([hbuf[b, top(n)] for b in range(hbuf.shape[NIL])], axis=ONE)

    def front_sent():
        for g in range(n_kv):
            for j in range(FOUR):
                kp(g, j).wait_send()
            for side in range(TWO):
                k1(g, side).wait_send()
                k2(g, side).wait_send()
        wait(caches)
        for side in range(TWO):
            all_heads(side, rows, t_s, v_r).wait_send()
        for n, send, recv in ((wrow, wps, wpr), (wrow, w2s, w2r), (half, w3s, w3r)):
            b = wo_g.at[:, top(n)]
            for j in range(send.shape[NIL]):
                remote(b, b, send.at[j], recv.at[NIL, NIL], to_p).wait_send()
        for i in range(tp - ONE):
            w1(i + ONE).wait_send()
        for j in range(ONE, sp):
            sg(j).wait_send()

    n_g, n_d = ff // pair_w, nb * tp // FOUR

    def g_tile(n, slot, which):
        c = aligned(core * ff + n * pair_w, pair_w)
        return pltpu.make_async_copy((wg, wu)[which].at[:, c], wbuf.at[slot], wsem.at[slot, NIL])

    def g_pair(n, base):
        return [g_tile(n, (base + TWO * n + i) % slots, i) for i in range(TWO)]

    def d_cols(m):
        q = m // nb
        d = (TWO + THREE * q + THREE * (q * (q - ONE) // TWO)) % FOUR
        return aligned((y + d) % tp * col + m % nb * cb, cb)

    def d_tile(p, slot):
        return [pltpu.make_async_copy(wd.at[aligned(core * ff, ff), d_cols(TWO * p + i)],
                                      wbuf.at[slot, top(ff), pl.ds(i * cb, cb)], wsem.at[slot, i]) for i in range(TWO)]

    def d_pair(p, base):
        return [c for i in range(TWO) for c in d_tile(TWO * p + i, (base + TWO * p + i) % slots)]

    base = n_o

    lanes = srow.shape[-ONE]

    def stat(i, j):
        return remote(srow.at[i], sin.at[i, j], s_s.at[i, j], s_r.at[i, j], (to_p, to_m, to_2)[j])

    def x1_rows(i):
        r0, r = starts[i], chunks[i]
        def tile(t, w):
            v = jnp.dot(attn_rows(r0, r), wbuf[t, top(tp * part), top(w)], preferred_element_type=F32)
            for q in range(w // LANES):
                xmid[t * FOUR + q, pl.ds(r0, r)] = v[:, q * LANES:(q + ONE) * LANES]

        if not i:
            for t in range(n_o):
                wait([o_part(t, j) for j in range(tp)])

        @pl.loop(NIL, col // pair_w)
        def _(t):
            tile(t, pair_w)

        if col % pair_w:
            tile(n_o - ONE, col % pair_w)
        sq = jnp.zeros((r, LANES), F32)
        for b in range(col // LANES):
            v = xmid[b, pl.ds(r0, r)] + u2[rows_of(i, NIL, r), aligned(y * col + b * LANES, LANES)].astype(F32)
            xmid[b, pl.ds(r0, r)] = v
            sq += v * v
        tot = jnp.broadcast_to(jnp.sum(sq, axis=ONE, keepdims=True), (r, LANES))
        if r < lanes:
            tot = jnp.concatenate([tot, jnp.zeros((lanes - r, LANES), F32)], axis=NIL)
        srow[i] = tot.T[:SUB, :]
        for j in range(tp - ONE):
            stat(i, j).start()

    def norm_rows(i):
        r0, r = starts[i], chunks[i]
        for j in range(tp - ONE):
            stat(i, j).wait()
        tot = srow[i]
        for j in range(tp - ONE):
            tot += sin[i, j]
        inv = lax.rsqrt(tot * (1.0 / dim) + NORM_EPS)
        inv = jnp.broadcast_to(inv[:ONE, :], (LANES, lanes)).T[:r, :]
        for b in range(col // LANES):
            c = aligned(y * col + b * LANES, LANES)
            u2[rows_of(i, NIL, r), c] = (xmid[b, pl.ds(r0, r)] * inv * gain_m[:, c]).astype(BF16)

    def u_blk(i, row0, n_rows, rank):
        return u2.at[rows_of(i, row0, n_rows), cols(rank, col)]

    def u_first(i, side, turn):
        h = chunks[i] // TWO
        b = u_blk(i, h * (side + turn - TWO * side * turn), h, y)
        return remote(b, b, u1s.at[i, side, turn], u1r.at[i, ONE - side, turn], (to_p, to_m)[side])

    def u_second(i, side):
        h = chunks[i] // TWO
        b = u_blk(i, h, h, yp) if side == NIL else u_blk(i, NIL, h, ym)
        return remote(b, b, u2s.at[i, side], u2r.at[i, side], (to_m, to_p)[side])

    def u_pair(i, j):
        r, rank = chunks[i], (y, yp, ym, y2)[j]
        return remote(u_blk(i, NIL, r, rank), u_blk(i, r, r, rank), ups.at[i, j], upr.at[i, j], to_pair)

    def u_start(i):
        for turn in range(TWO):
            u_first(i, NIL, turn).start()
            u_first(i, ONE, turn).start()
        u_pair(i, NIL).start()

    def u_mid(i):
        for side in range(TWO):
            u_first(i, ONE - side, NIL).wait_recv()
            u_second(i, side).start()

    def u_near(i):
        for side in range(TWO):
            u_first(i, ONE - side, ONE).wait_recv()
            u_pair(i, ONE + side).start()

    def u_far(i):
        for side in range(TWO):
            u_second(i, side).wait_recv()
        u_pair(i, THREE).start()

    def u_last(i):
        u_near(i)
        u_far(i)

    def u_ready(i):
        for j in range(FOUR):
            u_pair(i, j).wait_recv()

    def u_drain(i):
        for side in range(TWO):
            for turn in range(TWO):
                u_first(i, side, turn).wait_send()
            u_second(i, side).wait_send()
        for j in range(FOUR):
            u_pair(i, j).wait_send()

    def blk_rows(m, row0, n):
        return pl.ds(pl.multiple_of(m * max(chunks) + row0, EIGHT), n)

    def d_copy(i, p, out):
        r, par = chunks[i], i % TWO
        return remote(p_out.at[out, :, top(r)], d_in.at[par, pl.ds(FOUR * p, FOUR), top(r)], d_s.at[out], d_r.at[par, p], to_pair)

    def t_add(i, p):
        r, par = chunks[i], i % TWO
        d_copy(i, p, NIL).wait_recv()
        for q in range(FOUR):
            p_own[blk_rows(FOUR * p + q, NIL, r), :] += d_in[par, FOUR * p + q, top(r)]

    def f_copy(i, k, side):
        h, par = chunks[i] // TWO, i % TWO
        return remote(p_own.at[blk_rows(k, side * h, h)], f_in.at[par, side, k, top(h)],
                      f_s.at[side], f_r.at[par, side, k], (to_m, to_p)[side])

    def t_f(i, k):
        f_copy(i, k, NIL).start()
        f_copy(i, k, ONE).start()

    def e_copy(i, k, side):
        r, par = chunks[i], i % TWO
        return remote(p_own.at[blk_rows((TWO - side) * nb + k, NIL, r)], e_in.at[par, side, k, top(r)],
                      e_s.at[side], e_r.at[par, side, k], (to_m, to_p)[side])

    def t_e(i, k, side):
        h, par = chunks[i] // TWO, i % TWO
        f_copy(i, k, side).wait_recv()
        p_own[blk_rows((TWO - side) * nb + k, side * h, h), :] += f_in[par, side, k, top(h)]
        e_copy(i, k, side).start()

    def y_at(i, row0, n_rows, rank, k):
        return y_hbm.at[pl.ds(starts[i] + row0, n_rows), aligned(rank * col + k * cb, cb)]

    def a_copy_y(i, k, side):
        r, par = chunks[i], i % TWO
        return remote(ystage.at[par, k, top(r)], y_at(i, NIL, r, y, k), a_s.at[par, side], a_r.at[par, ONE - side, k],
                      (to_p, to_m)[side])

    def a_local(i, k):
        r, par = chunks[i], i % TWO
        return pltpu.make_async_copy(ystage.at[par, k, top(r)], y_at(i, NIL, r, y, k), a_l.at[par])

    def h_copy(i, k, side):
        h = chunks[i] // TWO
        b = y_at(i, h, h, yp, k) if side == NIL else y_at(i, NIL, h, ym, k)
        return remote(b, b, h_s.at[i, side], h_r.at[i, side], (to_m, to_p)[side])

    def t_final(i, k):
        r, par = chunks[i], i % TWO
        for side in range(TWO):
            e_copy(i, k, side).wait_recv()
        v = (p_own[blk_rows(THREE * nb + k, NIL, r), :] + e_in[par, NIL, k, top(r)] + e_in[par, ONE, k, top(r)]
             + jnp.concatenate([xmid[TWO * k + q, pl.ds(starts[i], r)] for q in range(TWO)], axis=ONE))
        ystage[par, k, top(r)] = v.astype(BF16)
        for side in range(TWO):
            a_copy_y(i, k, side).start()
        a_local(i, k).start()

    def t_fwd(i, k):
        for side in range(TWO):
            a_copy_y(i, k, ONE - side).wait_recv()
            h_copy(i, k, side).start()

    def sums_sent(i):
        for side in range(TWO):
            for n, send, recv in ((chunks[i] // TWO, f_s, f_r), (chunks[i], e_s, e_r)):
                b = p_own.at[top(nb * n)]
                remote(b, b, send.at[side], recv.at[NIL, NIL, NIL], to_p).wait_send()

    def rows_done(i):
        r, par = chunks[i], i % TWO
        b = y_hbm.at[pl.ds(starts[i], r), cols(y, col)]
        pltpu.make_async_copy(b, b, a_l.at[par]).wait()
        for side in range(TWO):
            remote(b, b, a_s.at[par, side], a_r.at[par, side, NIL], to_p).wait_send()
            c = y_hbm.at[pl.ds(starts[i], r // TWO), cols(y, col)]
            remote(c, c, h_s.at[i, side], h_r.at[i, side], to_p).wait()

    wait(xr_copies)
    x1_rows(NIL)
    x1_rows(n_ch - ONE)
    norm_rows(NIL)
    u_start(NIL)
    for i in range(ONE, n_ch - ONE):
        x1_rows(i)
    start(g_pair(NIL, base))
    start(g_pair(ONE, base))
    norm_rows(n_ch - ONE)
    u_mid(NIL)
    front_sent()
    u_near(NIL)
    for j in range(THREE):
        u_pair(NIL, j).wait_recv()

    def gate_up(q, ranks):
        return functools.reduce(jnp.add, [
            jnp.dot(u2[rows_of(NIL, NIL, TWO * chunks[NIL]), cols(rank, col)], wbuf[(base + q) % slots, cols(rank, col)],
                    preferred_element_type=F32) for rank in ranks])

    def put_hidden(i, j, g, u):
        g = (jax.nn.silu(g) * u).astype(BF16)
        for q in range(FOUR):
            hbuf[FOUR * j + q, top(TWO * chunks[i])] = g[:, q * LANES:(q + ONE) * LANES]

    wait(g_pair(NIL, base))
    r = chunks[NIL]

    @pl.loop(NIL, TWO)
    def _(q):
        v = gate_up(q, (y, yp, ym))
        for a in range(TWO):
            for b in range(TWO):
                d_in[ONE, FOUR * q + TWO * a + b, top(r)] = v[a * r:(a + ONE) * r, b * cb:(b + ONE) * cb]

    u_far(NIL)
    for i in range(ONE, n_ch - ONE):
        norm_rows(i)
    u_start(ONE)
    u_pair(NIL, THREE).wait_recv()
    part_sums = [jnp.concatenate([jnp.concatenate([d_in[ONE, FOUR * q + TWO * a + b, top(r)] for b in range(TWO)], axis=ONE)
                                  for a in range(TWO)], axis=NIL) for q in range(TWO)]
    put_hidden(NIL, NIL, *[part_sums[q] + gate_up(q, (y2,)) for q in range(TWO)])

    def t_own(i):
        t_add(i, n_d - ONE)

    tasks = {"own": t_own, "mid": u_mid, "last": u_last, "start": u_start, "e": t_e, "final": t_final, "fwd": t_fwd}

    def run(todo, at):
        for when, name, *args in todo:
            @pl.when(at == when)
            def _():
                tasks[name](*args)

    for i in range(n_ch):
        r = chunks[i]
        g_base, d_base = base % slots, (base + TWO * n_g) % slots
        base += TWO * (n_g + n_d)

        @pl.loop(NIL if i else ONE, n_g)
        def _(j):
            @pl.when(j + ONE < n_g)
            def _():
                start(g_pair(j + ONE, g_base))

            @pl.when(j + ONE >= n_g)
            def _():
                start(d_pair(NIL, d_base))

            wait(g_pair(j, g_base))
            put_hidden(i, j, *[jnp.dot(u2[rows_of(i, NIL, TWO * r), :], wbuf[(g_base + TWO * j + q) % slots],
                                       preferred_element_type=F32) for q in range(TWO)])
            run(plan[i][NIL], j)

        if i:
            sums_sent(i - ONE)

        @pl.loop(NIL, n_d)
        def _(p):
            @pl.when(p + ONE < n_d)
            def _():
                start(d_pair(p + ONE, d_base))

            if i + ONE < n_ch:
                @pl.when(p + ONE >= n_d)
                def _():
                    start(g_pair(NIL, base % slots))

            wait(d_pair(p, d_base))
            out = p % TWO

            @pl.when(p >= TWO)
            def _():
                d_copy(i, NIL, out).wait_send()

            if i:
                @pl.when(p < TWO)
                def _():
                    d_copy(i - ONE, NIL, out).wait_send()

            for q in range(TWO):
                v = jnp.dot(wide_rows(TWO * r), wbuf[(d_base + TWO * p + q) % slots, top(ff)],
                            preferred_element_type=F32)
                for e in range(TWO):
                    b = TWO * q + e
                    p_own[blk_rows(FOUR * p + b, NIL, r), :] = v[:r, e * cb:(e + ONE) * cb]
                    p_out[out, b, top(r)] = v[r:, e * cb:(e + ONE) * cb]
            d_copy(i, p, out).start()

            @pl.when(p >= ONE)
            def _():
                t_add(i, p - ONE)

            @pl.when(p == ONE)
            def _():
                for k in range(FOUR):
                    t_f(i, k)

            @pl.when(p == TWO)
            def _():
                for k in range(FOUR, nb):
                    t_f(i, k)
            run(plan[i][ONE], p)

        if i + ONE == n_ch:
            t_add(i, n_d - ONE)
            for out in range(TWO):
                d_copy(i, NIL, out).wait_send()
        for name, *args in plan[i][TWO]:
            tasks[name](*args)
        if i + ONE < n_ch:
            u_ready(i + ONE)

    last = n_ch - ONE
    if last >= TWO:
        rows_done(last - TWO)
    for k in range(nb):
        t_final(last, k)
        if k >= TWO:
            t_fwd(last, k - TWO)
    for k in range(nb - TWO, nb):
        t_fwd(last, k)
    for i in range(max(last - ONE, NIL), n_ch):
        rows_done(i)
    sums_sent(last)
    for i in range(n_ch):
        u_drain(i)


CHUNKS = (192, 192, 128)


def mlp_plan():
    early = lambda i: [(3, "e", i, 0, 1), (3, "e", i, 1, 1), (4, "e", i, 2, 1), (4, "e", i, 0, 0), (4, "e", i, 1, 0)]
    late = lambda i: [("e", i, 3, 1), ("e", i, 2, 0), ("e", i, 4, 1), ("e", i, 3, 0), ("e", i, 4, 0)]
    at_start = lambda i: [(0, *t) for t in late(i)] + [(0, "own", i)]
    finals = lambda i, at: [(a, "final", i, k) for k, a in enumerate(at)]
    passed = lambda i, at: [(a, "fwd", i, k) for k, a in enumerate(at)]
    gather = [(2, "mid", 1), (2, "start", 2), (4, "last", 1), (5, "mid", 2), (7, "last", 2)]
    return ((gather, early(0), ()),
            (at_start(0) + finals(0, (1, 2, 3, 4, 5)) + passed(0, (5, 6, 6, 6, 7)), early(1), ()),
            (at_start(1) + finals(1, (2, 3, 4, 6, 7)), passed(1, (0, 1, 1, 2, 2)) + early(2), late(2)))


def layer_call(x_in, positions, segments, gain_a, gain_m, wq, wk, wv, wo, wg, wu, wd):
    rows, dim = x_in.shape
    tp, sp = lax.axis_size("tp"), lax.axis_size("sp")
    heads, n_kv = wq.shape[ONE] // HEAD_DIM, wk.shape[ONE] // HEAD_DIM
    cb = TWO * LANES
    col, ff = dim // tp, wg.shape[ONE] // TWO
    nb = col // cb
    n_ch, rm = len(CHUNKS), max(CHUNKS)
    lanes = -(-rm // LANES) * LANES
    half_dim = (jnp.arange(HEAD_DIM) % (HEAD_DIM // TWO)).astype(F32)
    freq = jnp.power(F32(ROPE_BASE), -half_dim * (2.0 / HEAD_DIM))[None]
    dma = pltpu.SemaphoreType.DMA
    hbm, vmem = pl.BlockSpec(memory_space=pl.ANY), pl.BlockSpec(memory_space=pltpu.VMEM)
    bufs = [((FOUR, dim, TWO * cb), BF16), ((TWO * rows, dim), BF16), ((ff // LANES, rows, LANES), BF16),
            ((heads, rows, HEAD_DIM), BF16), ((rows, HEAD_DIM), F32), ((rows, HEAD_DIM), F32), ((SUB, rows), F32), ((sp, SUB, rows), F32), ((rows, LANES), BF16),
            ((col // LANES, rows, LANES), F32), ((n_ch, SUB, lanes), F32), ((n_ch, tp - ONE, SUB, lanes), F32),
            ((tp * nb * rm, cb), F32), ((TWO, FOUR, rm, cb), F32), ((TWO, tp * nb, rm, cb), F32),
            ((TWO, TWO, nb, rm // TWO, cb), F32), ((TWO, TWO, nb, rm, cb), F32), ((TWO, nb, rm, cb), BF16)]
    sems = [(FOUR,), (FOUR, TWO), (sp,), (sp,)] + [(n_kv, TWO)] * FOUR + [(n_kv, FOUR)] * TWO + [(tp - ONE,)] * TWO
    sems += [(TWO,), (tp - ONE, TWO)] * TWO + [(FOUR,), (tp - ONE, FOUR)] + [(TWO,), (TWO, heads), (TWO,), (TWO,)]
    sems += [(TWO, sp), (THREE, tp), (n_ch,)]
    sems += [(n_ch, tp - ONE)] * TWO + [(n_ch, TWO, TWO)] * TWO + [(n_ch, TWO)] * TWO + [(n_ch, FOUR)] * TWO
    sems += [(TWO,), (TWO, tp * nb // FOUR)] + [(TWO,), (TWO, TWO, nb)] * TWO + [(TWO,), (TWO, TWO), (TWO, TWO, nb)]
    sems += [(n_ch, TWO)] * TWO
    cache = jax.ShapeDtypeStruct((sp * rows, HEAD_DIM), BF16)
    kc, vc, _, y_out = pl.pallas_call(
        functools.partial(layer_kernel, CHUNKS, cb, mlp_plan()), name="layer",
        out_shape=[cache, cache, jax.ShapeDtypeStruct((tp - ONE, wo.shape[NIL], col), BF16),
                   jax.ShapeDtypeStruct((rows, dim), BF16)],
        in_specs=[hbm] + [vmem] * (FOUR + ONE) + [hbm] * (FOUR + THREE), out_specs=[hbm] * FOUR,
        scratch_shapes=[pltpu.VMEM(*b) for b in bufs] + [dma(q) for q in sems],
        compiler_params=pltpu.CompilerParams(collective_id=ONE, has_side_effects=True, vmem_limit_bytes=VMEM_BYTES),
    )(x_in, segments.reshape(ONE, rows), positions.reshape(ONE, rows), freq, gain_a.reshape(ONE, dim), gain_m.reshape(ONE, dim),
      wq, wk, wv, wo, wg, wu, wd)
    return copy_out(y_out, kc, vc)


def copy_kernel(*refs):
    n = len(refs) // FOUR
    ins, outs, bufs, sems = (refs[i * n:(i + ONE) * n] for i in range(FOUR))

    def parts(src, dst, sem):
        step = src.shape[NIL] // sem.shape[ONE]
        return [(src.at[pl.ds(k * step, step)], dst.at[pl.ds(k * step, step)], k) for k in range(sem.shape[ONE])]

    for a, b, sem in zip(ins, bufs, sems):
        start([pltpu.make_async_copy(x, v, sem.at[NIL, k]) for x, v, k in parts(a, b, sem)])
    for a, b, o, sem in zip(ins, bufs, outs, sems):
        for (x, v, k), (_, d, _) in zip(parts(a, b, sem), parts(b, o, sem)):
            pltpu.make_async_copy(x, v, sem.at[NIL, k]).wait()
            pltpu.make_async_copy(v, d, sem.at[ONE, k]).start()
    for b, o, sem in zip(bufs, outs, sems):
        wait([pltpu.make_async_copy(v, d, sem.at[ONE, k]) for v, d, k in parts(b, o, sem)])


def copy_out(*arrays):
    hbm = pl.BlockSpec(memory_space=pl.ANY)
    return pl.pallas_call(
        copy_kernel, name="copy_out", out_shape=[jax.ShapeDtypeStruct(a.shape, a.dtype) for a in arrays],
        in_specs=[hbm] * len(arrays), out_specs=[hbm] * len(arrays),
        scratch_shapes=[pltpu.VMEM(a.shape, a.dtype) for a in arrays] + [pltpu.SemaphoreType.DMA((TWO, FOUR)) for _ in arrays],
        compiler_params=pltpu.CompilerParams(vmem_limit_bytes=VMEM_BYTES),
    )(*arrays)


def solution(mesh):
    row_spec = P(("rep", "sp"), None)
    tok_spec = P(("rep", "sp"))
    full_spec = P(None)
    col_spec = P(None, "tp")
    wrow_spec = P("tp", None)
    cache_spec = P("rep", ("tp", "sp"), None)

    def local_layer(x_in, positions, segments, gain_attn, w_q, w_k, w_v, w_o, gain_mlp, w_gate, w_up, w_down):
        y_out, kc, vc = layer_call(x_in, positions, segments, gain_attn, gain_mlp, w_q, w_k, w_v, w_o, w_gate, w_up, w_down)
        return y_out, kc.reshape(-1, 1, HEAD_DIM), vc.reshape(-1, 1, HEAD_DIM)

    return jax.shard_map(local_layer, mesh=mesh,
                         in_specs=(row_spec, tok_spec, tok_spec, full_spec, col_spec, col_spec, col_spec, wrow_spec,
                                   full_spec, col_spec, col_spec, wrow_spec),
                         out_specs=(row_spec, cache_spec, cache_spec), check_vma=False)
```

```python
import functools

import jax
import jax.numpy as jnp
from jax import lax
from jax.experimental import pallas as pl
from jax.experimental.pallas import tpu as pltpu
from jax.sharding import PartitionSpec as P

HEAD_DIM = 128
ROPE_BASE = 500000.0
NORM_EPS = 1e-5
MESH = pl.DeviceIdType.MESH
BF16, F32 = jnp.bfloat16, jnp.float32
VMEM_BYTES = 67043328
NIL, ONE, TWO, THREE, FOUR, EIGHT, SUB, LANES = 0, 1, 2, 3, 4, 8, 8, 128


def remote(src, dst, send_sem, recv_sem, to):
    return pltpu.make_async_remote_copy(src, dst, send_sem, recv_sem, device_id=to, device_id_type=MESH)


def start(copies):
    for c in copies:
        c.start()


def wait(copies):
    for c in copies:
        c.wait()


def top(n):
    return pl.ds(NIL, n)


def aligned(offset, n):
    return pl.ds(pl.multiple_of(offset, LANES), n)


def layer_kernel(chunks, cb, plan, x_hbm, seg, pos, freq, gain_a, gain_m, wq, wk, wv, wo, wg, wu, wd,
                 kc, vc, wo_g, y_hbm,
                 wbuf, u2, hbuf, qb, rope_c, rope_s, seg_row, sgb, fq, xmid, srow, sin, p_own, p_out, d_in, f_in, e_in, ystage,
                 xsem, wsem, sg_s, sg_r, k1s, k1r, k2s, k2r, kps, kpr, w1s, w1r, w2s, w2r, w3s, w3r, wps, wpr,
                 t_s, t_r, v_s, v_r, csem, osem, xrsem,
                 s_s, s_r, u1s, u1r, u2s, u2r, ups, upr, d_s, d_r, f_s, f_r, e_s, e_r, a_l, a_s, a_r, h_s, h_r):
    rows, dim = x_hbm.shape
    tp, sp = lax.axis_size("tp"), lax.axis_size("sp")
    hd = HEAD_DIM
    heads = wq.shape[ONE] // hd
    n_kv = wk.shape[ONE] // hd
    group = heads // n_kv
    wide = heads * hd
    col, wrow = dim // tp, wo.shape[NIL] // sp
    half = wrow // TWO
    nb = col // cb
    pair_w = TWO * cb
    ff = wg.shape[ONE] // TWO
    slots = wbuf.shape[NIL]
    per_dev = TWO * n_kv
    y, s = lax.axis_index("tp"), lax.axis_index("sp")
    core, chip, n_chip = s % TWO, s // TWO, sp // TWO
    yp, ym, y2 = (y + ONE) % tp, (y + tp - ONE) % tp, (y + TWO) % tp
    chip_at = lambda d: (chip + d) % n_chip * TWO
    up, dn, far = (chip_at(d) + core for d in (ONE, n_chip - ONE, TWO))
    pair = s + ONE - TWO * core
    to_pair, to_up, to_dn = ({"tp": y, "sp": d} for d in (pair, up, dn))
    to_p, to_m, to_2 = ({"tp": d, "sp": s} for d in (yp, ym, y2))
    scale2 = HEAD_DIM ** -0.5 * 1.4426950408889634

    kw = n_kv * hd
    n_x = xsem.shape[NIL]
    x_rows = rows // n_x
    x_copies = [pltpu.make_async_copy(x_hbm.at[pl.ds(i * x_rows, x_rows)], u2.at[pl.ds(i * x_rows, x_rows)], xsem.at[i])
                for i in range(n_x)]
    start(x_copies)
    kv_copies = [pltpu.make_async_copy(w, wbuf.at[NIL, :, pl.ds(i * kw, kw)], wsem.at[NIL, i]) for i, w in enumerate((wk, wv))]

    def q_copy(t):
        return pltpu.make_async_copy(wq.at[:, aligned(t * TWO * kw, TWO * kw)], wbuf.at[ONE + t], wsem.at[ONE + t, NIL])

    barrier = pltpu.get_barrier_semaphore()
    for j in range(ONE, sp):
        pl.semaphore_signal(barrier, inc=ONE, device_id={"tp": y, "sp": (s + j) % sp}, device_id_type=MESH)
    for j in range(ONE, tp):
        pl.semaphore_signal(barrier, inc=ONE, device_id={"tp": (y + j) % tp, "sp": s}, device_id_type=MESH)

    def norm(i):
        x_copies[i].wait()
        step = x_rows // TWO

        @pl.loop(NIL, TWO)
        def _(j):
            rr = pl.ds(pl.multiple_of(i * x_rows + j * step, step), step)
            sq = jnp.zeros((step, LANES), F32)
            for b in range(dim // LANES):
                v = u2[rr, pl.ds(b * LANES, LANES)].astype(F32)
                sq += v * v
            inv = lax.rsqrt(jnp.sum(sq, axis=ONE, keepdims=True) * (1.0 / dim) + NORM_EPS)
            for b in range(dim // LANES):
                c = pl.ds(b * LANES, LANES)
                u2[rr, c] = (u2[rr, c].astype(F32) * inv * gain_a[:, c]).astype(BF16)

    seg_row[...] = jnp.broadcast_to(seg[...].astype(F32), (SUB, rows))
    norm(NIL)
    start(kv_copies)
    norm(ONE)
    pl.semaphore_wait(barrier, sp + tp - TWO)

    def w1(j):
        rank, mine = (y + j) % tp, aligned(s * wrow, wrow)
        return remote(wo.at[mine, aligned(rank * col, col)], wo_g.at[tp - ONE - j, mine],
                      w1s.at[j - ONE], w1r.at[tp - ONE - j], {"tp": rank, "sp": s})

    def sg(j):
        return remote(seg_row, sgb.at[s], sg_s.at[j], sg_r.at[j], {"tp": y, "sp": (s + j) % sp})

    for j in range(ONE, sp):
        sg(j).start()
    for j in range(ONE, tp):
        w1(j).start()

    def w_blk(i, dev, r0, n):
        return wo_g.at[i, pl.ds(pl.multiple_of(dev * wrow + r0, half), n)]

    def w2(i, side):
        b = w_blk(i, s, NIL, wrow)
        return remote(b, b, w2s.at[side], w2r.at[i, ONE - side], (to_up, to_dn)[side])

    def w3(i, side):
        b = w_blk(i, (up, dn)[side], (half, NIL)[side], half)
        return remote(b, b, w3s.at[side], w3r.at[i, side], (to_dn, to_up)[side])

    def wp(i, j):
        b = w_blk(i, (s, up, dn, far)[j], NIL, wrow)
        return remote(b, b, wps.at[j], wpr.at[i, j], to_pair)

    def w_start(i):
        w1(tp - ONE - i).wait_recv()
        w2(i, NIL).start()
        w2(i, ONE).start()
        wp(i, NIL).start()

    def w_mid(i):
        for side in range(TWO):
            w2(i, ONE - side).wait_recv()
            w3(i, side).start()
            wp(i, ONE + side).start()

    def w_last(i):
        w3(i, NIL).wait_recv()
        w3(i, ONE).wait_recv()
        wp(i, THREE).start()

    q_copy(NIL).start()
    q_copy(ONE).start()
    for i in range(TWO, n_x):
        norm(i)

    def rope(t):
        return (t * rope_c[...] + pltpu.roll(t, hd // TWO, ONE) * rope_s[...]).astype(BF16)

    wait(kv_copies)
    angles = jnp.broadcast_to(pos[...].astype(F32), (LANES, rows)).T * freq[...]
    sign = jnp.where(lax.broadcasted_iota(jnp.int32, (rows, hd), ONE) < hd // TWO, -1.0, 1.0)
    rope_c[...] = jnp.cos(angles)
    rope_s[...] = jnp.sin(angles) * sign
    r = jnp.dot(u2[top(rows), :], wbuf[NIL], preferred_element_type=F32)
    for g in range(n_kv):
        hbuf[s * per_dev + TWO * g] = rope(r[:, g * hd:(g + ONE) * hd])
        hbuf[s * per_dev + TWO * g + ONE] = r[:, kw + g * hd:kw + (g + ONE) * hd].astype(BF16)

    def k_blk(dev, g, lo=NIL, n=TWO):
        return hbuf.at[pl.ds(dev * per_dev + TWO * g + lo, n)]

    def k1(g, side):
        b = k_blk(s, g)
        return remote(b, b, k1s.at[g, side], k1r.at[g, ONE - side], (to_up, to_dn)[side])

    def k2(g, side):
        b = k_blk((up, dn)[side], g, ONE - side, ONE)
        return remote(b, b, k2s.at[g, side], k2r.at[g, side], (to_dn, to_up)[side])

    def kp(g, j):
        b = k_blk((s, up, dn, far)[j], g)
        return remote(b, b, kps.at[g, j], kpr.at[g, j], to_pair)

    def k_start(g):
        k1(g, NIL).start()
        k1(g, ONE).start()
        kp(g, NIL).start()

    def k_mid(g):
        for side in range(TWO):
            k1(g, ONE - side).wait_recv()
            k2(g, side).start()
            kp(g, ONE + side).start()

    def k_last(g):
        k2(g, NIL).wait_recv()
        k2(g, ONE).wait_recv()
        kp(g, THREE).start()

    k_start(NIL)

    @pl.loop(NIL, TWO)
    def _(t):
        q_copy(t).wait()
        r = jnp.dot(u2[top(rows), :], wbuf[ONE + t], preferred_element_type=F32)
        for g in range(heads // TWO):
            qb[t * (heads // TWO) + g] = rope(r[:, g * hd:(g + ONE) * hd])

    n_o = -(-col // pair_w)
    part = wide
    starts = [sum(chunks[:i]) for i in range(len(chunks))]
    n_ch = len(chunks)

    def cols(block, width):
        return aligned(block * width, width)

    def o_width(t):
        return min(pair_w, col - t * pair_w)

    def o_part(t, j):
        w = o_width(t)
        src = wo_g.at[j - ONE, :, pl.ds(t * pair_w, w)] if j else wo.at[:, aligned(y * col + t * pair_w, w)]
        return pltpu.make_async_copy(src, wbuf.at[t, aligned((y + j) % tp * part, part), top(w)], osem.at[t, j])

    def rows_of(i, row0, n):
        return pl.ds(TWO * starts[i] + row0, n)

    xr_copies = [pltpu.make_async_copy(x_hbm.at[pl.ds(r0, r), cols(y, col)], u2.at[rows_of(i, NIL, r), cols(y, col)], xrsem.at[i])
                 for i, (r0, r) in enumerate(zip(starts, chunks))]
    start(xr_copies)
    for t in range(n_o):
        o_part(t, NIL).start()

    for j in range(ONE, sp):
        sg(j).wait_recv()
    sgb[s] = seg_row[...]
    lane = lax.broadcasted_iota(jnp.int32, (rows, LANES), ONE).astype(F32)

    def seg_col(dev):
        return jnp.broadcast_to(sgb[dev, top(ONE), :], (LANES, rows)).T

    def key_cols(b):
        return aligned(yp * col + b * LANES, LANES)

    fq[...] = jnp.where(seg_col(s) == lane, 1.0, 0.0).astype(BF16)

    @pl.loop(NIL, sp)
    def _(b):
        u2[pl.ds(rows, rows), key_cols(b)] = jnp.where(seg_col(b) == lane, 0.0, -1e30).astype(BF16)

    def attend(h, i, g, b0, nb, own):
        nk = nb * rows
        both = lambda j: jnp.concatenate([hbuf[(b0 + d) * per_dev + TWO * g + j] for d in range(nb)], axis=NIL)
        q = jnp.concatenate([qb[h], fq[...]], axis=ONE)
        feat = jnp.concatenate([u2[pl.ds(rows, rows), key_cols(b0 + d)] for d in range(nb)], axis=NIL)
        k = jnp.concatenate([both(NIL), feat], axis=ONE)
        v = both(ONE)
        sc = lax.dot_general(q, k, (((ONE,), (ONE,)), ((), ())), preferred_element_type=F32)
        if own:
            lo = nk - rows
            a, b = (lax.broadcasted_iota(jnp.int32, (rows, rows), d) for d in range(TWO))
            tail = jnp.where(a >= b, sc[:, lo:], -1e30)
            sc = jnp.concatenate([sc[:, :lo], tail], axis=ONE) if lo else tail
        at = aligned(i * rows, rows)
        mx = jnp.max(sc, axis=ONE, keepdims=True)
        if own:
            mn = jnp.broadcast_to(mx, (rows, LANES))
        else:
            mn = jnp.maximum(xmid[group + i], mx)
            al = jnp.exp2((xmid[group + i] - mn) * scale2)
        ps = [jnp.exp2((sc[:, j * LANES:(j + ONE) * LANES] - mn) * scale2) for j in range(nk // LANES)]
        ls = functools.reduce(jnp.add, ps)
        o = jnp.dot(jnp.concatenate([p.astype(BF16) for p in ps], axis=ONE), v, preferred_element_type=F32)
        xmid[group + i] = mn
        if own:
            p_own[at, top(LANES)] = ls
            xmid[i] = o
        else:
            p_own[at, top(LANES)] = p_own[at, top(LANES)] * al + ls
            xmid[i] = xmid[i] * al + o

    def a_at(rank, h, r0, n):
        b = rank * heads + h
        return wbuf.at[slots - ONE, pl.ds(pl.multiple_of(b // FOUR * rows + r0, LANES), n), aligned(b % FOUR * hd, hd)]

    def a1(h, side):
        return remote(qb.at[h], a_at(y, h, NIL, rows), t_s.at[side], t_r.at[ONE - side, h], (to_p, to_m)[side])

    def a2(h, side):
        b = a_at((yp, ym)[side], h, (rows // TWO, NIL)[side], rows // TWO)
        return remote(b, b, v_s.at[side], v_r.at[side], (to_m, to_p)[side])

    def pass_on(h):
        for side in range(TWO):
            a1(h, ONE - side).wait_recv()
            a2(h, side).start()

    @pl.loop(NIL, n_kv)
    def _(g):
        @pl.when(g == NIL)
        def _():
            k_mid(NIL)
            k_start(ONE)

        kp(g, NIL).wait_recv()

        def own_keys(i):
            @pl.when(core == NIL)
            def _():
                attend(g * group + i, i, g, s, ONE, True)

            @pl.when(core == ONE)
            def _():
                attend(g * group + i, i, g, chip_at(NIL), TWO, True)

        @pl.when(g == NIL)
        def _():
            pl.loop(NIL, group)(own_keys)
            w_start(NIL)

        k_last(g)
        for j in range(ONE, FOUR):
            kp(g, j).wait_recv()

        @pl.loop(NIL, group)
        def _(i):
            h = g * group + i

            @pl.when(g > NIL)
            def _():
                own_keys(i)

            @pl.loop(ONE, n_chip)
            def _(e):
                @pl.when(chip >= e)
                def _():
                    attend(h, i, g, chip_at(n_chip - e), TWO, False)

            total = jnp.sum(p_own[aligned(i * rows, rows), top(LANES)], axis=ONE, keepdims=True)
            qb[h] = (xmid[i] / total).astype(BF16)
            a1(h, NIL).start()
            a1(h, ONE).start()

            @pl.when(h == NIL)
            def _():
                k_mid(ONE)
                for b in range(ONE, tp - ONE):
                    w_start(b)

            for b in range(tp - TWO):
                @pl.when(h == heads - FOUR + b)
                def _():
                    w_mid(b)

            @pl.when(h >= TWO)
            def _():
                pass_on(h - TWO)

    mine_kv = s // (sp // n_kv)
    caches = [pltpu.make_async_copy(hbuf.at[d * per_dev + TWO * mine_kv + i], c.at[pl.ds(d * rows, rows)], csem.at[i, d])
              for i, c in enumerate((kc, vc)) for d in range(sp)]
    start(caches)
    w_mid(tp - TWO)
    pass_on(heads - TWO)

    def w_done(i):
        for j in range(FOUR):
            wp(i, j).wait_recv()
        for t in range(n_o):
            o_part(t, i + ONE).start()

    for i in range(tp - ONE):
        if i == tp - TWO:
            pass_on(heads - ONE)
        w_last(i)
    for i in range(tp - TWO):
        w_done(i)
    for h in range(heads):
        b = y * heads + h
        wbuf[slots - ONE, aligned(b // FOUR * rows, rows), aligned(b % FOUR * hd, hd)] = qb[h]

    def all_heads(side, n, send, recv):
        b = qb.at[:, top(n)]
        return remote(b, b, send.at[side], recv.at[side], to_p)

    for side in range(TWO):
        all_heads(side, rows // TWO, v_s, v_r).wait_recv()
        all_heads(side, rows // TWO, v_s, v_r).wait_send()
    w_done(tp - TWO)

    def attn_rows(r0, n):
        return jnp.concatenate([wbuf[slots - ONE, pl.ds(b * rows + r0, n), :] for b in range(tp * heads // FOUR)], axis=ONE)

    def wide_rows(n):
        return jnp.concatenate([hbuf[b, top(n)] for b in range(hbuf.shape[NIL])], axis=ONE)

    def front_sent():
        for g in range(n_kv):
            for j in range(FOUR):
                kp(g, j).wait_send()
            for side in range(TWO):
                k1(g, side).wait_send()
                k2(g, side).wait_send()
        wait(caches)
        for side in range(TWO):
            all_heads(side, rows, t_s, v_r).wait_send()
        for n, send, recv in ((wrow, wps, wpr), (wrow, w2s, w2r), (half, w3s, w3r)):
            b = wo_g.at[:, top(n)]
            for j in range(send.shape[NIL]):
                remote(b, b, send.at[j], recv.at[NIL, NIL], to_p).wait_send()
        for i in range(tp - ONE):
            w1(i + ONE).wait_send()
        for j in range(ONE, sp):
            sg(j).wait_send()

    n_g, n_d = ff // pair_w, nb * tp // FOUR

    def g_tile(n, slot, which):
        c = aligned(core * ff + n * pair_w, pair_w)
        return pltpu.make_async_copy((wg, wu)[which].at[:, c], wbuf.at[slot], wsem.at[slot, NIL])

    def g_pair(n, base):
        return [g_tile(n, (base + TWO * n + i) % slots, i) for i in range(TWO)]

    def d_cols(m):
        q = m // nb
        d = (TWO + THREE * q + THREE * (q * (q - ONE) // TWO)) % FOUR
        return aligned((y + d) % tp * col + m % nb * cb, cb)

    def d_tile(p, slot):
        return [pltpu.make_async_copy(wd.at[aligned(core * ff, ff), d_cols(TWO * p + i)],
                                      wbuf.at[slot, top(ff), pl.ds(i * cb, cb)], wsem.at[slot, i]) for i in range(TWO)]

    def d_pair(p, base):
        return [c for i in range(TWO) for c in d_tile(TWO * p + i, (base + TWO * p + i) % slots)]

    base = n_o

    lanes = srow.shape[-ONE]

    def stat(i, j):
        return remote(srow.at[i], sin.at[i, j], s_s.at[i, j], s_r.at[i, j], (to_p, to_m, to_2)[j])

    def x1_rows(i):
        r0, r = starts[i], chunks[i]
        def tile(t, w):
            v = jnp.dot(attn_rows(r0, r), wbuf[t, top(tp * part), top(w)], preferred_element_type=F32)
            for q in range(w // LANES):
                xmid[t * FOUR + q, pl.ds(r0, r)] = v[:, q * LANES:(q + ONE) * LANES]

        if not i:
            for t in range(n_o):
                wait([o_part(t, j) for j in range(tp)])

        @pl.loop(NIL, col // pair_w)
        def _(t):
            tile(t, pair_w)

        if col % pair_w:
            tile(n_o - ONE, col % pair_w)
        sq = jnp.zeros((r, LANES), F32)
        for b in range(col // LANES):
            v = xmid[b, pl.ds(r0, r)] + u2[rows_of(i, NIL, r), aligned(y * col + b * LANES, LANES)].astype(F32)
            xmid[b, pl.ds(r0, r)] = v
            sq += v * v
        tot = jnp.broadcast_to(jnp.sum(sq, axis=ONE, keepdims=True), (r, LANES))
        if r < lanes:
            tot = jnp.concatenate([tot, jnp.zeros((lanes - r, LANES), F32)], axis=NIL)
        srow[i] = tot.T[:SUB, :]
        for j in range(tp - ONE):
            stat(i, j).start()

    def norm_rows(i):
        r0, r = starts[i], chunks[i]
        for j in range(tp - ONE):
            stat(i, j).wait()
        tot = srow[i]
        for j in range(tp - ONE):
            tot += sin[i, j]
        inv = lax.rsqrt(tot * (1.0 / dim) + NORM_EPS)
        inv = jnp.broadcast_to(inv[:ONE, :], (LANES, lanes)).T[:r, :]
        for b in range(col // LANES):
            c = aligned(y * col + b * LANES, LANES)
            u2[rows_of(i, NIL, r), c] = (xmid[b, pl.ds(r0, r)] * inv * gain_m[:, c]).astype(BF16)

    def u_blk(i, row0, n_rows, rank):
        return u2.at[rows_of(i, row0, n_rows), cols(rank, col)]

    def u_first(i, side, turn):
        h = chunks[i] // TWO
        b = u_blk(i, h * (side + turn - TWO * side * turn), h, y)
        return remote(b, b, u1s.at[i, side, turn], u1r.at[i, ONE - side, turn], (to_p, to_m)[side])

    def u_second(i, side):
        h = chunks[i] // TWO
        b = u_blk(i, h, h, yp) if side == NIL else u_blk(i, NIL, h, ym)
        return remote(b, b, u2s.at[i, side], u2r.at[i, side], (to_m, to_p)[side])

    def u_pair(i, j):
        r, rank = chunks[i], (y, yp, ym, y2)[j]
        return remote(u_blk(i, NIL, r, rank), u_blk(i, r, r, rank), ups.at[i, j], upr.at[i, j], to_pair)

    def u_start(i):
        for turn in range(TWO):
            u_first(i, NIL, turn).start()
            u_first(i, ONE, turn).start()
        u_pair(i, NIL).start()

    def u_mid(i):
        for side in range(TWO):
            u_first(i, ONE - side, NIL).wait_recv()
            u_second(i, side).start()

    def u_near(i):
        for side in range(TWO):
            u_first(i, ONE - side, ONE).wait_recv()
            u_pair(i, ONE + side).start()

    def u_far(i):
        for side in range(TWO):
            u_second(i, side).wait_recv()
        u_pair(i, THREE).start()

    def u_last(i):
        u_near(i)
        u_far(i)

    def u_ready(i):
        for j in range(FOUR):
            u_pair(i, j).wait_recv()

    def u_drain(i):
        for side in range(TWO):
            for turn in range(TWO):
                u_first(i, side, turn).wait_send()
            u_second(i, side).wait_send()
        for j in range(FOUR):
            u_pair(i, j).wait_send()

    def blk_rows(m, row0, n):
        return pl.ds(pl.multiple_of(m * max(chunks) + row0, EIGHT), n)

    def d_copy(i, p, out):
        r, par = chunks[i], i % TWO
        return remote(p_out.at[out, :, top(r)], d_in.at[par, pl.ds(FOUR * p, FOUR), top(r)], d_s.at[out], d_r.at[par, p], to_pair)

    def t_add(i, p):
        r, par = chunks[i], i % TWO
        d_copy(i, p, NIL).wait_recv()
        for q in range(FOUR):
            p_own[blk_rows(FOUR * p + q, NIL, r), :] += d_in[par, FOUR * p + q, top(r)]

    def f_copy(i, k, side):
        h, par = chunks[i] // TWO, i % TWO
        return remote(p_own.at[blk_rows(k, side * h, h)], f_in.at[par, side, k, top(h)],
                      f_s.at[side], f_r.at[par, side, k], (to_m, to_p)[side])

    def t_f(i, k):
        f_copy(i, k, NIL).start()
        f_copy(i, k, ONE).start()

    def e_copy(i, k, side):
        r, par = chunks[i], i % TWO
        return remote(p_own.at[blk_rows((TWO - side) * nb + k, NIL, r)], e_in.at[par, side, k, top(r)],
                      e_s.at[side], e_r.at[par, side, k], (to_m, to_p)[side])

    def t_e(i, k, side):
        h, par = chunks[i] // TWO, i % TWO
        f_copy(i, k, side).wait_recv()
        p_own[blk_rows((TWO - side) * nb + k, side * h, h), :] += f_in[par, side, k, top(h)]
        e_copy(i, k, side).start()

    def y_at(i, row0, n_rows, rank, k):
        return y_hbm.at[pl.ds(starts[i] + row0, n_rows), aligned(rank * col + k * cb, cb)]

    def a_copy_y(i, k, side):
        r, par = chunks[i], i % TWO
        return remote(ystage.at[par, k, top(r)], y_at(i, NIL, r, y, k), a_s.at[par, side], a_r.at[par, ONE - side, k],
                      (to_p, to_m)[side])

    def a_local(i, k):
        r, par = chunks[i], i % TWO
        return pltpu.make_async_copy(ystage.at[par, k, top(r)], y_at(i, NIL, r, y, k), a_l.at[par])

    def h_copy(i, k, side):
        h = chunks[i] // TWO
        b = y_at(i, h, h, yp, k) if side == NIL else y_at(i, NIL, h, ym, k)
        return remote(b, b, h_s.at[i, side], h_r.at[i, side], (to_m, to_p)[side])

    def t_final(i, k):
        r, par = chunks[i], i % TWO
        for side in range(TWO):
            e_copy(i, k, side).wait_recv()
        v = (p_own[blk_rows(THREE * nb + k, NIL, r), :] + e_in[par, NIL, k, top(r)] + e_in[par, ONE, k, top(r)]
             + jnp.concatenate([xmid[TWO * k + q, pl.ds(starts[i], r)] for q in range(TWO)], axis=ONE))
        ystage[par, k, top(r)] = v.astype(BF16)
        for side in range(TWO):
            a_copy_y(i, k, side).start()
        a_local(i, k).start()

    def t_fwd(i, k):
        for side in range(TWO):
            a_copy_y(i, k, ONE - side).wait_recv()
            h_copy(i, k, side).start()

    def sums_sent(i):
        for side in range(TWO):
            for n, send, recv in ((chunks[i] // TWO, f_s, f_r), (chunks[i], e_s, e_r)):
                b = p_own.at[top(nb * n)]
                remote(b, b, send.at[side], recv.at[NIL, NIL, NIL], to_p).wait_send()

    def rows_done(i):
        r, par = chunks[i], i % TWO
        b = y_hbm.at[pl.ds(starts[i], r), cols(y, col)]
        pltpu.make_async_copy(b, b, a_l.at[par]).wait()
        for side in range(TWO):
            remote(b, b, a_s.at[par, side], a_r.at[par, side, NIL], to_p).wait_send()
            c = y_hbm.at[pl.ds(starts[i], r // TWO), cols(y, col)]
            remote(c, c, h_s.at[i, side], h_r.at[i, side], to_p).wait()

    wait(xr_copies)
    x1_rows(NIL)
    x1_rows(n_ch - ONE)
    norm_rows(NIL)
    u_start(NIL)
    for i in range(ONE, n_ch - ONE):
        x1_rows(i)
    start(g_pair(NIL, base))
    start(g_pair(ONE, base))
    norm_rows(n_ch - ONE)
    u_mid(NIL)
    front_sent()
    u_near(NIL)
    for j in range(THREE):
        u_pair(NIL, j).wait_recv()

    def gate_up(q, ranks):
        return functools.reduce(jnp.add, [
            jnp.dot(u2[rows_of(NIL, NIL, TWO * chunks[NIL]), cols(rank, col)], wbuf[(base + q) % slots, cols(rank, col)],
                    preferred_element_type=F32) for rank in ranks])

    def put_hidden(i, j, g, u):
        g = (jax.nn.silu(g) * u).astype(BF16)
        for q in range(FOUR):
            hbuf[FOUR * j + q, top(TWO * chunks[i])] = g[:, q * LANES:(q + ONE) * LANES]

    wait(g_pair(NIL, base))
    r = chunks[NIL]

    @pl.loop(NIL, TWO)
    def _(q):
        v = gate_up(q, (y, yp, ym))
        for a in range(TWO):
            for b in range(TWO):
                d_in[ONE, FOUR * q + TWO * a + b, top(r)] = v[a * r:(a + ONE) * r, b * cb:(b + ONE) * cb]

    u_far(NIL)
    for i in range(ONE, n_ch - ONE):
        norm_rows(i)
    u_start(ONE)
    u_pair(NIL, THREE).wait_recv()
    part_sums = [jnp.concatenate([jnp.concatenate([d_in[ONE, FOUR * q + TWO * a + b, top(r)] for b in range(TWO)], axis=ONE)
                                  for a in range(TWO)], axis=NIL) for q in range(TWO)]
    put_hidden(NIL, NIL, *[part_sums[q] + gate_up(q, (y2,)) for q in range(TWO)])

    def t_own(i):
        t_add(i, n_d - ONE)

    tasks = {"own": t_own, "mid": u_mid, "last": u_last, "start": u_start, "e": t_e, "final": t_final, "fwd": t_fwd}

    def run(todo, at):
        for when, name, *args in todo:
            @pl.when(at == when)
            def _():
                tasks[name](*args)

    for i in range(n_ch):
        r = chunks[i]
        g_base, d_base = base % slots, (base + TWO * n_g) % slots
        base += TWO * (n_g + n_d)

        @pl.loop(NIL if i else ONE, n_g)
        def _(j):
            @pl.when(j + ONE < n_g)
            def _():
                start(g_pair(j + ONE, g_base))

            @pl.when(j + ONE >= n_g)
            def _():
                start(d_pair(NIL, d_base))

            wait(g_pair(j, g_base))
            put_hidden(i, j, *[jnp.dot(u2[rows_of(i, NIL, TWO * r), :], wbuf[(g_base + TWO * j + q) % slots],
                                       preferred_element_type=F32) for q in range(TWO)])
            run(plan[i][NIL], j)

        if i:
            sums_sent(i - ONE)

        @pl.loop(NIL, n_d)
        def _(p):
            @pl.when(p + ONE < n_d)
            def _():
                start(d_pair(p + ONE, d_base))

            if i + ONE < n_ch:
                @pl.when(p + ONE >= n_d)
                def _():
                    start(g_pair(NIL, base % slots))

            wait(d_pair(p, d_base))
            out = p % TWO

            @pl.when(p >= TWO)
            def _():
                d_copy(i, NIL, out).wait_send()

            if i:
                @pl.when(p < TWO)
                def _():
                    d_copy(i - ONE, NIL, out).wait_send()

            for q in range(TWO):
                v = jnp.dot(wide_rows(TWO * r), wbuf[(d_base + TWO * p + q) % slots, top(ff)],
                            preferred_element_type=F32)
                for e in range(TWO):
                    b = TWO * q + e
                    p_own[blk_rows(FOUR * p + b, NIL, r), :] = v[:r, e * cb:(e + ONE) * cb]
                    p_out[out, b, top(r)] = v[r:, e * cb:(e + ONE) * cb]
            d_copy(i, p, out).start()

            @pl.when(p >= ONE)
            def _():
                t_add(i, p - ONE)

            @pl.when(p == ONE)
            def _():
                for k in range(FOUR):
                    t_f(i, k)

            @pl.when(p == TWO)
            def _():
                for k in range(FOUR, nb):
                    t_f(i, k)
            run(plan[i][ONE], p)

        if i + ONE == n_ch:
            t_add(i, n_d - ONE)
            for out in range(TWO):
                d_copy(i, NIL, out).wait_send()
        for name, *args in plan[i][TWO]:
            tasks[name](*args)
        if i + ONE < n_ch:
            u_ready(i + ONE)

    last = n_ch - ONE
    if last >= TWO:
        rows_done(last - TWO)
    for k in range(nb):
        t_final(last, k)
        if k >= TWO:
            t_fwd(last, k - TWO)
    for k in range(nb - TWO, nb):
        t_fwd(last, k)
    for i in range(max(last - ONE, NIL), n_ch):
        rows_done(i)
    sums_sent(last)
    for i in range(n_ch):
        u_drain(i)


CHUNKS = (192, 192, 128)


def mlp_plan():
    early = lambda i: [(3, "e", i, 0, 1), (3, "e", i, 1, 1), (4, "e", i, 2, 1), (4, "e", i, 0, 0), (4, "e", i, 1, 0)]
    late = lambda i: [("e", i, 3, 1), ("e", i, 2, 0), ("e", i, 4, 1), ("e", i, 3, 0), ("e", i, 4, 0)]
    at_start = lambda i: [(0, *t) for t in late(i)] + [(0, "own", i)]
    finals = lambda i, at: [(a, "final", i, k) for k, a in enumerate(at)]
    passed = lambda i, at: [(a, "fwd", i, k) for k, a in enumerate(at)]
    gather = [(2, "mid", 1), (2, "start", 2), (4, "last", 1), (5, "mid", 2), (7, "last", 2)]
    return ((gather, early(0), ()),
            (at_start(0) + finals(0, (1, 2, 3, 4, 5)) + passed(0, (6, 6, 7, 7, 7)), early(1), ()),
            (at_start(1) + finals(1, (2, 3, 4, 5, 6)), passed(1, (0, 0, 0, 1, 1)) + early(2), late(2)))


def layer_call(x_in, positions, segments, gain_a, gain_m, wq, wk, wv, wo, wg, wu, wd):
    rows, dim = x_in.shape
    tp, sp = lax.axis_size("tp"), lax.axis_size("sp")
    heads, n_kv = wq.shape[ONE] // HEAD_DIM, wk.shape[ONE] // HEAD_DIM
    cb = TWO * LANES
    col, ff = dim // tp, wg.shape[ONE] // TWO
    nb = col // cb
    n_ch, rm = len(CHUNKS), max(CHUNKS)
    lanes = -(-rm // LANES) * LANES
    half_dim = (jnp.arange(HEAD_DIM) % (HEAD_DIM // TWO)).astype(F32)
    freq = jnp.power(F32(ROPE_BASE), -half_dim * (2.0 / HEAD_DIM))[None]
    dma = pltpu.SemaphoreType.DMA
    hbm, vmem = pl.BlockSpec(memory_space=pl.ANY), pl.BlockSpec(memory_space=pltpu.VMEM)
    bufs = [((FOUR, dim, TWO * cb), BF16), ((TWO * rows, dim), BF16), ((ff // LANES, rows, LANES), BF16),
            ((heads, rows, HEAD_DIM), BF16), ((rows, HEAD_DIM), F32), ((rows, HEAD_DIM), F32), ((SUB, rows), F32), ((sp, SUB, rows), F32), ((rows, LANES), BF16),
            ((col // LANES, rows, LANES), F32), ((n_ch, SUB, lanes), F32), ((n_ch, tp - ONE, SUB, lanes), F32),
            ((tp * nb * rm, cb), F32), ((TWO, FOUR, rm, cb), F32), ((TWO, tp * nb, rm, cb), F32),
            ((TWO, TWO, nb, rm // TWO, cb), F32), ((TWO, TWO, nb, rm, cb), F32), ((TWO, nb, rm, cb), BF16)]
    sems = [(FOUR,), (FOUR, TWO), (sp,), (sp,)] + [(n_kv, TWO)] * FOUR + [(n_kv, FOUR)] * TWO + [(tp - ONE,)] * TWO
    sems += [(TWO,), (tp - ONE, TWO)] * TWO + [(FOUR,), (tp - ONE, FOUR)] + [(TWO,), (TWO, heads), (TWO,), (TWO,)]
    sems += [(TWO, sp), (THREE, tp), (n_ch,)]
    sems += [(n_ch, tp - ONE)] * TWO + [(n_ch, TWO, TWO)] * TWO + [(n_ch, TWO)] * TWO + [(n_ch, FOUR)] * TWO
    sems += [(TWO,), (TWO, tp * nb // FOUR)] + [(TWO,), (TWO, TWO, nb)] * TWO + [(TWO,), (TWO, TWO), (TWO, TWO, nb)]
    sems += [(n_ch, TWO)] * TWO
    cache = jax.ShapeDtypeStruct((sp * rows, HEAD_DIM), BF16)
    kc, vc, _, y_out = pl.pallas_call(
        functools.partial(layer_kernel, CHUNKS, cb, mlp_plan()), name="layer",
        out_shape=[cache, cache, jax.ShapeDtypeStruct((tp - ONE, wo.shape[NIL], col), BF16),
                   jax.ShapeDtypeStruct((rows, dim), BF16)],
        in_specs=[hbm] + [vmem] * (FOUR + ONE) + [hbm] * (FOUR + THREE), out_specs=[hbm] * FOUR,
        scratch_shapes=[pltpu.VMEM(*b) for b in bufs] + [dma(q) for q in sems],
        compiler_params=pltpu.CompilerParams(collective_id=ONE, has_side_effects=True, vmem_limit_bytes=VMEM_BYTES),
    )(x_in, segments.reshape(ONE, rows), positions.reshape(ONE, rows), freq, gain_a.reshape(ONE, dim), gain_m.reshape(ONE, dim),
      wq, wk, wv, wo, wg, wu, wd)
    return copy_out(y_out, kc, vc)


def copy_kernel(*refs):
    n = len(refs) // FOUR
    ins, outs, bufs, sems = (refs[i * n:(i + ONE) * n] for i in range(FOUR))

    def parts(src, dst, sem):
        step = src.shape[NIL] // sem.shape[ONE]
        return [(src.at[pl.ds(k * step, step)], dst.at[pl.ds(k * step, step)], k) for k in range(sem.shape[ONE])]

    for a, b, sem in zip(ins, bufs, sems):
        start([pltpu.make_async_copy(x, v, sem.at[NIL, k]) for x, v, k in parts(a, b, sem)])
    for a, b, o, sem in zip(ins, bufs, outs, sems):
        for (x, v, k), (_, d, _) in zip(parts(a, b, sem), parts(b, o, sem)):
            pltpu.make_async_copy(x, v, sem.at[NIL, k]).wait()
            pltpu.make_async_copy(v, d, sem.at[ONE, k]).start()
    for b, o, sem in zip(bufs, outs, sems):
        wait([pltpu.make_async_copy(v, d, sem.at[ONE, k]) for v, d, k in parts(b, o, sem)])


def copy_out(*arrays):
    hbm = pl.BlockSpec(memory_space=pl.ANY)
    return pl.pallas_call(
        copy_kernel, name="copy_out", out_shape=[jax.ShapeDtypeStruct(a.shape, a.dtype) for a in arrays],
        in_specs=[hbm] * len(arrays), out_specs=[hbm] * len(arrays),
        scratch_shapes=[pltpu.VMEM(a.shape, a.dtype) for a in arrays] + [pltpu.SemaphoreType.DMA((TWO, FOUR)) for _ in arrays],
        compiler_params=pltpu.CompilerParams(vmem_limit_bytes=VMEM_BYTES),
    )(*arrays)


def solution(mesh):
    row_spec = P(("rep", "sp"), None)
    tok_spec = P(("rep", "sp"))
    full_spec = P(None)
    col_spec = P(None, "tp")
    wrow_spec = P("tp", None)
    cache_spec = P("rep", ("tp", "sp"), None)

    def local_layer(x_in, positions, segments, gain_attn, w_q, w_k, w_v, w_o, gain_mlp, w_gate, w_up, w_down):
        y_out, kc, vc = layer_call(x_in, positions, segments, gain_attn, gain_mlp, w_q, w_k, w_v, w_o, w_gate, w_up, w_down)
        return y_out, kc.reshape(-1, 1, HEAD_DIM), vc.reshape(-1, 1, HEAD_DIM)

    return jax.shard_map(local_layer, mesh=mesh,
                         in_specs=(row_spec, tok_spec, tok_spec, full_spec, col_spec, col_spec, col_spec, wrow_spec,
                                   full_spec, col_spec, col_spec, wrow_spec),
                         out_specs=(row_spec, cache_spec, cache_spec), check_vma=False)
```
